32 devices in a mesh: grp: 2 (over y), seq: 16 (over z, x, core).
Axes of the slice: x: 2, y: 2, z: 4, core: 2. Of those that a mesh axis runs over, the one named last changes fastest.
Arguments:
- hidden: bfloat16 [16, 4096], P('grp'), parts along dimension 0, may hold values from -6 to 6
- mix_gain: float32 [4096], replicated, may hold values from 0.5 to 1.5
- in_gate_input: bfloat16 [4096, 2048], P(None, 'seq'), may hold values from -0.09375 to 0.09375
- in_step: bfloat16 [4096, 16], P(None, 'seq'), may hold values from -0.09375 to 0.09375
- in_groups: bfloat16 [4096, 2048], P(None, 'seq'), may hold values from -0.09375 to 0.09375
- conv_input: bfloat16 [16, 3, 1024], P('grp', None, 'seq'), parts along dimension 0, may hold values from -6 to 6
- conv_groups: bfloat16 [16, 3, 2048], P('grp', None, 'seq'), parts along dimension 0, may hold values from -6 to 6
- taps_input: float32 [5, 1024], P(None, 'seq'), may hold values from -0.6 to 0.6
- taps_groups: float32 [5, 2048], P(None, 'seq'), may hold values from -0.6 to 0.6
- decay_rate: float32 [16], P('seq'), may hold values from 1 to 16
- step_bias: float32 [16], P('seq'), may hold values from -4 to -1
- skip_gain: float32 [16], P('seq'), may hold values from 0.1 to 1.9
- norm_gain: float32 [1024], P('seq'), may hold values from 0.5 to 1.5
- out_mixer: bfloat16 [1024, 4096], P('seq'), may hold values from -0.1875 to 0.1875
- ssm_state: float32 [16, 16, 64, 128], P('grp', 'seq'), parts along dimension 0, may hold values from -6 to 6
- attn_gain: float32 [4096], P('seq'), may hold values from 0.5 to 1.5
- w_qkv: bfloat16 [4096, 6144], P('seq'), may hold values from -0.09375 to 0.09375
- w_out: bfloat16 [4096, 4096], P(None, 'seq'), may hold values from -0.09375 to 0.09375
- kv_cache: bfloat16 [64, 128, 2048], P(('grp', 'seq')), parts along dimension 0, may hold values from -310 to 310
- page_table: int32 [16, 4], P('grp'), parts along dimension 0, may hold values from 0 to 31, as said below
- lengths: int32 [16], P('grp'), parts along dimension 0, may hold values from 1 to 512
Outputs:
- final: bfloat16 [16, 4096], P('grp', 'seq'), parts along dimension 0
- new_state: float32 [16, 16, 64, 128], P('grp', 'seq'), parts along dimension 0
- new_kv: bfloat16 [16, 2048], P('grp'), parts along dimension 0
The draws below stay inside these ranges and needn't reach their ends.
There are 2 independent parts, one for each index of `grp`. The reference program is written for one: setup_inputs(seed, part) draws one part's arguments, and reference() takes and returns one part's arrays. A program takes and returns all parts, laid end to end along the dimension named above; an argument that names none is the same for every part. Nothing has to cross between parts.
Inputs may be any that keep to these rules, and one draw needn't show every extreme that they name: `page_table`: each number 0 to 31 appears exactly once.
All inputs are finite; a program needn't handle non-finite values.
Results may differ from the reference program's by a relative error of at most 0.018.
Values may be sent and summed in bfloat16 or wider, within the bound.
No kernel may reach another device: no remote copies, remote signals or barrier semaphores. Data moves between devices by JAX's collectives and lax.ppermute only.
A program may use at most 64 MiB of HBM per device.

```python
import math
import jax
import jax.numpy as jnp
from jax import lax

D = 4096
QH = 32
KVH = 8
HD = 128
HEAD_P = 64
STATE = 128
GROUPS = 8
TAPS = 4
PAGE = 128
REQS = 8
HEADS = 16
D_INNER = 1024
BCW = 2048
TOTAL_PAGES = 32
PAGES_REQ = 4


def draw_page_table(key, part):
    order = jax.random.permutation(jax.random.fold_in(key, 11), TOTAL_PAGES)
    return order.astype(jnp.int32).reshape(REQS, PAGES_REQ)


def draw_kv_cache(key, part):
    base = jax.random.normal(jax.random.fold_in(key, 3), (TOTAL_PAGES, PAGE, 2 * KVH * HD), jnp.float32)
    base = jnp.clip(base, -6.0, 6.0)
    return base.astype(jnp.bfloat16)


def touch_ends(values, key, low, top_value):
    shape = values.shape
    spot = [jax.random.randint(jax.random.fold_in(key, axis), (), 0, shape[axis]) for axis in range(len(shape))]
    values = values.at[tuple(spot)].set(low)
    longest = shape.index(max(shape))
    spot[longest] = (spot[longest] + 1) % shape[longest]
    return values.at[tuple(spot)].set(top_value)


def levels(key, extent, shards, smallest, largest):
    factor_of = 1.0
    for axis_at, blocks in shards:
        steps = jax.random.uniform(jax.random.fold_in(jax.random.fold_in(key, 6), axis_at), (blocks,), jnp.float32, smallest / len(shards), largest / len(shards))
        factor_of = factor_of * jnp.repeat(jnp.exp(steps), extent[axis_at] // blocks).reshape((-1,) + (1,) * (len(extent) - 1 - axis_at))
    return factor_of


def bell_draw(rng, dims, width, bound, split=(), held_as=jnp.bfloat16):
    values = width * jax.random.normal(rng, dims, jnp.float32)
    if split:
        values = values * levels(rng, dims, split, -0.22, 0.18)
    return jnp.clip(values, -bound, bound).astype(held_as)


def setup_inputs(seed: int = 0, part: int = 0) -> dict:
    key_list = jax.random.split(jax.random.key(seed), 22)
    own_keys = jax.random.split(jax.random.fold_in(key_list[21], part), 22)
    return {
        "hidden": bell_draw(own_keys[0], (REQS, D), 1.0, 6.0),
        "mix_gain": jnp.clip(1.0 + 0.1 * jax.random.normal(key_list[1], (D,), jnp.float32), 0.5, 1.5),
        "in_gate_input": bell_draw(key_list[2], (D, 2 * D_INNER), D ** -0.5, 0.09375, ((1, 16),)),
        "in_step": bell_draw(key_list[3], (D, HEADS), D ** -0.5, 0.09375, ((1, 16),)),
        "in_groups": bell_draw(key_list[4], (D, BCW), D ** -0.5, 0.09375, ((1, 16),)),
        "conv_input": bell_draw(own_keys[5], (REQS, TAPS - 1, D_INNER), 1.0, 6.0, ((2, 16),)),
        "conv_groups": bell_draw(own_keys[6], (REQS, TAPS - 1, BCW), 1.0, 6.0, ((2, 16),)),
        "taps_input": jnp.clip(jax.random.uniform(key_list[7], (TAPS + 1, D_INNER), jnp.float32, -0.6, 0.6) * levels(key_list[7], (TAPS + 1, D_INNER), ((1, 16),), -0.4, 0.0), -0.6, 0.6),
        "taps_groups": jnp.clip(jax.random.uniform(key_list[8], (TAPS + 1, BCW), jnp.float32, -0.6, 0.6) * levels(key_list[8], (TAPS + 1, BCW), ((1, 16),), -0.4, 0.0), -0.6, 0.6),
        "decay_rate": jnp.clip(jnp.exp(math.log(16.0) - 2.7725887 * jax.random.uniform(key_list[9], (HEADS,), jnp.float32) ** levels(key_list[9], (HEADS,), ((0, 16),), -0.2, 0.2)), 1.0, 16.0),
        "step_bias": jnp.clip(-4.0 + 3.0 * jax.random.uniform(key_list[10], (HEADS,), jnp.float32) ** levels(key_list[10], (HEADS,), ((0, 16),), -0.2, 0.2), -4.0, -1.0),
        "skip_gain": jnp.clip(1.0 + 0.18 * jax.random.normal(key_list[11], (HEADS,), jnp.float32), 0.1, 1.9),
        "norm_gain": jnp.clip(1.0 + 0.1 * jax.random.normal(key_list[12], (D_INNER,), jnp.float32), 0.5, 1.5),
        "out_mixer": bell_draw(key_list[13], (D_INNER, D), D_INNER ** -0.5, 0.1875, ((0, 16),)),
        "ssm_state": bell_draw(own_keys[14], (REQS, HEADS, HEAD_P, STATE), 1.0, 6.0, ((1, 16),), jnp.float32),
        "attn_gain": jnp.clip(1.0 + 0.1 * jax.random.normal(key_list[15], (D,), jnp.float32), 0.5, 1.5),
        "w_qkv": bell_draw(key_list[16], (D, (QH + 2 * KVH) * HD), D ** -0.5, 0.09375, ((0, 16),)),
        "w_out": bell_draw(key_list[17], (QH * HD, D), (QH * HD) ** -0.5, 0.09375, ((1, 16),)),
        "kv_cache": draw_kv_cache(jax.random.fold_in(jax.random.fold_in(key_list[21], part), 71), part),
        "page_table": draw_page_table(jax.random.fold_in(jax.random.fold_in(key_list[21], part), 71), part),
        "lengths": touch_ends(jax.random.randint(own_keys[20], (REQS,), 1, PAGES_REQ * PAGE + 1), jax.random.fold_in(own_keys[20], 1), 1, PAGES_REQ * PAGE).astype(jnp.int32),
    }


epsilon = 1e-05
lowest = -1e+30

def conv_step(state, fresh, taps):
    window = jnp.concatenate([state.astype(jnp.float32), fresh[:, None, :]], axis=1)
    summed = lax.optimization_barrier(jnp.sum(window * taps[:-1][None], axis=1)) + taps[-1][None]
    return jax.nn.silu(summed)

def reference(hidden, mix_gain, in_gate_input, in_step, in_groups, conv_input, conv_groups, taps_input, taps_groups, decay_rate, step_bias, skip_gain, norm_gain, out_mixer, ssm_state, attn_gain, w_qkv, w_out, kv_cache, page_table, lengths):
    highest = lax.Precision.HIGHEST
    stream = hidden.astype(jnp.float32)
    normed = (stream * lax.rsqrt(lax.optimization_barrier(jnp.mean(stream * stream, axis=-1, keepdims=True)) + epsilon) * mix_gain).astype(jnp.bfloat16)
    gate_input = jnp.dot(normed, in_gate_input, preferred_element_type=jnp.float32).reshape(REQS, HEADS, 2, HEAD_P)
    gate_part = gate_input[:, :, 0]
    input_part = gate_input[:, :, 1].reshape(REQS, HEADS * HEAD_P)
    step_raw = jnp.dot(normed, in_step, preferred_element_type=jnp.float32)
    group_raw = jnp.dot(normed, in_groups, preferred_element_type=jnp.float32)
    conv_out = conv_step(conv_input, input_part, taps_input).reshape(REQS, HEADS, HEAD_P)
    group_conv = conv_step(conv_groups, group_raw, taps_groups).astype(jnp.bfloat16)
    group_conv = lax.optimization_barrier(group_conv).astype(jnp.float32)
    inject = group_conv[:, :GROUPS * STATE].reshape(REQS, GROUPS, STATE)
    readout = group_conv[:, GROUPS * STATE:].reshape(REQS, GROUPS, STATE)
    head_group = jnp.arange(HEADS, dtype=jnp.int32) % GROUPS
    inject_heads = inject[:, head_group]
    readout_heads = readout[:, head_group]
    step_size = jax.nn.softplus(step_raw + step_bias)
    decay = jnp.exp(-decay_rate * step_size)
    new_state = decay[:, :, None, None] * ssm_state + (step_size[:, :, None] * conv_out)[:, :, :, None] * inject_heads[:, :, None, :]
    ssm_out = jnp.einsum('rhpn,rhn->rhp', new_state, readout_heads, precision=highest) + skip_gain[None, :, None] * conv_out
    gated = ssm_out * jax.nn.silu(gate_part)
    grouped = gated.reshape(REQS, HEADS // GROUPS, GROUPS, HEAD_P)
    group_scale = lax.rsqrt(lax.optimization_barrier(jnp.mean(grouped * grouped, axis=(1, 3), keepdims=True)) + epsilon)
    normed_mix = ((grouped * group_scale).reshape(REQS, HEADS * HEAD_P) * norm_gain).astype(jnp.bfloat16)
    mixer = jnp.dot(normed_mix, out_mixer, preferred_element_type=jnp.float32)
    middle = (stream + mixer).astype(jnp.bfloat16)
    middle_f = middle.astype(jnp.float32)
    total_sq = lax.optimization_barrier(jnp.sum(middle_f * middle_f, axis=-1))
    scaled = (middle_f * attn_gain).astype(jnp.bfloat16)
    projected = jnp.dot(scaled, w_qkv, preferred_element_type=jnp.float32)
    qkv = (projected * lax.rsqrt(total_sq / D + epsilon)[:, None]).astype(jnp.bfloat16)
    group_size = QH // KVH
    queries = qkv[:, :QH * HD].reshape(REQS, KVH, group_size, HD)
    fresh_keys = qkv[:, QH * HD:(QH + KVH) * HD].reshape(REQS, KVH, HD)
    fresh_values = qkv[:, (QH + KVH) * HD:].reshape(REQS, KVH, HD)
    new_kv = qkv[:, QH * HD:]
    scale = 1.0 / HD ** 0.5
    context = PAGES_REQ * PAGE

    def one_request(request):
        table_row = page_table[request]
        pages = kv_cache[table_row].reshape(context, 2, KVH, HD).astype(jnp.float32)
        query_f = queries[request].astype(jnp.float32)
        key_own = fresh_keys[request].astype(jnp.float32)
        value_own = fresh_values[request].astype(jnp.float32)
        scores = jnp.einsum('gjd,tgd->gjt', query_f, pages[:, 0]) * scale
        live = jnp.arange(context, dtype=jnp.int32) < lengths[request]
        masked = jnp.where(live[None, None, :], scores, lowest)
        own = jnp.einsum('gjd,gd->gj', query_f, key_own) * scale
        peak = jnp.maximum(lax.optimization_barrier(jnp.max(masked, axis=-1)), own)
        weights = jnp.where(live[None, None, :], jnp.exp(masked - peak[..., None]), 0.0)
        rounded = lax.optimization_barrier(weights.astype(jnp.bfloat16)).astype(jnp.float32)
        own_weight = jnp.exp(own - peak)
        summed = jnp.einsum('gjt,tgd->gjd', rounded, pages[:, 1]) + own_weight[..., None] * value_own[:, None, :]
        total = lax.optimization_barrier(jnp.sum(weights, axis=-1)) + own_weight
        return (summed / total[..., None]).astype(jnp.bfloat16).reshape(QH * HD)
    attended = lax.map(one_request, jnp.arange(REQS, dtype=jnp.int32))
    final = (middle_f + jnp.dot(attended, w_out, preferred_element_type=jnp.float32)).astype(jnp.bfloat16)
    return (final, new_state, new_kv)
```

```python
import jax
import jax.numpy as jnp
from jax import lax
from jax.sharding import PartitionSpec as P

QH = 32
KVH = 8
HD = 128
STATE = 128
GROUPS = 8
LANES = 128

epsilon = 1e-05
lowest = -1e30


def conv_step(state, fresh, taps):
    window = jnp.concatenate([state.astype(jnp.float32), fresh[:, None, :]], axis=1)
    summed = jnp.sum(window * taps[:-1][None], axis=1) + taps[-1][None]
    return jax.nn.silu(summed)


def split(value, parts):
    pieces = []
    rest = value
    for _ in range(parts):
        piece = lax.reduce_precision(rest, 8, 7)
        pieces.append(piece.astype(jnp.bfloat16))
        rest = rest - piece
    return pieces


def group_vectors(group_conv, heads_here, requests):
    count = lax.axis_size("seq")
    position = lax.axis_index("seq")
    if heads_here == 1 and group_conv.shape[1] == STATE and count == 2 * GROUPS:
        swap = [(i, (i + GROUPS) % count) for i in range(count)]
        other = lax.ppermute(group_conv, "seq", swap)
        first = position < GROUPS
        inject = jnp.where(first, group_conv, other)
        readout = jnp.where(first, other, group_conv)
        return (
            inject.astype(jnp.float32)[:, None, :],
            readout.astype(jnp.float32)[:, None, :],
        )
    group_all = lax.all_gather(group_conv, "seq", axis=1, tiled=True).astype(jnp.float32)
    inject = group_all[:, : GROUPS * STATE].reshape(requests, GROUPS, STATE)
    readout = group_all[:, GROUPS * STATE :].reshape(requests, GROUPS, STATE)
    head_ids = position * heads_here + jnp.arange(heads_here, dtype=jnp.int32)
    return inject[:, head_ids % GROUPS], readout[:, head_ids % GROUPS]


def shards(
    hidden,
    mix_gain,
    in_gate_input,
    in_step,
    in_groups,
    conv_input,
    conv_groups,
    taps_input,
    taps_groups,
    decay_rate,
    step_bias,
    skip_gain,
    norm_gain,
    out_mixer,
    ssm_state,
    attn_gain,
    w_qkv,
    w_out,
    kv_cache,
    page_table,
    lengths,
):
    count_seq = lax.axis_size("seq")
    position = lax.axis_index("seq")
    requests = hidden.shape[0]
    width = hidden.shape[1]
    heads_here = in_step.shape[1]
    head_width = in_gate_input.shape[1] // (2 * heads_here)
    heads_total = heads_here * count_seq
    per_group = heads_total // GROUPS
    columns = width // count_seq
    stream = hidden.astype(jnp.float32)
    normed = (
        stream * lax.rsqrt(jnp.mean(stream * stream, axis=-1, keepdims=True) + epsilon) * mix_gain
    ).astype(jnp.bfloat16)
    group_raw = jnp.dot(normed, in_groups, preferred_element_type=jnp.float32)
    group_conv = conv_step(conv_groups, group_raw, taps_groups).astype(jnp.bfloat16)
    inject_heads, readout_heads = group_vectors(group_conv, heads_here, requests)
    gate_input = jnp.dot(normed, in_gate_input, preferred_element_type=jnp.float32).reshape(
        requests, heads_here, 2, head_width
    )
    gate_part = gate_input[:, :, 0]
    input_part = gate_input[:, :, 1].reshape(requests, heads_here * head_width)
    step_raw = jnp.dot(normed, in_step, preferred_element_type=jnp.float32)
    conv_out = conv_step(conv_input, input_part, taps_input).reshape(
        requests, heads_here, head_width
    )
    step_size = jax.nn.softplus(step_raw + step_bias)
    decay = jnp.exp(-decay_rate * step_size)
    new_state = (
        decay[:, :, None, None] * ssm_state
        + (step_size[:, :, None] * conv_out)[:, :, :, None] * inject_heads[:, :, None, :]
    )
    ssm_out = (
        jnp.sum(new_state * readout_heads[:, :, None, :], axis=-1)
        + skip_gain[None, :, None] * conv_out
    )
    gated = ssm_out * jax.nn.silu(gate_part)
    head_squares = jnp.sum(gated * gated, axis=-1)
    weighted = (gated * norm_gain.reshape(heads_here, head_width)).astype(jnp.bfloat16)
    products = jnp.einsum(
        "rhp,hpd->hrd",
        weighted,
        out_mixer.reshape(heads_here, head_width, width),
        preferred_element_type=jnp.float32,
    ).astype(jnp.bfloat16)
    products = products.reshape(heads_here, requests, count_seq, columns).transpose(2, 0, 1, 3)
    marks = jnp.stack(split(head_squares.T, 2), axis=-1)
    marks = jnp.pad(marks, ((0, 0), (0, 0), (0, LANES - 2)))
    marks = jnp.broadcast_to(marks[None], (count_seq,) + marks.shape)
    received = lax.all_to_all(jnp.concatenate([products, marks], axis=-1), "seq", 0, 0)
    received = received.astype(jnp.float32)
    squares = (received[..., columns] + received[..., columns + 1]).reshape(
        per_group, GROUPS, requests
    )
    scales = lax.rsqrt(jnp.sum(squares, axis=0) / (per_group * head_width) + epsilon)
    mixer = jnp.sum(
        received[..., :columns].reshape(per_group, GROUPS, requests, columns)
        * scales[None, :, :, None],
        axis=(0, 1),
    )
    stream_cols = lax.dynamic_slice_in_dim(stream, position * columns, columns, 1)
    middle = (stream_cols + mixer).astype(jnp.bfloat16)
    middle_f = middle.astype(jnp.float32)
    scaled = (middle_f * attn_gain).astype(jnp.bfloat16)
    partial_sq = jnp.sum(middle_f * middle_f, axis=-1)
    pages_here = kv_cache.shape[0]
    page_len = kv_cache.shape[1]
    pages_req = page_table.shape[1]
    pages_all = pages_here * count_seq
    matches = page_table[None, :, :] == jnp.arange(pages_all, dtype=jnp.int32)[:, None, None]
    owner = jnp.any(matches, axis=2)
    page_rows = jnp.dot(
        owner.astype(jnp.bfloat16), scaled, preferred_element_type=jnp.float32
    ).astype(jnp.bfloat16)
    page_proj = jnp.dot(page_rows, w_qkv, preferred_element_type=jnp.float32).astype(jnp.bfloat16)
    page_sq = jnp.sum(jnp.where(owner, partial_sq[None, :], 0.0), axis=1)
    sq_parts = jnp.pad(jnp.stack(split(page_sq, 2), axis=-1), ((0, 0), (0, LANES - 2)))
    sent = jnp.concatenate([page_proj, sq_parts], axis=-1).reshape(count_seq, pages_here, -1)
    arrived = jnp.sum(lax.all_to_all(sent, "seq", 0, 0).astype(jnp.float32), axis=0)
    qkv_width = w_qkv.shape[1]
    total_sq = arrived[:, qkv_width] + arrived[:, qkv_width + 1]
    qkv = (arrived[:, :qkv_width] * lax.rsqrt(total_sq / width + epsilon)[:, None]).astype(
        jnp.bfloat16
    )
    group_size = QH // KVH
    queries = qkv[:, : QH * HD].reshape(pages_here, KVH, group_size, HD)
    fresh_kv = qkv[:, QH * HD :]
    fresh_keys = fresh_kv[:, : KVH * HD].reshape(pages_here, KVH, 1, HD).astype(jnp.float32)
    fresh_values = fresh_kv[:, KVH * HD :].reshape(pages_here, KVH, 1, HD).astype(jnp.float32)
    scale = 1.0 / HD**0.5
    slots = position * pages_here + jnp.arange(pages_here, dtype=jnp.int32)
    own_matches = page_table[None, :, :] == slots[:, None, None]
    logical = jnp.sum(
        jnp.any(own_matches, axis=1) * jnp.arange(pages_req, dtype=jnp.int32)[None, :], axis=1
    )
    page_length = jnp.sum(jnp.where(jnp.any(own_matches, axis=2), lengths[None, :], 0), axis=1)
    token_pos = logical[:, None] * page_len + jnp.arange(page_len, dtype=jnp.int32)[None, :]
    live = (token_pos < page_length[:, None])[:, None, None, :]
    leads = (logical == 0)[:, None, None]
    cached = kv_cache.reshape(pages_here, page_len, 2, KVH, HD)
    scores = (
        jnp.einsum("pgjd,ptgd->pgjt", queries, cached[:, :, 0], preferred_element_type=jnp.float32)
        * scale
    )
    own = jnp.sum(queries.astype(jnp.float32) * fresh_keys, axis=-1) * scale
    masked = jnp.where(live, scores, lowest)
    own = jnp.where(leads, own, lowest)
    peak = jnp.maximum(jnp.max(masked, axis=-1), own)
    weights = jnp.where(live, jnp.exp(masked - peak[..., None]), 0.0)
    own_weight = jnp.where(leads, jnp.exp(own - peak), 0.0)
    total = jnp.sum(weights, axis=-1) + own_weight
    values = jnp.einsum(
        "pgjt,ptgd->pgjd",
        weights.astype(jnp.bfloat16),
        cached[:, :, 1],
        preferred_element_type=jnp.float32,
    )
    values = values + own_weight[..., None] * fresh_values
    some = total > 0.0
    safe = jnp.where(some, total, 1.0)
    values = (values / safe[..., None]).astype(jnp.bfloat16)
    logsum = jnp.where(some, peak + jnp.log(safe), lowest)
    logs = jnp.concatenate(split(logsum.reshape(1, pages_here * QH), 3), axis=0)
    logs = jnp.pad(logs, ((0, 5), (0, LANES - pages_here * QH)))
    value_rows = pages_here * QH
    kv_rows = pages_here * 2 * KVH
    package = jnp.concatenate(
        [values.reshape(value_rows, HD), fresh_kv.reshape(kv_rows, HD), logs], axis=0
    )
    package = jnp.broadcast_to(package[None], (count_seq,) + package.shape)
    everything = lax.all_to_all(package, "seq", 0, 0)
    all_values = everything[:, :value_rows].reshape(pages_all, QH, HD)
    all_kv = everything[:, value_rows : value_rows + kv_rows].reshape(pages_all, 2 * KVH * HD)
    all_logs = everything[:, value_rows + kv_rows :, : pages_here * QH].astype(jnp.float32)
    all_logs = (all_logs[:, 0] + all_logs[:, 1] + all_logs[:, 2]).reshape(pages_all, QH)
    new_kv = all_kv[page_table[:, 0]]
    req_logs = all_logs[page_table]
    top = jnp.max(req_logs, axis=1, keepdims=True)
    factors = jnp.exp(req_logs - top)
    summed = jnp.sum(factors[..., None] * all_values[page_table].astype(jnp.float32), axis=1)
    attended = (summed / jnp.sum(factors, axis=1)[..., None]).astype(jnp.bfloat16)
    final = (
        middle_f
        + jnp.dot(
            attended.reshape(requests, QH * HD), w_out, preferred_element_type=jnp.float32
        )
    ).astype(jnp.bfloat16)
    return (final, new_state, new_kv)


def solution(mesh):
    placed = (
        P("grp", None),
        P(),
        P(None, "seq"),
        P(None, "seq"),
        P(None, "seq"),
        P("grp", None, "seq"),
        P("grp", None, "seq"),
        P(None, "seq"),
        P(None, "seq"),
        P("seq"),
        P("seq"),
        P("seq"),
        P("seq"),
        P("seq", None),
        P("grp", "seq", None, None),
        P("seq"),
        P("seq", None),
        P(None, "seq"),
        P(("grp", "seq"), None, None),
        P("grp", None),
        P("grp"),
    )
    return jax.shard_map(
        shards,
        mesh=mesh,
        in_specs=placed,
        out_specs=(P("grp", "seq"), P("grp", "seq", None, None), P("grp", None)),
        check_vma=False,
    )
```

```python
import functools

import jax
import jax.numpy as jnp
from jax import lax
from jax.experimental import pallas as pl
from jax.experimental.pallas import tpu as pltpu
from jax.sharding import PartitionSpec as P

QH = 32
KVH = 8
HD = 128
STATE = 128
GROUPS = 8
LANES = 128

epsilon = 1e-05
lowest = -1e30


def conv_step(state, fresh, taps):
    window = jnp.concatenate([state.astype(jnp.float32), fresh[:, None, :]], axis=1)
    summed = jnp.sum(window * taps[:-1][None], axis=1) + taps[-1][None]
    return jax.nn.silu(summed)


def split(value, parts):
    pieces = []
    rest = value
    for _ in range(parts):
        piece = lax.reduce_precision(rest, 8, 7)
        pieces.append(piece.astype(jnp.bfloat16))
        rest = rest - piece
    return pieces


def group_vectors(group_conv, heads_here, requests):
    count = lax.axis_size("seq")
    position = lax.axis_index("seq")
    if heads_here == 1 and group_conv.shape[1] == STATE and count == 2 * GROUPS:
        swap = [(i, (i + GROUPS) % count) for i in range(count)]
        other = lax.ppermute(group_conv, "seq", swap)
        first = position < GROUPS
        inject = jnp.where(first, group_conv, other)
        readout = jnp.where(first, other, group_conv)
        return (
            inject.astype(jnp.float32)[:, None, :],
            readout.astype(jnp.float32)[:, None, :],
        )
    group_all = lax.all_gather(group_conv, "seq", axis=1, tiled=True).astype(jnp.float32)
    inject = group_all[:, : GROUPS * STATE].reshape(requests, GROUPS, STATE)
    readout = group_all[:, GROUPS * STATE :].reshape(requests, GROUPS, STATE)
    head_ids = position * heads_here + jnp.arange(heads_here, dtype=jnp.int32)
    return inject[:, head_ids % GROUPS], readout[:, head_ids % GROUPS]


def plain_shards(
    hidden,
    mix_gain,
    in_gate_input,
    in_step,
    in_groups,
    conv_input,
    conv_groups,
    taps_input,
    taps_groups,
    decay_rate,
    step_bias,
    skip_gain,
    norm_gain,
    out_mixer,
    ssm_state,
    attn_gain,
    w_qkv,
    w_out,
    kv_cache,
    page_table,
    lengths,
):
    count_seq = lax.axis_size("seq")
    position = lax.axis_index("seq")
    requests = hidden.shape[0]
    width = hidden.shape[1]
    heads_here = in_step.shape[1]
    head_width = in_gate_input.shape[1] // (2 * heads_here)
    heads_total = heads_here * count_seq
    per_group = heads_total // GROUPS
    columns = width // count_seq
    stream = hidden.astype(jnp.float32)
    normed = (
        stream * lax.rsqrt(jnp.mean(stream * stream, axis=-1, keepdims=True) + epsilon) * mix_gain
    ).astype(jnp.bfloat16)
    group_raw = jnp.dot(normed, in_groups, preferred_element_type=jnp.float32)
    group_conv = conv_step(conv_groups, group_raw, taps_groups).astype(jnp.bfloat16)
    inject_heads, readout_heads = group_vectors(group_conv, heads_here, requests)
    gate_input = jnp.dot(normed, in_gate_input, preferred_element_type=jnp.float32).reshape(
        requests, heads_here, 2, head_width
    )
    gate_part = gate_input[:, :, 0]
    input_part = gate_input[:, :, 1].reshape(requests, heads_here * head_width)
    step_raw = jnp.dot(normed, in_step, preferred_element_type=jnp.float32)
    conv_out = conv_step(conv_input, input_part, taps_input).reshape(
        requests, heads_here, head_width
    )
    step_size = jax.nn.softplus(step_raw + step_bias)
    decay = jnp.exp(-decay_rate * step_size)
    new_state = (
        decay[:, :, None, None] * ssm_state
        + (step_size[:, :, None] * conv_out)[:, :, :, None] * inject_heads[:, :, None, :]
    )
    ssm_out = (
        jnp.sum(new_state * readout_heads[:, :, None, :], axis=-1)
        + skip_gain[None, :, None] * conv_out
    )
    gated = ssm_out * jax.nn.silu(gate_part)
    head_squares = jnp.sum(gated * gated, axis=-1)
    weighted = (gated * norm_gain.reshape(heads_here, head_width)).astype(jnp.bfloat16)
    products = jnp.einsum(
        "rhp,hpd->hrd",
        weighted,
        out_mixer.reshape(heads_here, head_width, width),
        preferred_element_type=jnp.float32,
    ).astype(jnp.bfloat16)
    products = products.reshape(heads_here, requests, count_seq, columns).transpose(2, 0, 1, 3)
    marks = jnp.stack(split(head_squares.T, 2), axis=-1)
    marks = jnp.pad(marks, ((0, 0), (0, 0), (0, LANES - 2)))
    marks = jnp.broadcast_to(marks[None], (count_seq,) + marks.shape)
    received = lax.all_to_all(jnp.concatenate([products, marks], axis=-1), "seq", 0, 0)
    received = received.astype(jnp.float32)
    squares = (received[..., columns] + received[..., columns + 1]).reshape(
        per_group, GROUPS, requests
    )
    scales = lax.rsqrt(jnp.sum(squares, axis=0) / (per_group * head_width) + epsilon)
    mixer = jnp.sum(
        received[..., :columns].reshape(per_group, GROUPS, requests, columns)
        * scales[None, :, :, None],
        axis=(0, 1),
    )
    stream_cols = lax.dynamic_slice_in_dim(stream, position * columns, columns, 1)
    middle = (stream_cols + mixer).astype(jnp.bfloat16)
    middle_f = middle.astype(jnp.float32)
    scaled = (middle_f * attn_gain).astype(jnp.bfloat16)
    partial_sq = jnp.sum(middle_f * middle_f, axis=-1)
    pages_here = kv_cache.shape[0]
    page_len = kv_cache.shape[1]
    pages_req = page_table.shape[1]
    pages_all = pages_here * count_seq
    matches = page_table[None, :, :] == jnp.arange(pages_all, dtype=jnp.int32)[:, None, None]
    owner = jnp.any(matches, axis=2)
    page_rows = jnp.dot(
        owner.astype(jnp.bfloat16), scaled, preferred_element_type=jnp.float32
    ).astype(jnp.bfloat16)
    page_proj = jnp.dot(page_rows, w_qkv, preferred_element_type=jnp.float32).astype(jnp.bfloat16)
    page_sq = jnp.sum(jnp.where(owner, partial_sq[None, :], 0.0), axis=1)
    sq_parts = jnp.pad(jnp.stack(split(page_sq, 2), axis=-1), ((0, 0), (0, LANES - 2)))
    sent = jnp.concatenate([page_proj, sq_parts], axis=-1).reshape(count_seq, pages_here, -1)
    arrived = jnp.sum(lax.all_to_all(sent, "seq", 0, 0).astype(jnp.float32), axis=0)
    qkv_width = w_qkv.shape[1]
    total_sq = arrived[:, qkv_width] + arrived[:, qkv_width + 1]
    qkv = (arrived[:, :qkv_width] * lax.rsqrt(total_sq / width + epsilon)[:, None]).astype(
        jnp.bfloat16
    )
    group_size = QH // KVH
    queries = qkv[:, : QH * HD].reshape(pages_here, KVH, group_size, HD)
    fresh_kv = qkv[:, QH * HD :]
    fresh_keys = fresh_kv[:, : KVH * HD].reshape(pages_here, KVH, 1, HD).astype(jnp.float32)
    fresh_values = fresh_kv[:, KVH * HD :].reshape(pages_here, KVH, 1, HD).astype(jnp.float32)
    scale = 1.0 / HD**0.5
    slots = position * pages_here + jnp.arange(pages_here, dtype=jnp.int32)
    own_matches = page_table[None, :, :] == slots[:, None, None]
    logical = jnp.sum(
        jnp.any(own_matches, axis=1) * jnp.arange(pages_req, dtype=jnp.int32)[None, :], axis=1
    )
    page_length = jnp.sum(jnp.where(jnp.any(own_matches, axis=2), lengths[None, :], 0), axis=1)
    token_pos = logical[:, None] * page_len + jnp.arange(page_len, dtype=jnp.int32)[None, :]
    live = (token_pos < page_length[:, None])[:, None, None, :]
    leads = (logical == 0)[:, None, None]
    cached = kv_cache.reshape(pages_here, page_len, 2, KVH, HD)
    scores = (
        jnp.einsum("pgjd,ptgd->pgjt", queries, cached[:, :, 0], preferred_element_type=jnp.float32)
        * scale
    )
    own = jnp.sum(queries.astype(jnp.float32) * fresh_keys, axis=-1) * scale
    masked = jnp.where(live, scores, lowest)
    own = jnp.where(leads, own, lowest)
    peak = jnp.maximum(jnp.max(masked, axis=-1), own)
    weights = jnp.where(live, jnp.exp(masked - peak[..., None]), 0.0)
    own_weight = jnp.where(leads, jnp.exp(own - peak), 0.0)
    total = jnp.sum(weights, axis=-1) + own_weight
    values = jnp.einsum(
        "pgjt,ptgd->pgjd",
        weights.astype(jnp.bfloat16),
        cached[:, :, 1],
        preferred_element_type=jnp.float32,
    )
    values = values + own_weight[..., None] * fresh_values
    some = total > 0.0
    safe = jnp.where(some, total, 1.0)
    values = (values / safe[..., None]).astype(jnp.bfloat16)
    logsum = jnp.where(some, peak + jnp.log(safe), lowest)
    logs = jnp.concatenate(split(logsum.reshape(1, pages_here * QH), 3), axis=0)
    logs = jnp.pad(logs, ((0, 5), (0, LANES - pages_here * QH)))
    value_rows = pages_here * QH
    kv_rows = pages_here * 2 * KVH
    package = jnp.concatenate(
        [values.reshape(value_rows, HD), fresh_kv.reshape(kv_rows, HD), logs], axis=0
    )
    package = jnp.broadcast_to(package[None], (count_seq,) + package.shape)
    everything = lax.all_to_all(package, "seq", 0, 0)
    all_values = everything[:, :value_rows].reshape(pages_all, QH, HD)
    all_kv = everything[:, value_rows : value_rows + kv_rows].reshape(pages_all, 2 * KVH * HD)
    all_logs = everything[:, value_rows + kv_rows :, : pages_here * QH].astype(jnp.float32)
    all_logs = (all_logs[:, 0] + all_logs[:, 1] + all_logs[:, 2]).reshape(pages_all, QH)
    new_kv = all_kv[page_table[:, 0]]
    req_logs = all_logs[page_table]
    top = jnp.max(req_logs, axis=1, keepdims=True)
    factors = jnp.exp(req_logs - top)
    summed = jnp.sum(factors[..., None] * all_values[page_table].astype(jnp.float32), axis=1)
    attended = (summed / jnp.sum(factors, axis=1)[..., None]).astype(jnp.bfloat16)
    final = (
        middle_f
        + jnp.dot(
            attended.reshape(requests, QH * HD), w_out, preferred_element_type=jnp.float32
        )
    ).astype(jnp.bfloat16)
    return (final, new_state, new_kv)


f32 = jnp.float32
bf16 = jnp.bfloat16
SUB = 8
PARTS = 3
VMEM = pl.BlockSpec(memory_space=pltpu.VMEM)
SMEM = pl.BlockSpec(memory_space=pltpu.SMEM)


def call(kernel, outs, specs, scratch=()):
    return pl.pallas_call(
        kernel,
        out_shape=outs,
        in_specs=specs,
        out_specs=jax.tree.map(lambda _: VMEM, outs),
        scratch_shapes=scratch,
    )


def shape(dims, kind):
    return jax.ShapeDtypeStruct(dims, kind)


def silu(x):
    return x * jax.nn.sigmoid(x)


def pieces(value, parts):
    out = []
    for _ in range(parts):
        piece = value.astype(bf16).astype(f32)
        out.append(piece)
        value = value - piece
    return out


def marked(value, parts):
    lane = lax.broadcasted_iota(jnp.int32, (value.shape[0], LANES), 1)
    out = jnp.zeros((value.shape[0], LANES), f32)
    for k, piece in enumerate(pieces(value, parts)):
        out = jnp.where(lane == k, piece, out)
    return out


def convolve(state_ref, fresh, taps_ref):
    taps = state_ref.shape[0]
    total = taps_ref[taps : taps + 1, :] * fresh + taps_ref[taps + 1 : taps + 2, :]
    for k in range(taps):
        total = total + taps_ref[k : k + 1, :] * state_ref[k].astype(f32)
    return silu(total)


def group_kernel(hidden, gain, weights, state, taps, group_out, normed_out):
    stream = hidden[...].astype(f32)
    mean = jnp.mean(stream * stream, axis=-1, keepdims=True)
    normed = (stream * lax.rsqrt(mean + epsilon) * gain[...]).astype(bf16)
    normed_out[...] = normed
    raw = jnp.dot(normed, weights[...], preferred_element_type=f32)
    group_out[...] = convolve(state, raw, taps).astype(bf16)


def gate_kernel(
    normed_ref, weights, step_row, state, taps, rate, bias, gate_out, conv_out, step_out, decay_out
):
    normed = normed_ref[...]
    both = jnp.dot(normed, weights[...], preferred_element_type=f32)
    half = both.shape[1] // 2
    gate_out[...] = silu(both[:, :half])
    conv_out[...] = convolve(state, both[:, half:], taps)
    raw = jnp.sum(
        normed.astype(f32) * step_row[...].astype(f32), axis=-1, keepdims=True
    )
    step = jax.nn.softplus(raw + bias[0])
    step_out[...] = jnp.broadcast_to(step, step_out.shape)
    decay_out[...] = jnp.broadcast_to(jnp.exp(-rate[0] * step), decay_out.shape)


def chosen(position, own, other):
    first = position[0] < GROUPS
    mine, theirs = own[...].astype(f32), other[...].astype(f32)
    return jnp.where(first, mine, theirs), jnp.where(first, theirs, mine)


def mixer_kernel(
    position, skip, own, other, gate, conv, step, decay, state, weights, gain, sent
):
    requests = own.shape[0]
    inject, readout = chosen(position, own, other)
    row = lax.broadcasted_iota(jnp.int32, conv.shape, 0)
    read = jnp.zeros(conv.shape, f32)
    for r in range(requests):
        part = lax.dot_general(
            readout,
            state[r],
            (((1,), (1,)), ((), ())),
            precision=lax.Precision.HIGHEST,
            preferred_element_type=f32,
        )
        read = jnp.where(row == r, part, read)
    along = jnp.sum(inject * readout, axis=-1, keepdims=True)
    fresh = conv[...]
    out = (
        decay[:, :1] * read
        + step[:, :1] * fresh * along
        + skip[0] * fresh
    )
    gated = out * gate[...]
    marks = marked(jnp.sum(gated * gated, axis=-1, keepdims=True), 2).astype(bf16)
    weighted = (gated * gain[...]).astype(bf16)
    count = sent.shape[0]
    columns = weights.shape[1] // count
    for e in range(count):
        product = jnp.dot(
            weighted, weights[:, e * columns : (e + 1) * columns], preferred_element_type=f32
        )
        sent[e, :, :columns] = product.astype(bf16)
        sent[e, :, columns:] = marks


def state_kernel(position, own, other, conv, step, decay, state, new_state):
    inject, _ = chosen(position, own, other)
    fresh = step[:, :1] * conv[...]
    new_state[...] = (
        decay[:, :1][:, :, None] * state[...] + fresh[:, :, None] * inject[:, None, :]
    )


def project_kernel(
    chunks, head_width, position, received, hidden, gain, weights, table, sent, middle_out
):
    count, requests, _ = received.shape
    columns = weights.shape[0]
    squares = [received[k, :, columns:].astype(f32) for k in range(count)]
    mixer = jnp.zeros((requests, columns), f32)
    for g in range(GROUPS):
        members = range(g, count, GROUPS)
        marks = sum(squares[k] for k in members)
        total = marks[:, :1] + marks[:, 1:2]
        scale = lax.rsqrt(total / (len(members) * head_width) + epsilon)
        products = sum(received[k, :, :columns].astype(f32) for k in members)
        mixer = mixer + scale * products
    start = pl.multiple_of(position[0] * columns, columns)
    middle = (hidden[:, pl.ds(start, columns)].astype(f32) + mixer).astype(bf16).astype(f32)
    middle_out[...] = middle
    marks = marked(jnp.sum(middle * middle, axis=-1, keepdims=True), 2)
    extended = jnp.concatenate([middle * gain[...], marks], axis=-1).astype(bf16)
    rows = count * SUB
    pages = SUB // chunks
    index = lax.broadcasted_iota(jnp.int32, (rows, requests), 0)
    page = (index // SUB) * pages + index % pages
    hits = page == table[0:1, :]
    for j in range(1, table.shape[0]):
        hits = jnp.logical_or(hits, page == table[j : j + 1, :])
    onehot = jnp.where(hits, 1.0, 0.0).astype(bf16)
    spread = jnp.dot(onehot, extended, preferred_element_type=f32)
    lines = spread[:, :columns]
    which = (lax.broadcasted_iota(jnp.int32, lines.shape, 0) % SUB) // pages
    lhs = [jnp.where(which == c, lines, 0.0).astype(bf16) for c in range(chunks)]
    chunk = weights.shape[1] // chunks
    tile = 256
    for n in range(0, chunk, tile):
        total = None
        for c in range(chunks):
            part = jnp.dot(
                lhs[c],
                weights[:, c * chunk + n : c * chunk + n + tile],
                preferred_element_type=f32,
            )
            total = part if total is None else total + part
        for e in range(count):
            sent[e, :, n : n + tile] = total[e * SUB : (e + 1) * SUB].astype(bf16)
    for e in range(count):
        sent[e, :, chunk:] = spread[e * SUB : (e + 1) * SUB, columns:].astype(bf16)


def attend_kernel(width, position, received, cache, table, lengths, sent, lines):
    count, _, full = received.shape
    pages, page_len, _ = cache.shape
    chunks = SUB // pages
    chunk = full - LANES
    tiles = chunk // HD
    total = received[0].astype(f32)
    for k in range(1, count):
        total = total + received[k].astype(f32)
    squares = total[:, chunk : chunk + 1] + total[:, chunk + 1 : chunk + 2]
    inverse = lax.rsqrt(squares / width + epsilon)
    for t in range(tiles):
        lines[t * SUB : (t + 1) * SUB, :] = (
            (total[:, t * HD : (t + 1) * HD] * inverse).astype(bf16).astype(f32)
        )

    def heads(page, first, many):
        start = (first % tiles) * SUB + (first // tiles) * pages + page
        return lines[pl.ds(start, many, stride=SUB), :]

    group = QH // KVH
    scale = 1.0 / HD**0.5
    lane = lax.broadcasted_iota(jnp.int32, (1, page_len), 1)
    head_group = lax.broadcasted_iota(jnp.int32, (QH, HD), 0) // group
    eye = lax.broadcasted_iota(jnp.int32, (QH, LANES), 0)
    eye_lane = lax.broadcasted_iota(jnp.int32, (QH, LANES), 1)
    order = lax.broadcasted_iota(jnp.int32, table.shape, 0)
    value_rows = pages * QH
    fresh_rows = 2 * KVH
    log_row = jnp.zeros((1, LANES), f32)
    for p in range(pages):
        slot = position[0] * pages + p
        hit = table[...] == slot
        logical = jnp.sum(jnp.where(hit, order, 0), axis=(0, 1), keepdims=True)
        length = jnp.sum(
            jnp.where(hit, jnp.broadcast_to(lengths[...], hit.shape), 0),
            axis=(0, 1),
            keepdims=True,
        )
        live = logical * page_len + lane < length
        leads = logical == 0
        query = jnp.concatenate([heads(p, g * group, group) for g in range(KVH)], axis=0)
        keys = [heads(p, QH + g, 1) for g in range(KVH)]
        values = [heads(p, QH + KVH + g, 1) for g in range(KVH)]
        key_rows = jnp.concatenate([jnp.broadcast_to(k, (group, HD)) for k in keys], axis=0)
        value_own = jnp.concatenate([jnp.broadcast_to(v, (group, HD)) for v in values], axis=0)
        spread = jnp.concatenate(
            [jnp.where(head_group == g, query, 0.0).astype(bf16) for g in range(KVH)], axis=-1
        )
        scores = (
            lax.dot_general(
                spread,
                cache[p, :, : KVH * HD],
                (((1,), (1,)), ((), ())),
                preferred_element_type=f32,
            )
            * scale
        )
        own = jnp.sum(query * key_rows, axis=-1, keepdims=True) * scale
        masked = jnp.where(live, scores, lowest)
        own = jnp.where(leads, own, lowest)
        peak = jnp.maximum(jnp.max(masked, axis=-1, keepdims=True), own)
        weights = jnp.where(live, jnp.exp(masked - peak), 0.0)
        own_weight = jnp.where(leads, jnp.exp(own - peak), 0.0)
        mass = jnp.sum(weights, axis=-1, keepdims=True) + own_weight
        wide = jnp.dot(
            weights.astype(bf16), cache[p, :, KVH * HD :], preferred_element_type=f32
        )
        summed = own_weight * value_own
        for g in range(KVH):
            summed = summed + jnp.where(head_group == g, wide[:, g * HD : (g + 1) * HD], 0.0)
        some = mass > 0.0
        safe = jnp.where(some, mass, 1.0)
        result = (summed / safe).astype(bf16)
        logs = jnp.where(some, peak + jnp.log(safe), lowest)
        log_row = log_row + jnp.sum(
            jnp.where(eye_lane == eye + p * QH, logs, 0.0), axis=0, keepdims=True
        )
        fresh = jnp.concatenate(keys + values, axis=0).astype(bf16)
        for e in range(count):
            sent[e, p * QH : (p + 1) * QH, :] = result
            first = value_rows + p * fresh_rows
            sent[e, first : first + fresh_rows, :] = fresh
    terms = pieces(log_row, PARTS) + [jnp.zeros((SUB - PARTS, LANES), f32)]
    terms = jnp.concatenate(terms, axis=0).astype(bf16)
    for e in range(count):
        sent[e, value_rows + pages * fresh_rows :, :] = terms


def merge_kernel(pages, table, received, weights, middle, final, new_kv, spread, rows, fresh):
    count, package, _ = received.shape
    requests, pages_req = table.shape
    value_rows = pages * QH
    kv_rows = 2 * KVH
    last = value_rows + pages * kv_rows
    logs = jnp.concatenate([received[k, last:, :] for k in range(count)], axis=0)
    source = lax.broadcasted_iota(jnp.int32, (count * SUB, LANES), 0) // SUB
    for k in range(count):
        mask = jnp.where(source == k, 1.0, 0.0).astype(bf16)
        spread[k] = lax.dot_general(
            logs, mask, (((0,), (0,)), ((), ())), preferred_element_type=f32
        )
    for r in range(requests):
        peaks, values = [], []
        for j in range(pages_req):
            page = table[r, j]
            device, slot = page // pages, page % pages
            first = pl.multiple_of(slot * QH, QH)
            peaks.append(spread[device, pl.ds(first, QH), :])
            values.append(received[device, pl.ds(first, QH), :].astype(f32))
        top = functools.reduce(jnp.maximum, peaks)
        mass = jnp.zeros(top.shape, f32)
        summed = jnp.zeros(top.shape, f32)
        for peak, value in zip(peaks, values):
            factor = jnp.exp(peak - top)
            mass = mass + factor
            summed = summed + factor * value
        rows[r * QH : (r + 1) * QH, :] = summed / mass
        page = table[r, 0]
        first = pl.multiple_of(value_rows + (page % pages) * kv_rows, kv_rows)
        fresh[r * kv_rows : (r + 1) * kv_rows, :] = received[
            page // pages, pl.ds(first, kv_rows), :
        ].astype(f32)
    for c in range(kv_rows):
        new_kv[:, c * HD : (c + 1) * HD] = fresh[pl.ds(c, requests, stride=kv_rows), :].astype(
            bf16
        )
    attended = jnp.concatenate(
        [rows[pl.ds(h, requests, stride=QH), :].astype(bf16) for h in range(QH)], axis=-1
    )
    total = jnp.dot(attended, weights[...], preferred_element_type=f32)
    final[...] = (middle[...] + total).astype(bf16)


def fused_shards(
    hidden,
    mix_gain,
    in_gate_input,
    in_step,
    in_groups,
    conv_input,
    conv_groups,
    taps_input,
    taps_groups,
    decay_rate,
    step_bias,
    skip_gain,
    norm_gain,
    out_mixer,
    ssm_state,
    attn_gain,
    w_qkv,
    w_out,
    kv_cache,
    page_table,
    lengths,
):
    count = lax.axis_size("seq")
    position = lax.axis_index("seq").astype(jnp.int32).reshape(1)
    requests, width = hidden.shape
    columns = width // count
    head_width = in_gate_input.shape[1] // 2
    pages = kv_cache.shape[0]
    chunks = SUB // pages
    gcols = in_groups.shape[1]
    group_conv, normed = call(
        group_kernel,
        (shape((requests, gcols), bf16), shape((requests, width), bf16)),
        [VMEM] * 5,
    )(
        hidden,
        mix_gain.reshape(1, width),
        in_groups,
        conv_groups.transpose(1, 0, 2),
        taps_groups,
    )
    swap = [(i, (i + GROUPS) % count) for i in range(count)]
    other = lax.ppermute(group_conv, "seq", swap)
    gate, conv, step, decay = call(
        gate_kernel,
        (
            shape((requests, head_width), f32),
            shape((requests, head_width), f32),
            shape((requests, LANES), f32),
            shape((requests, LANES), f32),
        ),
        [VMEM] * 5 + [SMEM] * 2,
    )(
        normed,
        in_gate_input,
        in_step.T,
        conv_input.transpose(1, 0, 2),
        taps_input,
        decay_rate,
        step_bias,
    )
    state = ssm_state.reshape(requests, head_width, STATE)
    sent = call(
        mixer_kernel,
        shape((count, requests, columns + LANES), bf16),
        [SMEM] * 2 + [VMEM] * 9,
    )(
        position,
        skip_gain,
        group_conv,
        other,
        gate,
        conv,
        step,
        decay,
        state,
        out_mixer,
        norm_gain.reshape(1, head_width),
    )
    received = lax.all_to_all(sent, "seq", 0, 0)
    new_state = call(state_kernel, shape(state.shape, f32), [SMEM] + [VMEM] * 6)(
        position, group_conv, other, conv, step, decay, state
    )
    chunk = w_qkv.shape[1] // chunks
    sent, middle = call(
        functools.partial(project_kernel, chunks, head_width),
        (
            shape((count, SUB, chunk + LANES), bf16),
            shape((requests, columns), f32),
        ),
        [SMEM] + [VMEM] * 5,
    )(position, received, hidden, attn_gain.reshape(1, columns), w_qkv, page_table.T)
    received = lax.all_to_all(sent, "seq", 0, 0)
    package = pages * (QH + 2 * KVH) + SUB
    sent = call(
        functools.partial(attend_kernel, width),
        shape((count, package, HD), bf16),
        [SMEM] + [VMEM] * 4,
        [pltpu.VMEM((chunk // HD * SUB, HD), f32)],
    )(position, received, kv_cache, page_table.T, lengths.reshape(1, requests))
    received = lax.all_to_all(sent, "seq", 0, 0)
    final, new_kv = call(
        functools.partial(merge_kernel, pages),
        (
            shape((requests, columns), bf16),
            shape((requests, 2 * KVH * HD), bf16),
        ),
        [SMEM] + [VMEM] * 3,
        [
            pltpu.VMEM((count, LANES, LANES), f32),
            pltpu.VMEM((requests * QH, HD), f32),
            pltpu.VMEM((requests * 2 * KVH, HD), f32),
        ],
    )(page_table, received, w_out, middle)
    return (final, new_state.reshape(ssm_state.shape), new_kv)


def shards(*args):
    hidden, in_step, in_groups = args[0], args[3], args[4]
    kv_cache, page_table = args[18], args[19]
    count = lax.axis_size("seq")
    whole_tiles = (
        in_step.shape[1] == 1
        and in_groups.shape[1] == STATE
        and count == 2 * GROUPS
        and hidden.shape[0] == SUB
        and (hidden.shape[1] // count) % LANES == 0
        and SUB % kv_cache.shape[0] == 0
        and kv_cache.shape[0] * QH <= LANES
        and kv_cache.shape[1] == LANES
    )
    return (fused_shards if whole_tiles else plain_shards)(*args)


def solution(mesh):
    placed = (
        P("grp", None),
        P(),
        P(None, "seq"),
        P(None, "seq"),
        P(None, "seq"),
        P("grp", None, "seq"),
        P("grp", None, "seq"),
        P(None, "seq"),
        P(None, "seq"),
        P("seq"),
        P("seq"),
        P("seq"),
        P("seq"),
        P("seq", None),
        P("grp", "seq", None, None),
        P("seq"),
        P("seq", None),
        P(None, "seq"),
        P(("grp", "seq"), None, None),
        P("grp", None),
        P("grp"),
    )
    return jax.shard_map(
        shards,
        mesh=mesh,
        in_specs=placed,
        out_specs=(P("grp", "seq"), P("grp", "seq", None, None), P("grp", None)),
        check_vma=False,
    )
```

```python
import functools

import jax
import jax.numpy as jnp
from jax import lax
from jax.experimental import pallas as pl
from jax.experimental.pallas import tpu as pltpu
from jax.sharding import PartitionSpec as P

QH = 32
KVH = 8
HD = 128
STATE = 128
GROUPS = 8
LANES = 128

epsilon = 1e-05
lowest = -1e30


def conv_step(state, fresh, taps):
    window = jnp.concatenate([state.astype(jnp.float32), fresh[:, None, :]], axis=1)
    summed = jnp.sum(window * taps[:-1][None], axis=1) + taps[-1][None]
    return jax.nn.silu(summed)


def split(value, parts):
    pieces = []
    rest = value
    for _ in range(parts):
        piece = lax.reduce_precision(rest, 8, 7)
        pieces.append(piece.astype(jnp.bfloat16))
        rest = rest - piece
    return pieces


def group_vectors(group_conv, heads_here, requests):
    count = lax.axis_size("seq")
    position = lax.axis_index("seq")
    if heads_here == 1 and group_conv.shape[1] == STATE and count == 2 * GROUPS:
        swap = [(i, (i + GROUPS) % count) for i in range(count)]
        other = lax.ppermute(group_conv, "seq", swap)
        first = position < GROUPS
        inject = jnp.where(first, group_conv, other)
        readout = jnp.where(first, other, group_conv)
        return (
            inject.astype(jnp.float32)[:, None, :],
            readout.astype(jnp.float32)[:, None, :],
        )
    group_all = lax.all_gather(group_conv, "seq", axis=1, tiled=True).astype(jnp.float32)
    inject = group_all[:, : GROUPS * STATE].reshape(requests, GROUPS, STATE)
    readout = group_all[:, GROUPS * STATE :].reshape(requests, GROUPS, STATE)
    head_ids = position * heads_here + jnp.arange(heads_here, dtype=jnp.int32)
    return inject[:, head_ids % GROUPS], readout[:, head_ids % GROUPS]


def plain_shards(
    hidden,
    mix_gain,
    in_gate_input,
    in_step,
    in_groups,
    conv_input,
    conv_groups,
    taps_input,
    taps_groups,
    decay_rate,
    step_bias,
    skip_gain,
    norm_gain,
    out_mixer,
    ssm_state,
    attn_gain,
    w_qkv,
    w_out,
    kv_cache,
    page_table,
    lengths,
):
    count_seq = lax.axis_size("seq")
    position = lax.axis_index("seq")
    requests = hidden.shape[0]
    width = hidden.shape[1]
    heads_here = in_step.shape[1]
    head_width = in_gate_input.shape[1] // (2 * heads_here)
    heads_total = heads_here * count_seq
    per_group = heads_total // GROUPS
    columns = width // count_seq
    stream = hidden.astype(jnp.float32)
    normed = (
        stream * lax.rsqrt(jnp.mean(stream * stream, axis=-1, keepdims=True) + epsilon) * mix_gain
    ).astype(jnp.bfloat16)
    group_raw = jnp.dot(normed, in_groups, preferred_element_type=jnp.float32)
    group_conv = conv_step(conv_groups, group_raw, taps_groups).astype(jnp.bfloat16)
    inject_heads, readout_heads = group_vectors(group_conv, heads_here, requests)
    gate_input = jnp.dot(normed, in_gate_input, preferred_element_type=jnp.float32).reshape(
        requests, heads_here, 2, head_width
    )
    gate_part = gate_input[:, :, 0]
    input_part = gate_input[:, :, 1].reshape(requests, heads_here * head_width)
    step_raw = jnp.dot(normed, in_step, preferred_element_type=jnp.float32)
    conv_out = conv_step(conv_input, input_part, taps_input).reshape(
        requests, heads_here, head_width
    )
    step_size = jax.nn.softplus(step_raw + step_bias)
    decay = jnp.exp(-decay_rate * step_size)
    new_state = (
        decay[:, :, None, None] * ssm_state
        + (step_size[:, :, None] * conv_out)[:, :, :, None] * inject_heads[:, :, None, :]
    )
    ssm_out = (
        jnp.sum(new_state * readout_heads[:, :, None, :], axis=-1)
        + skip_gain[None, :, None] * conv_out
    )
    gated = ssm_out * jax.nn.silu(gate_part)
    head_squares = jnp.sum(gated * gated, axis=-1)
    weighted = (gated * norm_gain.reshape(heads_here, head_width)).astype(jnp.bfloat16)
    products = jnp.einsum(
        "rhp,hpd->hrd",
        weighted,
        out_mixer.reshape(heads_here, head_width, width),
        preferred_element_type=jnp.float32,
    ).astype(jnp.bfloat16)
    products = products.reshape(heads_here, requests, count_seq, columns).transpose(2, 0, 1, 3)
    marks = jnp.stack(split(head_squares.T, 2), axis=-1)
    marks = jnp.pad(marks, ((0, 0), (0, 0), (0, LANES - 2)))
    marks = jnp.broadcast_to(marks[None], (count_seq,) + marks.shape)
    received = lax.all_to_all(jnp.concatenate([products, marks], axis=-1), "seq", 0, 0)
    received = received.astype(jnp.float32)
    squares = (received[..., columns] + received[..., columns + 1]).reshape(
        per_group, GROUPS, requests
    )
    scales = lax.rsqrt(jnp.sum(squares, axis=0) / (per_group * head_width) + epsilon)
    mixer = jnp.sum(
        received[..., :columns].reshape(per_group, GROUPS, requests, columns)
        * scales[None, :, :, None],
        axis=(0, 1),
    )
    stream_cols = lax.dynamic_slice_in_dim(stream, position * columns, columns, 1)
    middle = (stream_cols + mixer).astype(jnp.bfloat16)
    middle_f = middle.astype(jnp.float32)
    scaled = (middle_f * attn_gain).astype(jnp.bfloat16)
    partial_sq = jnp.sum(middle_f * middle_f, axis=-1)
    pages_here = kv_cache.shape[0]
    page_len = kv_cache.shape[1]
    pages_req = page_table.shape[1]
    pages_all = pages_here * count_seq
    matches = page_table[None, :, :] == jnp.arange(pages_all, dtype=jnp.int32)[:, None, None]
    owner = jnp.any(matches, axis=2)
    page_rows = jnp.dot(
        owner.astype(jnp.bfloat16), scaled, preferred_element_type=jnp.float32
    ).astype(jnp.bfloat16)
    page_proj = jnp.dot(page_rows, w_qkv, preferred_element_type=jnp.float32).astype(jnp.bfloat16)
    page_sq = jnp.sum(jnp.where(owner, partial_sq[None, :], 0.0), axis=1)
    sq_parts = jnp.pad(jnp.stack(split(page_sq, 2), axis=-1), ((0, 0), (0, LANES - 2)))
    sent = jnp.concatenate([page_proj, sq_parts], axis=-1).reshape(count_seq, pages_here, -1)
    arrived = jnp.sum(lax.all_to_all(sent, "seq", 0, 0).astype(jnp.float32), axis=0)
    qkv_width = w_qkv.shape[1]
    total_sq = arrived[:, qkv_width] + arrived[:, qkv_width + 1]
    qkv = (arrived[:, :qkv_width] * lax.rsqrt(total_sq / width + epsilon)[:, None]).astype(
        jnp.bfloat16
    )
    group_size = QH // KVH
    queries = qkv[:, : QH * HD].reshape(pages_here, KVH, group_size, HD)
    fresh_kv = qkv[:, QH * HD :]
    fresh_keys = fresh_kv[:, : KVH * HD].reshape(pages_here, KVH, 1, HD).astype(jnp.float32)
    fresh_values = fresh_kv[:, KVH * HD :].reshape(pages_here, KVH, 1, HD).astype(jnp.float32)
    scale = 1.0 / HD**0.5
    slots = position * pages_here + jnp.arange(pages_here, dtype=jnp.int32)
    own_matches = page_table[None, :, :] == slots[:, None, None]
    logical = jnp.sum(
        jnp.any(own_matches, axis=1) * jnp.arange(pages_req, dtype=jnp.int32)[None, :], axis=1
    )
    page_length = jnp.sum(jnp.where(jnp.any(own_matches, axis=2), lengths[None, :], 0), axis=1)
    token_pos = logical[:, None] * page_len + jnp.arange(page_len, dtype=jnp.int32)[None, :]
    live = (token_pos < page_length[:, None])[:, None, None, :]
    leads = (logical == 0)[:, None, None]
    cached = kv_cache.reshape(pages_here, page_len, 2, KVH, HD)
    scores = (
        jnp.einsum("pgjd,ptgd->pgjt", queries, cached[:, :, 0], preferred_element_type=jnp.float32)
        * scale
    )
    own = jnp.sum(queries.astype(jnp.float32) * fresh_keys, axis=-1) * scale
    masked = jnp.where(live, scores, lowest)
    own = jnp.where(leads, own, lowest)
    peak = jnp.maximum(jnp.max(masked, axis=-1), own)
    weights = jnp.where(live, jnp.exp(masked - peak[..., None]), 0.0)
    own_weight = jnp.where(leads, jnp.exp(own - peak), 0.0)
    total = jnp.sum(weights, axis=-1) + own_weight
    values = jnp.einsum(
        "pgjt,ptgd->pgjd",
        weights.astype(jnp.bfloat16),
        cached[:, :, 1],
        preferred_element_type=jnp.float32,
    )
    values = values + own_weight[..., None] * fresh_values
    some = total > 0.0
    safe = jnp.where(some, total, 1.0)
    values = (values / safe[..., None]).astype(jnp.bfloat16)
    logsum = jnp.where(some, peak + jnp.log(safe), lowest)
    logs = jnp.concatenate(split(logsum.reshape(1, pages_here * QH), 3), axis=0)
    logs = jnp.pad(logs, ((0, 5), (0, LANES - pages_here * QH)))
    value_rows = pages_here * QH
    kv_rows = pages_here * 2 * KVH
    package = jnp.concatenate(
        [values.reshape(value_rows, HD), fresh_kv.reshape(kv_rows, HD), logs], axis=0
    )
    package = jnp.broadcast_to(package[None], (count_seq,) + package.shape)
    everything = lax.all_to_all(package, "seq", 0, 0)
    all_values = everything[:, :value_rows].reshape(pages_all, QH, HD)
    all_kv = everything[:, value_rows : value_rows + kv_rows].reshape(pages_all, 2 * KVH * HD)
    all_logs = everything[:, value_rows + kv_rows :, : pages_here * QH].astype(jnp.float32)
    all_logs = (all_logs[:, 0] + all_logs[:, 1] + all_logs[:, 2]).reshape(pages_all, QH)
    new_kv = all_kv[page_table[:, 0]]
    req_logs = all_logs[page_table]
    top = jnp.max(req_logs, axis=1, keepdims=True)
    factors = jnp.exp(req_logs - top)
    summed = jnp.sum(factors[..., None] * all_values[page_table].astype(jnp.float32), axis=1)
    attended = (summed / jnp.sum(factors, axis=1)[..., None]).astype(jnp.bfloat16)
    final = (
        middle_f
        + jnp.dot(
            attended.reshape(requests, QH * HD), w_out, preferred_element_type=jnp.float32
        )
    ).astype(jnp.bfloat16)
    return (final, new_state, new_kv)


f32 = jnp.float32
bf16 = jnp.bfloat16
SUB = 8
PARTS = 3
SCOPED = 16 << 20
BLOCKS = 4
VMEM = pl.BlockSpec(memory_space=pltpu.VMEM)
NEAR = pl.BlockSpec(memory_space=pltpu.VMEM)
SMEM = pl.BlockSpec(memory_space=pltpu.SMEM)
FAR = pl.BlockSpec(memory_space=pltpu.HBM)


def call(kernel, outs, specs, scratch=()):
    grid_free = pl.pallas_call(
        kernel,
        out_shape=outs,
        in_specs=specs,
        out_specs=jax.tree.map(lambda _: VMEM, outs, is_leaf=lambda x: hasattr(x, "shape")),
        scratch_shapes=scratch,
        compiler_params=pltpu.CompilerParams(vmem_limit_bytes=SCOPED),
    )

    def run(*args):
        spaces = {id(NEAR): pltpu.VMEM, id(FAR): pltpu.HBM}
        placed = [
            pltpu.with_memory_space_constraint(arg, spaces[id(spec)]) if id(spec) in spaces else arg
            for arg, spec in zip(args, specs)
        ]
        return grid_free(*placed)

    return run


def shape(dims, kind):
    return jax.ShapeDtypeStruct(dims, kind)


def near(dims, kind):
    return pltpu.VMEM(dims, kind)


def silu(x):
    return x * jax.nn.sigmoid(x)


def pieces(value, parts):
    out = []
    for _ in range(parts):
        piece = value.astype(bf16).astype(f32)
        out.append(piece)
        value = value - piece
    return out


def marked(value, parts):
    lane = lax.broadcasted_iota(jnp.int32, (value.shape[0], LANES), 1)
    out = jnp.zeros((value.shape[0], LANES), f32)
    for k, piece in enumerate(pieces(value, parts)):
        out = jnp.where(lane == k, piece, out)
    return out


def convolve(state_ref, fresh, taps_ref):
    taps = state_ref.shape[0]
    total = taps_ref[taps : taps + 1, :] * fresh + taps_ref[taps + 1 : taps + 2, :]
    for k in range(taps):
        total = total + taps_ref[k : k + 1, :] * state_ref[k].astype(f32)
    return silu(total)


def fetch_all(pairs, sems):
    copies = [
        pltpu.make_async_copy(source, target, sems.at[k])
        for k, (source, target) in enumerate(pairs)
    ]
    for copy in copies:
        copy.start()
    return copies


def group_kernel(
    hidden_far,
    gain_far,
    weights_far,
    state_far,
    taps_far,
    group_out,
    normed_out,
    hidden,
    gain,
    weights,
    state,
    taps,
    sems,
):
    depth = weights.shape[0] // BLOCKS
    rows = [pl.ds(k * depth, depth) for k in range(BLOCKS)]
    copies = fetch_all(
        [(hidden_far, hidden), (gain_far, gain)]
        + [(weights_far.at[r], weights.at[r]) for r in rows]
        + [(state_far, state), (taps_far, taps)],
        sems,
    )
    copies[0].wait()
    copies[1].wait()
    stream = hidden[...].astype(f32)
    mean = jnp.mean(stream * stream, axis=-1, keepdims=True)
    normed_out[...] = (stream * lax.rsqrt(mean + epsilon) * gain[...]).astype(bf16)
    raw = jnp.zeros(group_out.shape, f32)
    for k in range(BLOCKS):
        copies[2 + k].wait()
        span = slice(k * depth, (k + 1) * depth)
        raw = raw + jnp.dot(normed_out[:, span], weights[span, :], preferred_element_type=f32)
    copies[-2].wait()
    copies[-1].wait()
    group_out[...] = convolve(state, raw, taps).astype(bf16)


def gate_kernel(carried, position, normed_ref, *refs):
    weights_far, step_far, state_far, taps_far, numbers, hidden_far = refs[:6]
    inputs, outputs, scratch = refs[6 : 6 + carried], refs[6 + carried : -5], refs[-5:]
    gate_out, conv_out, step_out, decay_out, columns_out = outputs[:5]
    weights, step_row, state, taps, sems = scratch
    columns = columns_out.shape[1]
    start = pl.multiple_of(position[0] * columns, columns)
    depth = weights.shape[0] // BLOCKS
    rows = [pl.ds(k * depth, depth) for k in range(BLOCKS)]
    copies = fetch_all(
        [(weights_far.at[r], weights.at[r]) for r in rows]
        + [
            (step_far, step_row),
            (state_far, state),
            (taps_far, taps),
            (hidden_far.at[:, pl.ds(start, columns)], columns_out),
        ]
        + list(zip(inputs, outputs[5:])),
        sems,
    )
    half = gate_out.shape[1]
    both = jnp.zeros((gate_out.shape[0], weights.shape[1]), f32)
    for k in range(BLOCKS):
        copies[k].wait()
        span = slice(k * depth, (k + 1) * depth)
        both = both + jnp.dot(normed_ref[:, span], weights[span, :], preferred_element_type=f32)
    for copy in copies[BLOCKS : BLOCKS + 3]:
        copy.wait()
    gate_out[...] = silu(both[:, :half])
    fresh = convolve(state, both[:, half:], taps)
    conv_out[:, :half] = fresh
    conv_out[:, half:] = numbers[2] * fresh
    raw = jnp.sum(normed_ref[...].astype(f32) * step_row[...].astype(f32), axis=-1, keepdims=True)
    step = jax.nn.softplus(raw + numbers[1])
    step_out[...] = jnp.broadcast_to(step, step_out.shape)
    decay_out[...] = jnp.broadcast_to(jnp.exp(-numbers[0] * step), decay_out.shape)
    for copy in copies[BLOCKS + 3 :]:
        copy.wait()


def chosen(position, own, other):
    first = position[0] < GROUPS
    mine, theirs = own[...].astype(f32), other[...].astype(f32)
    return jnp.where(first, mine, theirs), jnp.where(first, theirs, mine)


def mixer_kernel(position, own, other, gate, conv, step, decay, state, weights, gain, sent):
    requests = own.shape[0]
    inject, readout = chosen(position, own, other)
    half = gate.shape[1]
    row = lax.broadcasted_iota(jnp.int32, gate.shape, 0)
    read = jnp.zeros(gate.shape, f32)
    for r in range(requests):
        part = lax.dot_general(
            readout,
            state[r],
            (((1,), (1,)), ((), ())),
            precision=lax.Precision.HIGHEST,
            preferred_element_type=f32,
        )
        read = jnp.where(row == r, part, read)
    along = jnp.sum(inject * readout, axis=-1, keepdims=True)
    fresh = conv[:, :half]
    out = decay[:, :1] * read + step[:, :1] * fresh * along + conv[:, half:]
    gated = out * gate[...]
    marks = marked(jnp.sum(gated * gated, axis=-1, keepdims=True), 2).astype(bf16)
    weighted = (gated * gain[...]).astype(bf16)
    count = sent.shape[0]
    columns = weights.shape[1] // count
    for e in range(count):
        product = jnp.dot(
            weighted, weights[:, e * columns : (e + 1) * columns], preferred_element_type=f32
        )
        sent[e, :, :columns] = product.astype(bf16)
        sent[e, :, columns:] = marks


def state_kernel(position, own, other, conv, step, decay, state, new_state):
    inject, _ = chosen(position, own, other)
    fresh = step[:, :1] * conv[:, : state.shape[1]]
    new_state[...] = (
        decay[:, :1][:, :, None] * state[...] + fresh[:, :, None] * inject[:, None, :]
    )


def project_kernel(
    chunks, head_width, position, received, hidden, gain, weights, table, keep, give, middle_out
):
    count, requests, _ = received.shape
    columns = weights.shape[0]
    squares = [received[k, :, columns:].astype(f32) for k in range(count)]
    mixer = jnp.zeros((requests, columns), f32)
    for g in range(GROUPS):
        members = range(g, count, GROUPS)
        marks = sum(squares[k] for k in members)
        total = marks[:, :1] + marks[:, 1:2]
        scale = lax.rsqrt(total / (len(members) * head_width) + epsilon)
        products = sum(received[k, :, :columns].astype(f32) for k in members)
        mixer = mixer + scale * products
    middle = (hidden[...].astype(f32) + mixer).astype(bf16).astype(f32)
    middle_out[...] = middle
    marks = marked(jnp.sum(middle * middle, axis=-1, keepdims=True), 2)
    extended = jnp.concatenate([middle * gain[...], marks], axis=-1).astype(bf16)
    rows = count * SUB
    pages = SUB // chunks
    chips = count // 2
    core = position[0] % 2
    index = lax.broadcasted_iota(jnp.int32, (rows, requests), 0)
    line = index % (chips * SUB)
    parity = jnp.where(index < chips * SUB, core, 1 - core)
    page = ((line // SUB) * 2 + parity) * pages + index % pages
    hits = page == table[0:1, :]
    for j in range(1, table.shape[0]):
        hits = jnp.logical_or(hits, page == table[j : j + 1, :])
    onehot = jnp.where(hits, 1.0, 0.0).astype(bf16)
    spread = jnp.dot(onehot, extended, preferred_element_type=f32)
    lines = spread[:, :columns]
    which = (lax.broadcasted_iota(jnp.int32, lines.shape, 0) % SUB) // pages
    lhs = [jnp.where(which == c, lines, 0.0).astype(bf16) for c in range(chunks)]
    chunk = weights.shape[1] // chunks
    tile = 256
    for n in range(0, chunk, tile):
        total = None
        for c in range(chunks):
            part = jnp.dot(
                lhs[c],
                weights[:, c * chunk + n : c * chunk + n + tile],
                preferred_element_type=f32,
            )
            total = part if total is None else total + part
        for e in range(chips):
            keep[e, :, n : n + tile] = total[e * SUB : (e + 1) * SUB]
            first = (chips + e) * SUB
            give[e, :, n : n + tile] = total[first : first + SUB].astype(bf16)
    for e in range(chips):
        keep[e, :, chunk:] = spread[e * SUB : (e + 1) * SUB, columns:]
        first = (chips + e) * SUB
        give[e, :, chunk:] = spread[first : first + SUB, columns:].astype(bf16)


def pair_kernel(keep, taken, sent):
    chunk = keep.shape[2] - LANES
    for e in range(keep.shape[0]):
        total = keep[e] + taken[e].astype(f32)
        marks = total[:, chunk : chunk + 1] + total[:, chunk + 1 : chunk + 2]
        sent[e, :, :chunk] = total[:, :chunk].astype(bf16)
        sent[e, :, chunk:] = marked(marks, 2).astype(bf16)


def attend_kernel(width, position, received, cache, table, lengths, sent, lines):
    count, _, full = received.shape
    pages, page_len, _ = cache.shape
    chunks = SUB // pages
    chunk = full - LANES
    tiles = chunk // HD
    total = received[0].astype(f32)
    for k in range(1, count):
        total = total + received[k].astype(f32)
    squares = total[:, chunk : chunk + 1] + total[:, chunk + 1 : chunk + 2]
    inverse = lax.rsqrt(squares / width + epsilon)
    for t in range(tiles):
        lines[t * SUB : (t + 1) * SUB, :] = (
            (total[:, t * HD : (t + 1) * HD] * inverse).astype(bf16).astype(f32)
        )

    def heads(page, first, many):
        start = (first % tiles) * SUB + (first // tiles) * pages + page
        return lines[pl.ds(start, many, stride=SUB), :]

    group = QH // KVH
    scale = 1.0 / HD**0.5
    lane = lax.broadcasted_iota(jnp.int32, (1, page_len), 1)
    head_group = lax.broadcasted_iota(jnp.int32, (QH, HD), 0) // group
    eye = lax.broadcasted_iota(jnp.int32, (QH, LANES), 0)
    eye_lane = lax.broadcasted_iota(jnp.int32, (QH, LANES), 1)
    order = lax.broadcasted_iota(jnp.int32, table.shape, 0)
    value_rows = pages * QH
    fresh_rows = 2 * KVH
    log_row = jnp.zeros((1, LANES), f32)
    for p in range(pages):
        slot = position[0] * pages + p
        hit = table[...] == slot
        logical = jnp.sum(jnp.where(hit, order, 0), axis=(0, 1), keepdims=True)
        length = jnp.sum(
            jnp.where(hit, jnp.broadcast_to(lengths[...], hit.shape), 0),
            axis=(0, 1),
            keepdims=True,
        )
        live = logical * page_len + lane < length
        leads = logical == 0
        query = jnp.concatenate([heads(p, g * group, group) for g in range(KVH)], axis=0)
        keys = [heads(p, QH + g, 1) for g in range(KVH)]
        values = [heads(p, QH + KVH + g, 1) for g in range(KVH)]
        key_rows = jnp.concatenate([jnp.broadcast_to(k, (group, HD)) for k in keys], axis=0)
        value_own = jnp.concatenate([jnp.broadcast_to(v, (group, HD)) for v in values], axis=0)
        spread = jnp.concatenate(
            [jnp.where(head_group == g, query, 0.0).astype(bf16) for g in range(KVH)], axis=-1
        )
        scores = (
            lax.dot_general(
                spread,
                cache[p, :, : KVH * HD],
                (((1,), (1,)), ((), ())),
                preferred_element_type=f32,
            )
            * scale
        )
        own = jnp.sum(query * key_rows, axis=-1, keepdims=True) * scale
        masked = jnp.where(live, scores, lowest)
        own = jnp.where(leads, own, lowest)
        peak = jnp.maximum(jnp.max(masked, axis=-1, keepdims=True), own)
        weights = jnp.where(live, jnp.exp(masked - peak), 0.0)
        own_weight = jnp.where(leads, jnp.exp(own - peak), 0.0)
        mass = jnp.sum(weights, axis=-1, keepdims=True) + own_weight
        wide = jnp.dot(
            weights.astype(bf16), cache[p, :, KVH * HD :], preferred_element_type=f32
        )
        summed = own_weight * value_own
        for g in range(KVH):
            summed = summed + jnp.where(head_group == g, wide[:, g * HD : (g + 1) * HD], 0.0)
        some = mass > 0.0
        safe = jnp.where(some, mass, 1.0)
        result = (summed / safe).astype(bf16)
        logs = jnp.where(some, peak + jnp.log(safe), lowest)
        log_row = log_row + jnp.sum(
            jnp.where(eye_lane == eye + p * QH, logs, 0.0), axis=0, keepdims=True
        )
        fresh = jnp.concatenate(keys + values, axis=0).astype(bf16)
        for e in range(count):
            sent[e, p * QH : (p + 1) * QH, :] = result
            first = value_rows + p * fresh_rows
            sent[e, first : first + fresh_rows, :] = fresh
    terms = pieces(log_row, PARTS) + [jnp.zeros((SUB - PARTS, LANES), f32)]
    terms = jnp.concatenate(terms, axis=0).astype(bf16)
    for e in range(count):
        sent[e, value_rows + pages * fresh_rows :, :] = terms


def merge_kernel(
    pages, position, table, near, far, weights, middle, final, new_kv, spread, rows, fresh
):
    chips, package, _ = near.shape
    pages_req, requests = table.shape
    value_rows = pages * QH
    kv_rows = 2 * KVH
    last = value_rows + pages * kv_rows
    source = lax.broadcasted_iota(jnp.int32, (chips * SUB, LANES), 0) // SUB
    masks = [jnp.where(source == k, 1.0, 0.0).astype(bf16) for k in range(chips)]
    for side, packages in enumerate((near, far)):
        logs = jnp.concatenate([packages[k, last:, :] for k in range(chips)], axis=0)
        for k in range(chips):
            spread[side * chips + k] = lax.dot_general(
                logs, masks[k], (((0,), (0,)), ((), ())), preferred_element_type=f32
            )
    core = position[0] % 2

    def fetch(chip, side, first, many):
        both = near[chip, pl.ds(first, many), :], far[chip, pl.ds(first, many), :]
        return jnp.where(side == 0, both[0].astype(f32), both[1].astype(f32))

    for r in range(requests):
        peaks, values = [], []
        for j in range(pages_req):
            page = table[j, r]
            device, slot = page // pages, page % pages
            chip = device // 2
            side = lax.rem(device + core, 2)
            first = pl.multiple_of(slot * QH, QH)
            peaks.append(spread[side * chips + chip, pl.ds(first, QH), :])
            values.append(fetch(chip, side, first, QH))
            if j == 0:
                first = pl.multiple_of(value_rows + slot * kv_rows, kv_rows)
                fresh[r * kv_rows : (r + 1) * kv_rows, :] = fetch(chip, side, first, kv_rows)
        top = functools.reduce(jnp.maximum, peaks)
        mass = jnp.zeros(top.shape, f32)
        summed = jnp.zeros(top.shape, f32)
        for peak, value in zip(peaks, values):
            factor = jnp.exp(peak - top)
            mass = mass + factor
            summed = summed + factor * value
        rows[r * QH : (r + 1) * QH, :] = summed / mass
    for c in range(kv_rows):
        new_kv[:, c * HD : (c + 1) * HD] = fresh[pl.ds(c, requests, stride=kv_rows), :].astype(
            bf16
        )
    attended = jnp.concatenate(
        [rows[pl.ds(h, requests, stride=QH), :].astype(bf16) for h in range(QH)], axis=-1
    )
    total = jnp.dot(attended, weights[...], preferred_element_type=f32)
    final[...] = (middle[...] + total).astype(bf16)


def fused_shards(
    hidden,
    mix_gain,
    in_gate_input,
    in_step,
    in_groups,
    conv_input,
    conv_groups,
    taps_input,
    taps_groups,
    decay_rate,
    step_bias,
    skip_gain,
    norm_gain,
    out_mixer,
    ssm_state,
    attn_gain,
    w_qkv,
    w_out,
    kv_cache,
    page_table,
    lengths,
):
    count = lax.axis_size("seq")
    position = lax.axis_index("seq").astype(jnp.int32).reshape(1)
    requests, width = hidden.shape
    columns = width // count
    head_width = in_gate_input.shape[1] // 2
    pages = kv_cache.shape[0]
    chunks = SUB // pages
    chips = count // 2
    gcols = in_groups.shape[1]
    state = ssm_state.reshape(requests, head_width, STATE)
    same_core = [list(range(core, count, 2)) for core in range(2)]
    cores = [(i, i ^ 1) for i in range(count)]
    group_args = (
        hidden,
        mix_gain.reshape(1, width),
        in_groups,
        conv_groups.transpose(1, 0, 2),
        taps_groups,
    )
    group_conv, normed = call(
        group_kernel,
        (near((requests, gcols), bf16), near((requests, width), bf16)),
        [FAR] * 5,
        [pltpu.VMEM(x.shape, x.dtype) for x in group_args]
        + [pltpu.SemaphoreType.DMA((len(group_args) - 1 + BLOCKS,))],
    )(*group_args)
    swap = [(i, (i + GROUPS) % count) for i in range(count)]
    other = lax.ppermute(group_conv, "seq", swap)
    carried = (
        state,
        out_mixer,
        norm_gain.reshape(1, head_width),
        attn_gain.reshape(1, columns),
        page_table.T,
        lengths.reshape(1, requests),
    )
    gate_args = (
        in_gate_input,
        in_step.T,
        conv_input.transpose(1, 0, 2),
        taps_input,
    )
    numbers = jnp.concatenate([decay_rate, step_bias, skip_gain])
    gate, conv, step, decay, stream, state_in, mixer, gain, scale, table, spans = call(
        functools.partial(gate_kernel, len(carried)),
        (
            near((requests, head_width), f32),
            near((requests, 2 * head_width), f32),
            near((requests, LANES), f32),
            near((requests, LANES), f32),
            near((requests, columns), bf16),
        )
        + tuple(near(x.shape, x.dtype) for x in carried),
        [SMEM, NEAR] + [FAR] * 4 + [SMEM] + [FAR] * (1 + len(carried)),
        [pltpu.VMEM(x.shape, x.dtype) for x in gate_args]
        + [pltpu.SemaphoreType.DMA((BLOCKS + 4 + len(carried),))],
    )(position, normed, *gate_args, numbers, hidden, *carried)
    sent = call(
        mixer_kernel,
        near((count, requests, columns + LANES), bf16),
        [SMEM] + [NEAR] * 9,
    )(position, group_conv, other, gate, conv, step, decay, state_in, mixer, gain)
    received = lax.all_to_all(sent, "seq", 0, 0)
    new_state = call(state_kernel, shape(state.shape, f32), [SMEM] + [NEAR] * 6)(
        position, group_conv, other, conv, step, decay, state_in
    )
    chunk = w_qkv.shape[1] // chunks
    keep, give, middle = call(
        functools.partial(project_kernel, chunks, head_width),
        (
            near((chips, SUB, chunk + LANES), f32),
            near((chips, SUB, chunk + LANES), bf16),
            near((requests, columns), f32),
        ),
        [SMEM] + [NEAR] * 5,
    )(position, received, stream, scale, w_qkv, table)
    taken = lax.ppermute(give, "seq", cores)
    sent = call(pair_kernel, near(give.shape, bf16), [NEAR] * 2)(keep, taken)
    received = lax.all_to_all(sent, "seq", 0, 0, axis_index_groups=same_core)
    package = pages * (QH + 2 * KVH) + SUB
    sent = call(
        functools.partial(attend_kernel, width),
        near((chips, package, HD), bf16),
        [SMEM] + [NEAR] * 4,
        [pltpu.VMEM((chunk // HD * SUB, HD), f32)],
    )(position, received, kv_cache, table, spans)
    received = lax.all_to_all(sent, "seq", 0, 0, axis_index_groups=same_core)
    far = lax.ppermute(received, "seq", cores)
    final, new_kv = call(
        functools.partial(merge_kernel, pages),
        (
            shape((requests, columns), bf16),
            shape((requests, 2 * KVH * HD), bf16),
        ),
        [SMEM] * 2 + [NEAR] * 4,
        [
            pltpu.VMEM((count, LANES, LANES), f32),
            pltpu.VMEM((requests * QH, HD), f32),
            pltpu.VMEM((requests * 2 * KVH, HD), f32),
        ],
    )(position, page_table.T, received, far, w_out, middle)
    return (final, new_state.reshape(ssm_state.shape), new_kv)


def shards(*args):
    hidden, in_step, in_groups = args[0], args[3], args[4]
    kv_cache, page_table = args[18], args[19]
    count = lax.axis_size("seq")
    whole_tiles = (
        in_step.shape[1] == 1
        and in_groups.shape[1] == STATE
        and count == 2 * GROUPS
        and hidden.shape[0] == SUB
        and (hidden.shape[1] // count) % LANES == 0
        and SUB % kv_cache.shape[0] == 0
        and kv_cache.shape[0] * QH <= LANES
        and kv_cache.shape[1] == LANES
    )
    return (fused_shards if whole_tiles else plain_shards)(*args)


def solution(mesh):
    placed = (
        P("grp", None),
        P(),
        P(None, "seq"),
        P(None, "seq"),
        P(None, "seq"),
        P("grp", None, "seq"),
        P("grp", None, "seq"),
        P(None, "seq"),
        P(None, "seq"),
        P("seq"),
        P("seq"),
        P("seq"),
        P("seq"),
        P("seq", None),
        P("grp", "seq", None, None),
        P("seq"),
        P("seq", None),
        P(None, "seq"),
        P(("grp", "seq"), None, None),
        P("grp", None),
        P("grp"),
    )
    return jax.shard_map(
        shards,
        mesh=mesh,
        in_specs=placed,
        out_specs=(P("grp", "seq"), P("grp", "seq", None, None), P("grp", None)),
        check_vma=False,
    )
```

```python
import functools

import jax
import jax.numpy as jnp
from jax import lax
from jax.experimental import pallas as pl
from jax.experimental.pallas import tpu as pltpu
from jax.sharding import PartitionSpec as P

QH = 32
KVH = 8
HD = 128
STATE = 128
GROUPS = 8
LANES = 128

epsilon = 1e-05
lowest = -1e30


def conv_step(state, fresh, taps):
    window = jnp.concatenate([state.astype(jnp.float32), fresh[:, None, :]], axis=1)
    summed = jnp.sum(window * taps[:-1][None], axis=1) + taps[-1][None]
    return jax.nn.silu(summed)


def split(value, parts):
    pieces = []
    rest = value
    for _ in range(parts):
        piece = lax.reduce_precision(rest, 8, 7)
        pieces.append(piece.astype(jnp.bfloat16))
        rest = rest - piece
    return pieces


def group_vectors(group_conv, heads_here, requests):
    count = lax.axis_size("seq")
    position = lax.axis_index("seq")
    if heads_here == 1 and group_conv.shape[1] == STATE and count == 2 * GROUPS:
        swap = [(i, (i + GROUPS) % count) for i in range(count)]
        other = lax.ppermute(group_conv, "seq", swap)
        first = position < GROUPS
        inject = jnp.where(first, group_conv, other)
        readout = jnp.where(first, other, group_conv)
        return (
            inject.astype(jnp.float32)[:, None, :],
            readout.astype(jnp.float32)[:, None, :],
        )
    group_all = lax.all_gather(group_conv, "seq", axis=1, tiled=True).astype(jnp.float32)
    inject = group_all[:, : GROUPS * STATE].reshape(requests, GROUPS, STATE)
    readout = group_all[:, GROUPS * STATE :].reshape(requests, GROUPS, STATE)
    head_ids = position * heads_here + jnp.arange(heads_here, dtype=jnp.int32)
    return inject[:, head_ids % GROUPS], readout[:, head_ids % GROUPS]


def plain_shards(
    hidden,
    mix_gain,
    in_gate_input,
    in_step,
    in_groups,
    conv_input,
    conv_groups,
    taps_input,
    taps_groups,
    decay_rate,
    step_bias,
    skip_gain,
    norm_gain,
    out_mixer,
    ssm_state,
    attn_gain,
    w_qkv,
    w_out,
    kv_cache,
    page_table,
    lengths,
):
    count_seq = lax.axis_size("seq")
    position = lax.axis_index("seq")
    requests = hidden.shape[0]
    width = hidden.shape[1]
    heads_here = in_step.shape[1]
    head_width = in_gate_input.shape[1] // (2 * heads_here)
    heads_total = heads_here * count_seq
    per_group = heads_total // GROUPS
    columns = width // count_seq
    stream = hidden.astype(jnp.float32)
    normed = (
        stream * lax.rsqrt(jnp.mean(stream * stream, axis=-1, keepdims=True) + epsilon) * mix_gain
    ).astype(jnp.bfloat16)
    group_raw = jnp.dot(normed, in_groups, preferred_element_type=jnp.float32)
    group_conv = conv_step(conv_groups, group_raw, taps_groups).astype(jnp.bfloat16)
    inject_heads, readout_heads = group_vectors(group_conv, heads_here, requests)
    gate_input = jnp.dot(normed, in_gate_input, preferred_element_type=jnp.float32).reshape(
        requests, heads_here, 2, head_width
    )
    gate_part = gate_input[:, :, 0]
    input_part = gate_input[:, :, 1].reshape(requests, heads_here * head_width)
    step_raw = jnp.dot(normed, in_step, preferred_element_type=jnp.float32)
    conv_out = conv_step(conv_input, input_part, taps_input).reshape(
        requests, heads_here, head_width
    )
    step_size = jax.nn.softplus(step_raw + step_bias)
    decay = jnp.exp(-decay_rate * step_size)
    new_state = (
        decay[:, :, None, None] * ssm_state
        + (step_size[:, :, None] * conv_out)[:, :, :, None] * inject_heads[:, :, None, :]
    )
    ssm_out = (
        jnp.sum(new_state * readout_heads[:, :, None, :], axis=-1)
        + skip_gain[None, :, None] * conv_out
    )
    gated = ssm_out * jax.nn.silu(gate_part)
    head_squares = jnp.sum(gated * gated, axis=-1)
    weighted = (gated * norm_gain.reshape(heads_here, head_width)).astype(jnp.bfloat16)
    products = jnp.einsum(
        "rhp,hpd->hrd",
        weighted,
        out_mixer.reshape(heads_here, head_width, width),
        preferred_element_type=jnp.float32,
    ).astype(jnp.bfloat16)
    products = products.reshape(heads_here, requests, count_seq, columns).transpose(2, 0, 1, 3)
    marks = jnp.stack(split(head_squares.T, 2), axis=-1)
    marks = jnp.pad(marks, ((0, 0), (0, 0), (0, LANES - 2)))
    marks = jnp.broadcast_to(marks[None], (count_seq,) + marks.shape)
    received = lax.all_to_all(jnp.concatenate([products, marks], axis=-1), "seq", 0, 0)
    received = received.astype(jnp.float32)
    squares = (received[..., columns] + received[..., columns + 1]).reshape(
        per_group, GROUPS, requests
    )
    scales = lax.rsqrt(jnp.sum(squares, axis=0) / (per_group * head_width) + epsilon)
    mixer = jnp.sum(
        received[..., :columns].reshape(per_group, GROUPS, requests, columns)
        * scales[None, :, :, None],
        axis=(0, 1),
    )
    stream_cols = lax.dynamic_slice_in_dim(stream, position * columns, columns, 1)
    middle = (stream_cols + mixer).astype(jnp.bfloat16)
    middle_f = middle.astype(jnp.float32)
    scaled = (middle_f * attn_gain).astype(jnp.bfloat16)
    partial_sq = jnp.sum(middle_f * middle_f, axis=-1)
    pages_here = kv_cache.shape[0]
    page_len = kv_cache.shape[1]
    pages_req = page_table.shape[1]
    pages_all = pages_here * count_seq
    matches = page_table[None, :, :] == jnp.arange(pages_all, dtype=jnp.int32)[:, None, None]
    owner = jnp.any(matches, axis=2)
    page_rows = jnp.dot(
        owner.astype(jnp.bfloat16), scaled, preferred_element_type=jnp.float32
    ).astype(jnp.bfloat16)
    page_proj = jnp.dot(page_rows, w_qkv, preferred_element_type=jnp.float32).astype(jnp.bfloat16)
    page_sq = jnp.sum(jnp.where(owner, partial_sq[None, :], 0.0), axis=1)
    sq_parts = jnp.pad(jnp.stack(split(page_sq, 2), axis=-1), ((0, 0), (0, LANES - 2)))
    sent = jnp.concatenate([page_proj, sq_parts], axis=-1).reshape(count_seq, pages_here, -1)
    arrived = jnp.sum(lax.all_to_all(sent, "seq", 0, 0).astype(jnp.float32), axis=0)
    qkv_width = w_qkv.shape[1]
    total_sq = arrived[:, qkv_width] + arrived[:, qkv_width + 1]
    qkv = (arrived[:, :qkv_width] * lax.rsqrt(total_sq / width + epsilon)[:, None]).astype(
        jnp.bfloat16
    )
    group_size = QH // KVH
    queries = qkv[:, : QH * HD].reshape(pages_here, KVH, group_size, HD)
    fresh_kv = qkv[:, QH * HD :]
    fresh_keys = fresh_kv[:, : KVH * HD].reshape(pages_here, KVH, 1, HD).astype(jnp.float32)
    fresh_values = fresh_kv[:, KVH * HD :].reshape(pages_here, KVH, 1, HD).astype(jnp.float32)
    scale = 1.0 / HD**0.5
    slots = position * pages_here + jnp.arange(pages_here, dtype=jnp.int32)
    own_matches = page_table[None, :, :] == slots[:, None, None]
    logical = jnp.sum(
        jnp.any(own_matches, axis=1) * jnp.arange(pages_req, dtype=jnp.int32)[None, :], axis=1
    )
    page_length = jnp.sum(jnp.where(jnp.any(own_matches, axis=2), lengths[None, :], 0), axis=1)
    token_pos = logical[:, None] * page_len + jnp.arange(page_len, dtype=jnp.int32)[None, :]
    live = (token_pos < page_length[:, None])[:, None, None, :]
    leads = (logical == 0)[:, None, None]
    cached = kv_cache.reshape(pages_here, page_len, 2, KVH, HD)
    scores = (
        jnp.einsum("pgjd,ptgd->pgjt", queries, cached[:, :, 0], preferred_element_type=jnp.float32)
        * scale
    )
    own = jnp.sum(queries.astype(jnp.float32) * fresh_keys, axis=-1) * scale
    masked = jnp.where(live, scores, lowest)
    own = jnp.where(leads, own, lowest)
    peak = jnp.maximum(jnp.max(masked, axis=-1), own)
    weights = jnp.where(live, jnp.exp(masked - peak[..., None]), 0.0)
    own_weight = jnp.where(leads, jnp.exp(own - peak), 0.0)
    total = jnp.sum(weights, axis=-1) + own_weight
    values = jnp.einsum(
        "pgjt,ptgd->pgjd",
        weights.astype(jnp.bfloat16),
        cached[:, :, 1],
        preferred_element_type=jnp.float32,
    )
    values = values + own_weight[..., None] * fresh_values
    some = total > 0.0
    safe = jnp.where(some, total, 1.0)
    values = (values / safe[..., None]).astype(jnp.bfloat16)
    logsum = jnp.where(some, peak + jnp.log(safe), lowest)
    logs = jnp.concatenate(split(logsum.reshape(1, pages_here * QH), 3), axis=0)
    logs = jnp.pad(logs, ((0, 5), (0, LANES - pages_here * QH)))
    value_rows = pages_here * QH
    kv_rows = pages_here * 2 * KVH
    package = jnp.concatenate(
        [values.reshape(value_rows, HD), fresh_kv.reshape(kv_rows, HD), logs], axis=0
    )
    package = jnp.broadcast_to(package[None], (count_seq,) + package.shape)
    everything = lax.all_to_all(package, "seq", 0, 0)
    all_values = everything[:, :value_rows].reshape(pages_all, QH, HD)
    all_kv = everything[:, value_rows : value_rows + kv_rows].reshape(pages_all, 2 * KVH * HD)
    all_logs = everything[:, value_rows + kv_rows :, : pages_here * QH].astype(jnp.float32)
    all_logs = (all_logs[:, 0] + all_logs[:, 1] + all_logs[:, 2]).reshape(pages_all, QH)
    new_kv = all_kv[page_table[:, 0]]
    req_logs = all_logs[page_table]
    top = jnp.max(req_logs, axis=1, keepdims=True)
    factors = jnp.exp(req_logs - top)
    summed = jnp.sum(factors[..., None] * all_values[page_table].astype(jnp.float32), axis=1)
    attended = (summed / jnp.sum(factors, axis=1)[..., None]).astype(jnp.bfloat16)
    final = (
        middle_f
        + jnp.dot(
            attended.reshape(requests, QH * HD), w_out, preferred_element_type=jnp.float32
        )
    ).astype(jnp.bfloat16)
    return (final, new_state, new_kv)


f32 = jnp.float32
bf16 = jnp.bfloat16
SUB = 8
PARTS = 3
SCOPED = 16 << 20
MOST = 63500 << 10
BLOCKS = 4
VMEM = pl.BlockSpec(memory_space=pltpu.VMEM)
NEAR = pl.BlockSpec(memory_space=pltpu.VMEM)
SMEM = pl.BlockSpec(memory_space=pltpu.SMEM)
FAR = pl.BlockSpec(memory_space=pltpu.HBM)


def call(kernel, outs, specs, scratch=(), scoped=SCOPED):
    grid_free = pl.pallas_call(
        kernel,
        out_shape=outs,
        in_specs=specs,
        out_specs=jax.tree.map(lambda _: VMEM, outs, is_leaf=lambda x: hasattr(x, "shape")),
        scratch_shapes=scratch,
        compiler_params=pltpu.CompilerParams(vmem_limit_bytes=scoped),
    )

    def run(*args):
        spaces = {id(NEAR): pltpu.VMEM, id(FAR): pltpu.HBM}
        placed = [
            pltpu.with_memory_space_constraint(arg, spaces[id(spec)]) if id(spec) in spaces else arg
            for arg, spec in zip(args, specs)
        ]
        return grid_free(*placed)

    return run


def shape(dims, kind):
    return jax.ShapeDtypeStruct(dims, kind)


def near(dims, kind):
    return pltpu.VMEM(dims, kind)


def silu(x):
    return x * jax.nn.sigmoid(x)


def pieces(value, parts):
    out = []
    for _ in range(parts):
        piece = value.astype(bf16).astype(f32)
        out.append(piece)
        value = value - piece
    return out


def marked(value, parts, first=0):
    lane = lax.broadcasted_iota(jnp.int32, (value.shape[0], LANES), 1)
    out = jnp.zeros((value.shape[0], LANES), f32)
    for k, piece in enumerate(pieces(value, parts)):
        out = jnp.where(lane == first + k, piece, out)
    return out


def summed(marks, first=0):
    return marks[:, first : first + 1] + marks[:, first + 1 : first + 2]


def convolve(state_ref, fresh, taps_ref):
    taps = state_ref.shape[0]
    total = taps_ref[taps : taps + 1, :] * fresh + taps_ref[taps + 1 : taps + 2, :]
    for k in range(taps):
        total = total + taps_ref[k : k + 1, :] * state_ref[k].astype(f32)
    return silu(total)


def fetch_all(pairs, sems):
    copies = [
        pltpu.make_async_copy(source, target, sems.at[k])
        for k, (source, target) in enumerate(pairs)
    ]
    for copy in copies:
        copy.start()
    return copies


def group_kernel(
    hidden_far,
    gain_far,
    weights_far,
    state_far,
    taps_far,
    group_out,
    normed_out,
    hidden,
    gain,
    weights,
    state,
    taps,
    sems,
):
    depth = weights.shape[0] // BLOCKS
    rows = [pl.ds(k * depth, depth) for k in range(BLOCKS)]
    copies = fetch_all(
        [(hidden_far, hidden), (gain_far, gain)]
        + [(weights_far.at[r], weights.at[r]) for r in rows]
        + [(state_far, state), (taps_far, taps)],
        sems,
    )
    copies[0].wait()
    copies[1].wait()
    stream = hidden[...].astype(f32)
    mean = jnp.mean(stream * stream, axis=-1, keepdims=True)
    normed_out[...] = (stream * lax.rsqrt(mean + epsilon) * gain[...]).astype(bf16)
    raw = jnp.zeros(group_out.shape, f32)
    for k in range(BLOCKS):
        copies[2 + k].wait()
        span = slice(k * depth, (k + 1) * depth)
        raw = raw + jnp.dot(normed_out[:, span], weights[span, :], preferred_element_type=f32)
    copies[-2].wait()
    copies[-1].wait()
    group_out[...] = convolve(state, raw, taps).astype(bf16)


def gate_kernel(carried, position, normed_ref, *refs):
    weights_far, step_far, state_far, taps_far, numbers, hidden_far = refs[:6]
    inputs, outputs, scratch = refs[6 : 6 + carried], refs[6 + carried : -5], refs[-5:]
    gate_out, conv_out, step_out, decay_out, columns_out = outputs[:5]
    weights, step_row, state, taps, sems = scratch
    columns = columns_out.shape[1]
    start = pl.multiple_of(position[0] * columns, columns)
    depth = weights.shape[0] // BLOCKS
    rows = [pl.ds(k * depth, depth) for k in range(BLOCKS)]
    copies = fetch_all(
        [(weights_far.at[r], weights.at[r]) for r in rows]
        + [
            (step_far, step_row),
            (state_far, state),
            (taps_far, taps),
            (hidden_far.at[:, pl.ds(start, columns)], columns_out),
        ]
        + list(zip(inputs, outputs[5:])),
        sems,
    )
    half = gate_out.shape[1]
    both = jnp.zeros((gate_out.shape[0], weights.shape[1]), f32)
    for k in range(BLOCKS):
        copies[k].wait()
        span = slice(k * depth, (k + 1) * depth)
        both = both + jnp.dot(normed_ref[:, span], weights[span, :], preferred_element_type=f32)
    for copy in copies[BLOCKS : BLOCKS + 3]:
        copy.wait()
    gate_out[...] = silu(both[:, :half])
    fresh = convolve(state, both[:, half:], taps)
    conv_out[:, :half] = fresh
    conv_out[:, half:] = numbers[2] * fresh
    raw = jnp.sum(normed_ref[...].astype(f32) * step_row[...].astype(f32), axis=-1, keepdims=True)
    step = jax.nn.softplus(raw + numbers[1])
    step_out[...] = jnp.broadcast_to(step, step_out.shape)
    decay_out[...] = jnp.broadcast_to(jnp.exp(-numbers[0] * step), decay_out.shape)
    for copy in copies[BLOCKS + 3 :]:
        copy.wait()


def chosen(position, own, other):
    first = position[0] < GROUPS
    mine, theirs = own[...].astype(f32), other[...].astype(f32)
    return jnp.where(first, mine, theirs), jnp.where(first, theirs, mine)


def mixer_kernel(position, own, other, gate, conv, step, decay, state, weights, gain, sent):
    requests = own.shape[0]
    inject, readout = chosen(position, own, other)
    half = gate.shape[1]
    row = lax.broadcasted_iota(jnp.int32, gate.shape, 0)
    read = jnp.zeros(gate.shape, f32)
    for r in range(requests):
        part = lax.dot_general(
            readout,
            state[r],
            (((1,), (1,)), ((), ())),
            precision=lax.Precision.HIGHEST,
            preferred_element_type=f32,
        )
        read = jnp.where(row == r, part, read)
    along = jnp.sum(inject * readout, axis=-1, keepdims=True)
    fresh = conv[:, :half]
    out = decay[:, :1] * read + step[:, :1] * fresh * along + conv[:, half:]
    gated = out * gate[...]
    marks = marked(jnp.sum(gated * gated, axis=-1, keepdims=True), 2).astype(bf16)
    weighted = (gated * gain[...]).astype(bf16)
    count = sent.shape[0]
    columns = weights.shape[1] // count
    for e in range(count):
        product = jnp.dot(
            weighted, weights[:, e * columns : (e + 1) * columns], preferred_element_type=f32
        )
        sent[e, :, :columns] = product.astype(bf16)
        sent[e, :, columns:] = marks


def state_kernel(position, own, other, conv, step, decay, state, new_state):
    inject, _ = chosen(position, own, other)
    fresh = step[:, :1] * conv[:, : state.shape[1]]
    new_state[...] = (
        decay[:, :1][:, :, None] * state[...] + fresh[:, :, None] * inject[:, None, :]
    )


def project_kernel(
    chunks, head_width, position, received, hidden, gain, weights, table, keep, give, middle_out
):
    count, requests, _ = received.shape
    columns = weights.shape[0]
    squares = [received[k, :, columns:].astype(f32) for k in range(count)]
    mixer = jnp.zeros((requests, columns), f32)
    for g in range(GROUPS):
        members = range(g, count, GROUPS)
        marks = sum(squares[k] for k in members)
        total = marks[:, :1] + marks[:, 1:2]
        scale = lax.rsqrt(total / (len(members) * head_width) + epsilon)
        products = sum(received[k, :, :columns].astype(f32) for k in members)
        mixer = mixer + scale * products
    middle = (hidden[...].astype(f32) + mixer).astype(bf16).astype(f32)
    middle_out[...] = middle
    square = jnp.sum(middle * middle, axis=-1, keepdims=True)
    scaled = middle * gain[...]
    extended = jnp.concatenate([scaled, marked(square, 2)], axis=-1).astype(bf16)
    rows = count * SUB
    pages = SUB // chunks
    chips = count // 2
    core = position[0] % 2
    index = lax.broadcasted_iota(jnp.int32, (rows, requests), 0)
    line = index % (chips * SUB)
    parity = jnp.where(index < chips * SUB, core, 1 - core)
    page = ((line // SUB) * 2 + parity) * pages + index % pages
    hits = page == table[0:1, :]
    for j in range(1, table.shape[0]):
        hits = jnp.logical_or(hits, page == table[j : j + 1, :])
    onehot = jnp.where(hits, 1.0, 0.0).astype(bf16)
    spread = jnp.dot(onehot, extended, preferred_element_type=f32)
    lines = spread[:, :columns]
    which = (lax.broadcasted_iota(jnp.int32, lines.shape, 0) % SUB) // pages
    chunk = weights.shape[1] // chunks
    fresh_from = QH * HD
    zeros = jnp.zeros((SUB, columns), f32)
    lhs = []
    for c in range(chunks):
        own = jnp.where(which == c, lines, 0.0)
        if (c + 1) * chunk > fresh_from:
            own = jnp.concatenate([own, scaled, zeros], axis=0)
        lhs.append(own.astype(bf16))
    tile = 2 * HD
    for n in range(0, chunk, tile):
        total = None
        for c in range(chunks):
            first = c * chunk + n
            part = jnp.dot(lhs[c], weights[:, first : first + tile], preferred_element_type=f32)
            if first >= fresh_from:
                fresh = part[rows : rows + SUB]
                chip = (first - fresh_from) // tile
                low, high = fresh[:, :HD], fresh[:, HD:]
                keep[chip, :, chunk + LANES :] = jnp.where(core == 0, low, high)
                give[chip, :, chunk + LANES :] = jnp.where(core == 0, high, low).astype(bf16)
            total = part[:rows] if total is None else total + part[:rows]
        for e in range(chips):
            keep[e, :, n : n + tile] = total[e * SUB : (e + 1) * SUB]
            first = (chips + e) * SUB
            give[e, :, n : n + tile] = total[first : first + SUB].astype(bf16)
    marks = spread[:, columns:]
    request_marks = marked(square, 2, 2)
    for e in range(chips):
        keep[e, :, chunk : chunk + LANES] = marks[e * SUB : (e + 1) * SUB] + request_marks
        first = (chips + e) * SUB
        give[e, :, chunk : chunk + LANES] = (marks[first : first + SUB] + request_marks).astype(
            bf16
        )


def pair_kernel(keep, taken, _, sent):
    chunk = keep.shape[2] - 2 * LANES
    for e in range(keep.shape[0]):
        total = keep[e] + taken[e].astype(f32)
        marks = total[:, chunk : chunk + LANES]
        sent[e, :, :chunk] = total[:, :chunk].astype(bf16)
        sent[e, :, chunk : chunk + LANES] = (
            marked(summed(marks), 2) + marked(summed(marks, 2), 2, 2)
        ).astype(bf16)
        sent[e, :, chunk + LANES :] = total[:, chunk + LANES :].astype(bf16)


def attend_kernel(width, position, received, cache, table, lengths, sent, lines):
    count, _, full = received.shape
    pages, page_len, _ = cache.shape
    chunks = SUB // pages
    chunk = full - 2 * LANES
    tiles = chunk // HD
    total = received[0].astype(f32)
    for k in range(1, count):
        total = total + received[k].astype(f32)
    marks = total[:, chunk : chunk + LANES]
    inverse = lax.rsqrt(summed(marks) / width + epsilon)
    fresh = total[:, chunk + LANES :] * lax.rsqrt(summed(marks, 2) / width + epsilon)
    fresh = fresh.astype(bf16)
    for t in range(tiles):
        lines[t * SUB : (t + 1) * SUB, :] = (
            (total[:, t * HD : (t + 1) * HD] * inverse).astype(bf16).astype(f32)
        )

    def heads(page, first, many):
        start = (first % tiles) * SUB + (first // tiles) * pages + page
        return lines[pl.ds(start, many, stride=SUB), :]

    group = QH // KVH
    scale = 1.0 / HD**0.5
    lane = lax.broadcasted_iota(jnp.int32, (1, page_len), 1)
    head_group = lax.broadcasted_iota(jnp.int32, (QH, HD), 0) // group
    eye = lax.broadcasted_iota(jnp.int32, (QH, LANES), 0)
    eye_lane = lax.broadcasted_iota(jnp.int32, (QH, LANES), 1)
    order = lax.broadcasted_iota(jnp.int32, table.shape, 0)
    value_rows = pages * QH
    log_row = jnp.zeros((1, LANES), f32)
    for p in range(pages):
        slot = position[0] * pages + p
        hit = table[...] == slot
        logical = jnp.sum(jnp.where(hit, order, 0), axis=(0, 1), keepdims=True)
        length = jnp.sum(
            jnp.where(hit, jnp.broadcast_to(lengths[...], hit.shape), 0),
            axis=(0, 1),
            keepdims=True,
        )
        live = logical * page_len + lane < length
        leads = logical == 0
        query = jnp.concatenate([heads(p, g * group, group) for g in range(KVH)], axis=0)
        keys = [heads(p, QH + g, 1) for g in range(KVH)]
        values = [heads(p, QH + KVH + g, 1) for g in range(KVH)]
        key_rows = jnp.concatenate([jnp.broadcast_to(k, (group, HD)) for k in keys], axis=0)
        value_own = jnp.concatenate([jnp.broadcast_to(v, (group, HD)) for v in values], axis=0)
        spread = jnp.concatenate(
            [jnp.where(head_group == g, query, 0.0).astype(bf16) for g in range(KVH)], axis=-1
        )
        scores = (
            lax.dot_general(
                spread,
                cache[p, :, : KVH * HD],
                (((1,), (1,)), ((), ())),
                preferred_element_type=f32,
            )
            * scale
        )
        own = jnp.sum(query * key_rows, axis=-1, keepdims=True) * scale
        masked = jnp.where(live, scores, lowest)
        own = jnp.where(leads, own, lowest)
        peak = jnp.maximum(jnp.max(masked, axis=-1, keepdims=True), own)
        weights = jnp.where(live, jnp.exp(masked - peak), 0.0)
        own_weight = jnp.where(leads, jnp.exp(own - peak), 0.0)
        mass = jnp.sum(weights, axis=-1, keepdims=True) + own_weight
        wide = jnp.dot(
            weights.astype(bf16), cache[p, :, KVH * HD :], preferred_element_type=f32
        )
        mixed = own_weight * value_own
        for g in range(KVH):
            mixed = mixed + jnp.where(head_group == g, wide[:, g * HD : (g + 1) * HD], 0.0)
        some = mass > 0.0
        safe = jnp.where(some, mass, 1.0)
        result = (mixed / safe).astype(bf16)
        logs = jnp.where(some, peak + jnp.log(safe), lowest)
        log_row = log_row + jnp.sum(
            jnp.where(eye_lane == eye + p * QH, logs, 0.0), axis=0, keepdims=True
        )
        for e in range(count):
            sent[e, p * QH : (p + 1) * QH, :] = result
    terms = pieces(log_row, PARTS) + [jnp.zeros((SUB - PARTS, LANES), f32)]
    terms = jnp.concatenate(terms, axis=0).astype(bf16)
    for e in range(count):
        sent[e, value_rows : value_rows + SUB, :] = fresh
        sent[e, value_rows + SUB :, :] = terms


def merge_kernel(
    pages, position, table, near_ref, far_ref, weights, middle, final, new_kv, scaled, rows
):
    chips = near_ref.shape[0]
    pages_req, requests = table.shape
    value_rows = pages * QH
    core = position[0] % 2
    packages = (near_ref, far_ref)
    logs = jnp.concatenate(
        [
            jnp.sum(ref[:, value_rows + SUB :, :].astype(f32), axis=1)
            for ref in packages
        ],
        axis=0,
    )
    row = lax.broadcasted_iota(jnp.int32, logs.shape, 0)
    slot = lax.broadcasted_iota(jnp.int32, logs.shape, 1) // QH
    parity = jnp.where(row < chips, core, 1 - core)
    page = jnp.where(slot < pages, ((row % chips) * 2 + parity) * pages + slot, -1)
    hits = []
    for r in range(requests):
        hit = page == table[0, r]
        for j in range(1, pages_req):
            hit = jnp.logical_or(hit, page == table[j, r])
        hits.append(hit)

    def over_slots(value, combine):
        out = value
        for k in range(1, pages):
            out = combine(out, pltpu.roll(value, k * QH, 1))
            out = combine(out, pltpu.roll(value, LANES - k * QH, 1))
        return out

    def back(per_request):
        out = jnp.zeros(logs.shape, f32)
        for r in range(requests):
            out = jnp.where(hits[r], per_request[r : r + 1, :], out)
        return out

    tops = jnp.concatenate(
        [jnp.max(jnp.where(hit, logs, lowest), axis=0, keepdims=True) for hit in hits], axis=0
    )
    factors = jnp.exp(jnp.where(slot < pages, logs - back(over_slots(tops, jnp.maximum)), lowest))
    masses = jnp.concatenate(
        [jnp.sum(jnp.where(hit, factors, 0.0), axis=0, keepdims=True) for hit in hits], axis=0
    )
    masses = over_slots(masses, jnp.add)
    inverse = 1.0 / jnp.where(masses > 0.0, masses, 1.0)
    shares = factors * back(inverse)
    turned = jnp.concatenate([shares, jnp.zeros((LANES - 2 * chips, LANES), f32)], axis=0).T
    for side, ref in enumerate(packages):
        for chip in range(chips):
            device = side * chips + chip
            scaled[device] = ref[chip, :value_rows, :].astype(f32) * turned[
                :value_rows, device : device + 1
            ]
    for r in range(requests):
        total = None
        for j in range(pages_req):
            device = lax.div(table[j, r], pages)
            side = lax.rem(device + core, 2)
            place = side * chips + lax.div(device, 2)
            first = pl.multiple_of(lax.rem(table[j, r], pages) * QH, QH)
            part = scaled[place, pl.ds(first, QH), :]
            total = part if total is None else total + part
        rows[r * QH : (r + 1) * QH, :] = total
    for chip in range(chips):
        mine, theirs = (ref[chip, value_rows : value_rows + SUB, :].astype(f32) for ref in packages)
        first = 2 * chip * HD
        new_kv[:, first : first + HD] = jnp.where(core == 0, mine, theirs).astype(bf16)
        new_kv[:, first + HD : first + 2 * HD] = jnp.where(core == 0, theirs, mine).astype(bf16)
    attended = jnp.concatenate(
        [rows[pl.ds(h, requests, stride=QH), :].astype(bf16) for h in range(QH)], axis=-1
    )
    total = jnp.dot(attended, weights[...], preferred_element_type=f32)
    final[...] = (middle[...] + total).astype(bf16)


def fused_shards(
    hidden,
    mix_gain,
    in_gate_input,
    in_step,
    in_groups,
    conv_input,
    conv_groups,
    taps_input,
    taps_groups,
    decay_rate,
    step_bias,
    skip_gain,
    norm_gain,
    out_mixer,
    ssm_state,
    attn_gain,
    w_qkv,
    w_out,
    kv_cache,
    page_table,
    lengths,
):
    count = lax.axis_size("seq")
    position = lax.axis_index("seq").astype(jnp.int32).reshape(1)
    requests, width = hidden.shape
    columns = width // count
    head_width = in_gate_input.shape[1] // 2
    pages = kv_cache.shape[0]
    chunks = SUB // pages
    chips = count // 2
    gcols = in_groups.shape[1]
    state = ssm_state.reshape(requests, head_width, STATE)
    same_core = [list(range(core, count, 2)) for core in range(2)]
    cores = [(i, i ^ 1) for i in range(count)]
    group_args = (
        hidden,
        mix_gain.reshape(1, width),
        in_groups,
        conv_groups.transpose(1, 0, 2),
        taps_groups,
    )
    group_conv, normed = call(
        group_kernel,
        (near((requests, gcols), bf16), near((requests, width), bf16)),
        [FAR] * 5,
        [pltpu.VMEM(x.shape, x.dtype) for x in group_args]
        + [pltpu.SemaphoreType.DMA((len(group_args) - 1 + BLOCKS,))],
        MOST,
    )(*group_args)
    swap = [(i, (i + GROUPS) % count) for i in range(count)]
    other = lax.ppermute(group_conv, "seq", swap)
    carried = (
        state,
        out_mixer,
        norm_gain.reshape(1, head_width),
        attn_gain.reshape(1, columns),
        page_table.T,
        lengths.reshape(1, requests),
    )
    gate_args = (
        in_gate_input,
        in_step.T,
        conv_input.transpose(1, 0, 2),
        taps_input,
    )
    numbers = jnp.concatenate([decay_rate, step_bias, skip_gain])
    gate, conv, step, decay, stream, state_in, mixer, gain, scale, table, spans = call(
        functools.partial(gate_kernel, len(carried)),
        (
            near((requests, head_width), f32),
            near((requests, 2 * head_width), f32),
            near((requests, LANES), f32),
            near((requests, LANES), f32),
            near((requests, columns), bf16),
        )
        + tuple(near(x.shape, x.dtype) for x in carried),
        [SMEM, NEAR] + [FAR] * 4 + [SMEM] + [FAR] * (1 + len(carried)),
        [pltpu.VMEM(x.shape, x.dtype) for x in gate_args]
        + [pltpu.SemaphoreType.DMA((BLOCKS + 4 + len(carried),))],
    )(position, normed, *gate_args, numbers, hidden, *carried)
    sent = call(
        mixer_kernel,
        near((count, requests, columns + LANES), bf16),
        [SMEM] + [NEAR] * 9,
    )(position, group_conv, other, gate, conv, step, decay, state_in, mixer, gain)
    received = lax.all_to_all(sent, "seq", 0, 0)
    new_state = call(state_kernel, shape(state.shape, f32), [SMEM] + [NEAR] * 6)(
        position, group_conv, other, conv, step, decay, state_in
    )
    chunk = w_qkv.shape[1] // chunks
    keep, give, middle = call(
        functools.partial(project_kernel, chunks, head_width),
        (
            near((chips, SUB, chunk + 2 * LANES), f32),
            near((chips, SUB, chunk + 2 * LANES), bf16),
            near((requests, columns), f32),
        ),
        [SMEM] + [NEAR] * 5,
    )(position, received, stream, scale, w_qkv, table)
    taken = lax.ppermute(give, "seq", cores)
    sent = call(pair_kernel, near(give.shape, bf16), [NEAR] * 2 + [FAR])(keep, taken, new_state)
    received = lax.all_to_all(sent, "seq", 0, 0, axis_index_groups=same_core)
    package = pages * QH + 2 * SUB
    sent = call(
        functools.partial(attend_kernel, width),
        near((chips, package, HD), bf16),
        [SMEM] + [NEAR] * 4,
        [pltpu.VMEM((chunk // HD * SUB, HD), f32)],
    )(position, received, kv_cache, table, spans)
    received = lax.all_to_all(sent, "seq", 0, 0, axis_index_groups=same_core)
    far = lax.ppermute(received, "seq", cores)
    final, new_kv = call(
        functools.partial(merge_kernel, pages),
        (
            shape((requests, columns), bf16),
            shape((requests, 2 * KVH * HD), bf16),
        ),
        [SMEM] * 2 + [NEAR] * 4,
        [
            pltpu.VMEM((count, pages * QH, HD), f32),
            pltpu.VMEM((requests * QH, HD), f32),
        ],
    )(position, page_table.T, received, far, w_out, middle)
    return (final, new_state.reshape(ssm_state.shape), new_kv)


def shards(*args):
    hidden, in_step, in_groups = args[0], args[3], args[4]
    kv_cache, page_table = args[18], args[19]
    count = lax.axis_size("seq")
    whole_tiles = (
        in_step.shape[1] == 1
        and in_groups.shape[1] == STATE
        and count == 2 * GROUPS
        and hidden.shape[0] == SUB
        and (hidden.shape[1] // count) % LANES == 0
        and SUB % kv_cache.shape[0] == 0
        and kv_cache.shape[0] * QH <= LANES
        and kv_cache.shape[1] == LANES
        and 2 * KVH == count
    )
    return (fused_shards if whole_tiles else plain_shards)(*args)


def solution(mesh):
    placed = (
        P("grp", None),
        P(),
        P(None, "seq"),
        P(None, "seq"),
        P(None, "seq"),
        P("grp", None, "seq"),
        P("grp", None, "seq"),
        P(None, "seq"),
        P(None, "seq"),
        P("seq"),
        P("seq"),
        P("seq"),
        P("seq"),
        P("seq", None),
        P("grp", "seq", None, None),
        P("seq"),
        P("seq", None),
        P(None, "seq"),
        P(("grp", "seq"), None, None),
        P("grp", None),
        P("grp"),
    )
    return jax.shard_map(
        shards,
        mesh=mesh,
        in_specs=placed,
        out_specs=(P("grp", "seq"), P("grp", "seq", None, None), P("grp", None)),
        check_vma=False,
    )
```

```python
import functools

import jax
import jax.numpy as jnp
from jax import lax
from jax.experimental import pallas as pl
from jax.experimental.pallas import tpu as pltpu
from jax.sharding import PartitionSpec as P

QH = 32
KVH = 8
HD = 128
STATE = 128
GROUPS = 8
LANES = 128

epsilon = 1e-05
lowest = -1e30


def conv_step(state, fresh, taps):
    window = jnp.concatenate([state.astype(jnp.float32), fresh[:, None, :]], axis=1)
    summed = jnp.sum(window * taps[:-1][None], axis=1) + taps[-1][None]
    return jax.nn.silu(summed)


def split(value, parts):
    pieces = []
    rest = value
    for _ in range(parts):
        piece = lax.reduce_precision(rest, 8, 7)
        pieces.append(piece.astype(jnp.bfloat16))
        rest = rest - piece
    return pieces


def group_vectors(group_conv, heads_here, requests):
    count = lax.axis_size("seq")
    position = lax.axis_index("seq")
    if heads_here == 1 and group_conv.shape[1] == STATE and count == 2 * GROUPS:
        swap = [(i, (i + GROUPS) % count) for i in range(count)]
        other = lax.ppermute(group_conv, "seq", swap)
        first = position < GROUPS
        inject = jnp.where(first, group_conv, other)
        readout = jnp.where(first, other, group_conv)
        return (
            inject.astype(jnp.float32)[:, None, :],
            readout.astype(jnp.float32)[:, None, :],
        )
    group_all = lax.all_gather(group_conv, "seq", axis=1, tiled=True).astype(jnp.float32)
    inject = group_all[:, : GROUPS * STATE].reshape(requests, GROUPS, STATE)
    readout = group_all[:, GROUPS * STATE :].reshape(requests, GROUPS, STATE)
    head_ids = position * heads_here + jnp.arange(heads_here, dtype=jnp.int32)
    return inject[:, head_ids % GROUPS], readout[:, head_ids % GROUPS]


def plain_shards(
    hidden,
    mix_gain,
    in_gate_input,
    in_step,
    in_groups,
    conv_input,
    conv_groups,
    taps_input,
    taps_groups,
    decay_rate,
    step_bias,
    skip_gain,
    norm_gain,
    out_mixer,
    ssm_state,
    attn_gain,
    w_qkv,
    w_out,
    kv_cache,
    page_table,
    lengths,
):
    count_seq = lax.axis_size("seq")
    position = lax.axis_index("seq")
    requests = hidden.shape[0]
    width = hidden.shape[1]
    heads_here = in_step.shape[1]
    head_width = in_gate_input.shape[1] // (2 * heads_here)
    heads_total = heads_here * count_seq
    per_group = heads_total // GROUPS
    columns = width // count_seq
    stream = hidden.astype(jnp.float32)
    normed = (
        stream * lax.rsqrt(jnp.mean(stream * stream, axis=-1, keepdims=True) + epsilon) * mix_gain
    ).astype(jnp.bfloat16)
    group_raw = jnp.dot(normed, in_groups, preferred_element_type=jnp.float32)
    group_conv = conv_step(conv_groups, group_raw, taps_groups).astype(jnp.bfloat16)
    inject_heads, readout_heads = group_vectors(group_conv, heads_here, requests)
    gate_input = jnp.dot(normed, in_gate_input, preferred_element_type=jnp.float32).reshape(
        requests, heads_here, 2, head_width
    )
    gate_part = gate_input[:, :, 0]
    input_part = gate_input[:, :, 1].reshape(requests, heads_here * head_width)
    step_raw = jnp.dot(normed, in_step, preferred_element_type=jnp.float32)
    conv_out = conv_step(conv_input, input_part, taps_input).reshape(
        requests, heads_here, head_width
    )
    step_size = jax.nn.softplus(step_raw + step_bias)
    decay = jnp.exp(-decay_rate * step_size)
    new_state = (
        decay[:, :, None, None] * ssm_state
        + (step_size[:, :, None] * conv_out)[:, :, :, None] * inject_heads[:, :, None, :]
    )
    ssm_out = (
        jnp.sum(new_state * readout_heads[:, :, None, :], axis=-1)
        + skip_gain[None, :, None] * conv_out
    )
    gated = ssm_out * jax.nn.silu(gate_part)
    head_squares = jnp.sum(gated * gated, axis=-1)
    weighted = (gated * norm_gain.reshape(heads_here, head_width)).astype(jnp.bfloat16)
    products = jnp.einsum(
        "rhp,hpd->hrd",
        weighted,
        out_mixer.reshape(heads_here, head_width, width),
        preferred_element_type=jnp.float32,
    ).astype(jnp.bfloat16)
    products = products.reshape(heads_here, requests, count_seq, columns).transpose(2, 0, 1, 3)
    marks = jnp.stack(split(head_squares.T, 2), axis=-1)
    marks = jnp.pad(marks, ((0, 0), (0, 0), (0, LANES - 2)))
    marks = jnp.broadcast_to(marks[None], (count_seq,) + marks.shape)
    received = lax.all_to_all(jnp.concatenate([products, marks], axis=-1), "seq", 0, 0)
    received = received.astype(jnp.float32)
    squares = (received[..., columns] + received[..., columns + 1]).reshape(
        per_group, GROUPS, requests
    )
    scales = lax.rsqrt(jnp.sum(squares, axis=0) / (per_group * head_width) + epsilon)
    mixer = jnp.sum(
        received[..., :columns].reshape(per_group, GROUPS, requests, columns)
        * scales[None, :, :, None],
        axis=(0, 1),
    )
    stream_cols = lax.dynamic_slice_in_dim(stream, position * columns, columns, 1)
    middle = (stream_cols + mixer).astype(jnp.bfloat16)
    middle_f = middle.astype(jnp.float32)
    scaled = (middle_f * attn_gain).astype(jnp.bfloat16)
    partial_sq = jnp.sum(middle_f * middle_f, axis=-1)
    pages_here = kv_cache.shape[0]
    page_len = kv_cache.shape[1]
    pages_req = page_table.shape[1]
    pages_all = pages_here * count_seq
    matches = page_table[None, :, :] == jnp.arange(pages_all, dtype=jnp.int32)[:, None, None]
    owner = jnp.any(matches, axis=2)
    page_rows = jnp.dot(
        owner.astype(jnp.bfloat16), scaled, preferred_element_type=jnp.float32
    ).astype(jnp.bfloat16)
    page_proj = jnp.dot(page_rows, w_qkv, preferred_element_type=jnp.float32).astype(jnp.bfloat16)
    page_sq = jnp.sum(jnp.where(owner, partial_sq[None, :], 0.0), axis=1)
    sq_parts = jnp.pad(jnp.stack(split(page_sq, 2), axis=-1), ((0, 0), (0, LANES - 2)))
    sent = jnp.concatenate([page_proj, sq_parts], axis=-1).reshape(count_seq, pages_here, -1)
    arrived = jnp.sum(lax.all_to_all(sent, "seq", 0, 0).astype(jnp.float32), axis=0)
    qkv_width = w_qkv.shape[1]
    total_sq = arrived[:, qkv_width] + arrived[:, qkv_width + 1]
    qkv = (arrived[:, :qkv_width] * lax.rsqrt(total_sq / width + epsilon)[:, None]).astype(
        jnp.bfloat16
    )
    group_size = QH // KVH
    queries = qkv[:, : QH * HD].reshape(pages_here, KVH, group_size, HD)
    fresh_kv = qkv[:, QH * HD :]
    fresh_keys = fresh_kv[:, : KVH * HD].reshape(pages_here, KVH, 1, HD).astype(jnp.float32)
    fresh_values = fresh_kv[:, KVH * HD :].reshape(pages_here, KVH, 1, HD).astype(jnp.float32)
    scale = 1.0 / HD**0.5
    slots = position * pages_here + jnp.arange(pages_here, dtype=jnp.int32)
    own_matches = page_table[None, :, :] == slots[:, None, None]
    logical = jnp.sum(
        jnp.any(own_matches, axis=1) * jnp.arange(pages_req, dtype=jnp.int32)[None, :], axis=1
    )
    page_length = jnp.sum(jnp.where(jnp.any(own_matches, axis=2), lengths[None, :], 0), axis=1)
    token_pos = logical[:, None] * page_len + jnp.arange(page_len, dtype=jnp.int32)[None, :]
    live = (token_pos < page_length[:, None])[:, None, None, :]
    leads = (logical == 0)[:, None, None]
    cached = kv_cache.reshape(pages_here, page_len, 2, KVH, HD)
    scores = (
        jnp.einsum("pgjd,ptgd->pgjt", queries, cached[:, :, 0], preferred_element_type=jnp.float32)
        * scale
    )
    own = jnp.sum(queries.astype(jnp.float32) * fresh_keys, axis=-1) * scale
    masked = jnp.where(live, scores, lowest)
    own = jnp.where(leads, own, lowest)
    peak = jnp.maximum(jnp.max(masked, axis=-1), own)
    weights = jnp.where(live, jnp.exp(masked - peak[..., None]), 0.0)
    own_weight = jnp.where(leads, jnp.exp(own - peak), 0.0)
    total = jnp.sum(weights, axis=-1) + own_weight
    values = jnp.einsum(
        "pgjt,ptgd->pgjd",
        weights.astype(jnp.bfloat16),
        cached[:, :, 1],
        preferred_element_type=jnp.float32,
    )
    values = values + own_weight[..., None] * fresh_values
    some = total > 0.0
    safe = jnp.where(some, total, 1.0)
    values = (values / safe[..., None]).astype(jnp.bfloat16)
    logsum = jnp.where(some, peak + jnp.log(safe), lowest)
    logs = jnp.concatenate(split(logsum.reshape(1, pages_here * QH), 3), axis=0)
    logs = jnp.pad(logs, ((0, 5), (0, LANES - pages_here * QH)))
    value_rows = pages_here * QH
    kv_rows = pages_here * 2 * KVH
    package = jnp.concatenate(
        [values.reshape(value_rows, HD), fresh_kv.reshape(kv_rows, HD), logs], axis=0
    )
    package = jnp.broadcast_to(package[None], (count_seq,) + package.shape)
    everything = lax.all_to_all(package, "seq", 0, 0)
    all_values = everything[:, :value_rows].reshape(pages_all, QH, HD)
    all_kv = everything[:, value_rows : value_rows + kv_rows].reshape(pages_all, 2 * KVH * HD)
    all_logs = everything[:, value_rows + kv_rows :, : pages_here * QH].astype(jnp.float32)
    all_logs = (all_logs[:, 0] + all_logs[:, 1] + all_logs[:, 2]).reshape(pages_all, QH)
    new_kv = all_kv[page_table[:, 0]]
    req_logs = all_logs[page_table]
    top = jnp.max(req_logs, axis=1, keepdims=True)
    factors = jnp.exp(req_logs - top)
    summed = jnp.sum(factors[..., None] * all_values[page_table].astype(jnp.float32), axis=1)
    attended = (summed / jnp.sum(factors, axis=1)[..., None]).astype(jnp.bfloat16)
    final = (
        middle_f
        + jnp.dot(
            attended.reshape(requests, QH * HD), w_out, preferred_element_type=jnp.float32
        )
    ).astype(jnp.bfloat16)
    return (final, new_state, new_kv)


f32 = jnp.float32
bf16 = jnp.bfloat16
SUB = 8
PARTS = 3
SCOPED = 16 << 20
MOST = 63500 << 10
BLOCKS = 4
VMEM = pl.BlockSpec(memory_space=pltpu.VMEM)
NEAR = pl.BlockSpec(memory_space=pltpu.VMEM)
SMEM = pl.BlockSpec(memory_space=pltpu.SMEM)
FAR = pl.BlockSpec(memory_space=pltpu.HBM)


def call(kernel, outs, specs, scratch=(), scoped=SCOPED):
    grid_free = pl.pallas_call(
        kernel,
        out_shape=outs,
        in_specs=specs,
        out_specs=jax.tree.map(lambda _: VMEM, outs, is_leaf=lambda x: hasattr(x, "shape")),
        scratch_shapes=scratch,
        compiler_params=pltpu.CompilerParams(vmem_limit_bytes=scoped),
    )

    def run(*args):
        spaces = {id(NEAR): pltpu.VMEM, id(FAR): pltpu.HBM}
        placed = [
            pltpu.with_memory_space_constraint(arg, spaces[id(spec)]) if id(spec) in spaces else arg
            for arg, spec in zip(args, specs)
        ]
        return grid_free(*placed)

    return run


def shape(dims, kind):
    return jax.ShapeDtypeStruct(dims, kind)


def near(dims, kind):
    return pltpu.VMEM(dims, kind)


def silu(x):
    return x * jax.nn.sigmoid(x)


def pieces(value, parts):
    out = []
    for _ in range(parts):
        piece = value.astype(bf16).astype(f32)
        out.append(piece)
        value = value - piece
    return out


def marked(value, parts, first=0):
    lane = lax.broadcasted_iota(jnp.int32, (value.shape[0], LANES), 1)
    out = jnp.zeros((value.shape[0], LANES), f32)
    for k, piece in enumerate(pieces(value, parts)):
        out = jnp.where(lane == first + k, piece, out)
    return out


def summed(marks, first=0):
    return marks[:, first : first + 1] + marks[:, first + 1 : first + 2]


def convolve(state_ref, fresh, taps_ref):
    taps = state_ref.shape[0]
    total = taps_ref[taps : taps + 1, :] * fresh + taps_ref[taps + 1 : taps + 2, :]
    for k in range(taps):
        total = total + taps_ref[k : k + 1, :] * state_ref[k].astype(f32)
    return silu(total)


def fetch_all(pairs, sems):
    copies = [
        pltpu.make_async_copy(source, target, sems.at[k])
        for k, (source, target) in enumerate(pairs)
    ]
    for copy in copies:
        copy.start()
    return copies


def group_kernel(
    hidden_far,
    gain_far,
    weights_far,
    state_far,
    taps_far,
    group_out,
    normed_out,
    hidden,
    gain,
    weights,
    state,
    taps,
    sems,
):
    depth = weights.shape[0] // BLOCKS
    rows = [pl.ds(k * depth, depth) for k in range(BLOCKS)]
    copies = fetch_all(
        [(hidden_far, hidden), (gain_far, gain)]
        + [(weights_far.at[r], weights.at[r]) for r in rows]
        + [(state_far, state), (taps_far, taps)],
        sems,
    )
    copies[0].wait()
    copies[1].wait()
    stream = hidden[...].astype(f32)
    mean = jnp.mean(stream * stream, axis=-1, keepdims=True)
    normed_out[...] = (stream * lax.rsqrt(mean + epsilon) * gain[...]).astype(bf16)
    raw = jnp.zeros(group_out.shape, f32)
    for k in range(BLOCKS):
        copies[2 + k].wait()
        span = slice(k * depth, (k + 1) * depth)
        raw = raw + jnp.dot(normed_out[:, span], weights[span, :], preferred_element_type=f32)
    copies[-2].wait()
    copies[-1].wait()
    group_out[...] = convolve(state, raw, taps).astype(bf16)


def gate_kernel(carried, position, normed_ref, *refs):
    weights_far, step_far, state_far, taps_far, numbers, hidden_far = refs[:6]
    inputs, outputs, scratch = refs[6 : 6 + carried], refs[6 + carried : -5], refs[-5:]
    gate_out, conv_out, step_out, decay_out, columns_out = outputs[:5]
    weights, step_row, state, taps, sems = scratch
    columns = columns_out.shape[1]
    start = pl.multiple_of(position[0] * columns, columns)
    depth = weights.shape[0] // BLOCKS
    rows = [pl.ds(k * depth, depth) for k in range(BLOCKS)]
    copies = fetch_all(
        [(weights_far.at[r], weights.at[r]) for r in rows]
        + [
            (step_far, step_row),
            (state_far, state),
            (taps_far, taps),
            (hidden_far.at[:, pl.ds(start, columns)], columns_out),
        ]
        + list(zip(inputs, outputs[5:])),
        sems,
    )
    half = gate_out.shape[1]
    both = jnp.zeros((gate_out.shape[0], weights.shape[1]), f32)
    for k in range(BLOCKS):
        copies[k].wait()
        span = slice(k * depth, (k + 1) * depth)
        both = both + jnp.dot(normed_ref[:, span], weights[span, :], preferred_element_type=f32)
    for copy in copies[BLOCKS : BLOCKS + 3]:
        copy.wait()
    gate_out[...] = silu(both[:, :half])
    fresh = convolve(state, both[:, half:], taps)
    conv_out[:, :half] = fresh
    conv_out[:, half:] = numbers[2] * fresh
    raw = jnp.sum(normed_ref[...].astype(f32) * step_row[...].astype(f32), axis=-1, keepdims=True)
    step = jax.nn.softplus(raw + numbers[1])
    step_out[...] = jnp.broadcast_to(step, step_out.shape)
    decay_out[...] = jnp.broadcast_to(jnp.exp(-numbers[0] * step), decay_out.shape)
    for copy in copies[BLOCKS + 3 :]:
        copy.wait()


def chosen(position, own, other):
    first = position[0] < GROUPS
    mine, theirs = own[...].astype(f32), other[...].astype(f32)
    return jnp.where(first, mine, theirs), jnp.where(first, theirs, mine)


def mixer_kernel(position, own, other, gate, conv, step, decay, state, weights, gain, sent):
    requests = own.shape[0]
    inject, readout = chosen(position, own, other)
    half = gate.shape[1]
    row = lax.broadcasted_iota(jnp.int32, gate.shape, 0)
    read = jnp.zeros(gate.shape, f32)
    for r in range(requests):
        part = lax.dot_general(
            readout,
            state[r],
            (((1,), (1,)), ((), ())),
            precision=lax.Precision.HIGHEST,
            preferred_element_type=f32,
        )
        read = jnp.where(row == r, part, read)
    along = jnp.sum(inject * readout, axis=-1, keepdims=True)
    fresh = conv[:, :half]
    out = decay[:, :1] * read + step[:, :1] * fresh * along + conv[:, half:]
    gated = out * gate[...]
    marks = marked(jnp.sum(gated * gated, axis=-1, keepdims=True), 2).astype(bf16)
    weighted = (gated * gain[...]).astype(bf16)
    count = sent.shape[0]
    columns = weights.shape[1] // count
    for e in range(count):
        product = jnp.dot(
            weighted, weights[:, e * columns : (e + 1) * columns], preferred_element_type=f32
        )
        sent[e, :, :columns] = product.astype(bf16)
        sent[e, :, columns:] = marks


def state_kernel(position, own, other, conv, step, decay, state, new_state):
    inject, _ = chosen(position, own, other)
    fresh = step[:, :1] * conv[:, : state.shape[1]]
    new_state[...] = (
        decay[:, :1][:, :, None] * state[...] + fresh[:, :, None] * inject[:, None, :]
    )


def project_kernel(
    chunks, head_width, position, received, hidden, gain, weights, table, keep, give, middle_out
):
    count, requests, _ = received.shape
    columns = weights.shape[0]
    squares = [received[k, :, columns:].astype(f32) for k in range(count)]
    mixer = jnp.zeros((requests, columns), f32)
    for g in range(GROUPS):
        members = range(g, count, GROUPS)
        marks = sum(squares[k] for k in members)
        total = marks[:, :1] + marks[:, 1:2]
        scale = lax.rsqrt(total / (len(members) * head_width) + epsilon)
        products = sum(received[k, :, :columns].astype(f32) for k in members)
        mixer = mixer + scale * products
    middle = (hidden[...].astype(f32) + mixer).astype(bf16).astype(f32)
    middle_out[...] = middle
    square = jnp.sum(middle * middle, axis=-1, keepdims=True)
    scaled = middle * gain[...]
    extended = jnp.concatenate([scaled, marked(square, 2)], axis=-1).astype(bf16)
    rows = count * SUB
    pages = SUB // chunks
    chips = count // 2
    core = position[0] % 2
    index = lax.broadcasted_iota(jnp.int32, (rows, requests), 0)
    line = index % (chips * SUB)
    parity = jnp.where(index < chips * SUB, core, 1 - core)
    page = ((line // SUB) * 2 + parity) * pages + index % pages
    hits = page == table[0:1, :]
    for j in range(1, table.shape[0]):
        hits = jnp.logical_or(hits, page == table[j : j + 1, :])
    onehot = jnp.where(hits, 1.0, 0.0).astype(bf16)
    spread = jnp.dot(onehot, extended, preferred_element_type=f32)
    lines = spread[:, :columns]
    which = (lax.broadcasted_iota(jnp.int32, lines.shape, 0) % SUB) // pages
    chunk = weights.shape[1] // chunks
    fresh_from = QH * HD
    zeros = jnp.zeros((SUB, columns), f32)
    lhs = []
    for c in range(chunks):
        own = jnp.where(which == c, lines, 0.0)
        if (c + 1) * chunk > fresh_from:
            own = jnp.concatenate([own, scaled, zeros], axis=0)
        lhs.append(own.astype(bf16))
    tile = 2 * HD
    for n in range(0, chunk, tile):
        total = None
        for c in range(chunks):
            first = c * chunk + n
            part = jnp.dot(lhs[c], weights[:, first : first + tile], preferred_element_type=f32)
            if first >= fresh_from:
                fresh = part[rows : rows + SUB]
                chip = (first - fresh_from) // tile
                low, high = fresh[:, :HD], fresh[:, HD:]
                keep[chip, :, chunk + LANES :] = jnp.where(core == 0, low, high)
                give[chip, :, chunk + LANES :] = jnp.where(core == 0, high, low).astype(bf16)
            total = part[:rows] if total is None else total + part[:rows]
        for e in range(chips):
            keep[e, :, n : n + tile] = total[e * SUB : (e + 1) * SUB]
            first = (chips + e) * SUB
            give[e, :, n : n + tile] = total[first : first + SUB].astype(bf16)
    marks = spread[:, columns:]
    request_marks = marked(square, 2, 2)
    for e in range(chips):
        keep[e, :, chunk : chunk + LANES] = marks[e * SUB : (e + 1) * SUB] + request_marks
        first = (chips + e) * SUB
        give[e, :, chunk : chunk + LANES] = (marks[first : first + SUB] + request_marks).astype(
            bf16
        )


def pair_kernel(keep, taken, _, sent):
    chunk = keep.shape[2] - 2 * LANES
    for e in range(keep.shape[0]):
        total = keep[e] + taken[e].astype(f32)
        marks = total[:, chunk : chunk + LANES]
        sent[e, :, :chunk] = total[:, :chunk].astype(bf16)
        sent[e, :, chunk : chunk + LANES] = (
            marked(summed(marks), 2) + marked(summed(marks, 2), 2, 2)
        ).astype(bf16)
        sent[e, :, chunk + LANES :] = total[:, chunk + LANES :].astype(bf16)


def attend_kernel(width, position, received, cache, table, lengths, sent, lines):
    count, _, full = received.shape
    pages, page_len, _ = cache.shape
    chunks = SUB // pages
    chunk = full - 2 * LANES
    tiles = chunk // HD
    total = received[0].astype(f32)
    for k in range(1, count):
        total = total + received[k].astype(f32)
    marks = total[:, chunk : chunk + LANES]
    inverse = lax.rsqrt(summed(marks) / width + epsilon)
    fresh = total[:, chunk + LANES :] * lax.rsqrt(summed(marks, 2) / width + epsilon)
    fresh = fresh.astype(bf16)
    for t in range(tiles):
        lines[t * SUB : (t + 1) * SUB, :] = (
            (total[:, t * HD : (t + 1) * HD] * inverse).astype(bf16).astype(f32)
        )

    def heads(page, first, many):
        start = (first % tiles) * SUB + (first // tiles) * pages + page
        return lines[pl.ds(start, many, stride=SUB), :]

    group = QH // KVH
    scale = 1.0 / HD**0.5
    lane = lax.broadcasted_iota(jnp.int32, (1, page_len), 1)
    head_group = lax.broadcasted_iota(jnp.int32, (QH, HD), 0) // group
    eye = lax.broadcasted_iota(jnp.int32, (QH, LANES), 0)
    value_rows = pages * QH
    place = (position[0] // 2) % (LANES // value_rows) * value_rows
    eye_lane = lax.broadcasted_iota(jnp.int32, (QH, LANES), 1) - place
    order = lax.broadcasted_iota(jnp.int32, table.shape, 0)
    log_row = jnp.zeros((1, LANES), f32)
    for p in range(pages):
        slot = position[0] * pages + p
        hit = table[...] == slot
        logical = jnp.sum(jnp.where(hit, order, 0), axis=(0, 1), keepdims=True)
        length = jnp.sum(
            jnp.where(hit, jnp.broadcast_to(lengths[...], hit.shape), 0),
            axis=(0, 1),
            keepdims=True,
        )
        live = logical * page_len + lane < length
        leads = logical == 0
        query = jnp.concatenate([heads(p, g * group, group) for g in range(KVH)], axis=0)
        keys = [heads(p, QH + g, 1) for g in range(KVH)]
        values = [heads(p, QH + KVH + g, 1) for g in range(KVH)]
        key_rows = jnp.concatenate([jnp.broadcast_to(k, (group, HD)) for k in keys], axis=0)
        value_own = jnp.concatenate([jnp.broadcast_to(v, (group, HD)) for v in values], axis=0)
        spread = jnp.concatenate(
            [jnp.where(head_group == g, query, 0.0).astype(bf16) for g in range(KVH)], axis=-1
        )
        scores = (
            lax.dot_general(
                spread,
                cache[p, :, : KVH * HD],
                (((1,), (1,)), ((), ())),
                preferred_element_type=f32,
            )
            * scale
        )
        own = jnp.sum(query * key_rows, axis=-1, keepdims=True) * scale
        masked = jnp.where(live, scores, lowest)
        own = jnp.where(leads, own, lowest)
        peak = jnp.maximum(jnp.max(masked, axis=-1, keepdims=True), own)
        weights = jnp.where(live, jnp.exp(masked - peak), 0.0)
        own_weight = jnp.where(leads, jnp.exp(own - peak), 0.0)
        mass = jnp.sum(weights, axis=-1, keepdims=True) + own_weight
        wide = jnp.dot(
            weights.astype(bf16), cache[p, :, KVH * HD :], preferred_element_type=f32
        )
        mixed = own_weight * value_own
        for g in range(KVH):
            mixed = mixed + jnp.where(head_group == g, wide[:, g * HD : (g + 1) * HD], 0.0)
        some = mass > 0.0
        safe = jnp.where(some, mass, 1.0)
        result = (mixed / safe).astype(bf16)
        logs = jnp.where(some, peak + jnp.log(safe), lowest)
        log_row = log_row + jnp.sum(
            jnp.where(eye_lane == eye + p * QH, logs, 0.0), axis=0, keepdims=True
        )
        for e in range(count):
            sent[e, p * QH : (p + 1) * QH, :] = result
    terms = pieces(log_row, PARTS) + [jnp.zeros((SUB - PARTS, LANES), f32)]
    terms = jnp.concatenate(terms, axis=0).astype(bf16)
    for e in range(count):
        sent[e, value_rows : value_rows + SUB, :] = fresh
        sent[e, value_rows + SUB :, :] = terms


def owner_kernel(chips, pages, position, table, _, owner):
    pages_req, requests = table.shape
    core = position[0] % 2
    span = pages * QH
    rows_each = owner.shape[0] // 2
    row = lax.broadcasted_iota(jnp.int32, owner.shape, 0)
    lane = lax.broadcasted_iota(jnp.int32, owner.shape, 1)
    chip = (row % rows_each) * (LANES // span) + lane // span
    parity = jnp.where(row < rows_each, core, 1 - core)
    page = (chip * 2 + parity) * pages + (lane % span) // QH
    found = jnp.zeros(owner.shape, jnp.int32)
    for r in range(requests):
        for j in range(pages_req):
            found = jnp.where(page == table[j, r], r, found)
    owner[...] = found


def merge_kernel(pages, position, near_ref, far_ref, owner, weights, middle, final, new_kv):
    chips = near_ref.shape[0]
    requests, width = middle.shape
    value_rows = pages * QH
    core = position[0] % 2
    packages = (near_ref, far_ref)
    for chip in range(chips):
        mine, theirs = (ref[chip, value_rows : value_rows + SUB, :].astype(f32) for ref in packages)
        first = 2 * chip * HD
        new_kv[:, first : first + HD] = jnp.where(core == 0, mine, theirs).astype(bf16)
        new_kv[:, first + HD : first + 2 * HD] = jnp.where(core == 0, theirs, mine).astype(bf16)
    each = LANES // value_rows
    request = lax.broadcasted_iota(jnp.int32, (requests, LANES), 0)
    lane = lax.broadcasted_iota(jnp.int32, (requests, LANES), 1)
    logs, hits = [], []
    for ref in packages:
        for chip in range(0, chips, each):
            terms = sum(ref[chip + k, value_rows + SUB :, :].astype(f32) for k in range(each))
            log = sum(terms[k : k + 1, :] for k in range(PARTS))
            logs.append(jnp.broadcast_to(log, (requests, LANES)))
            row = len(hits)
            hits.append(jnp.broadcast_to(owner[row : row + 1, :], (requests, LANES)) == request)

    def over_pages(value, combine):
        out = value
        for k in range(QH, LANES, QH):
            out = combine(out, pltpu.roll(value, k, 1))
        return out

    tops = functools.reduce(
        jnp.maximum, [jnp.where(hit, log, lowest) for hit, log in zip(hits, logs)]
    )
    tops = over_pages(tops, jnp.maximum)
    factors = [jnp.where(hit, jnp.exp(log - tops), 0.0) for hit, log in zip(hits, logs)]
    inverse = 1.0 / over_pages(functools.reduce(jnp.add, factors), jnp.add)
    shares = []
    for factor in factors:
        share = factor * inverse
        heads = [jnp.where(lane % QH == h, share, 0.0) for h in range(QH)]
        shares.append(jnp.concatenate(heads, axis=0).astype(bf16))
    half = len(shares) // 2
    mixed = None
    for side, ref in enumerate(packages):
        part = jnp.dot(
            jnp.concatenate(shares[side * half : (side + 1) * half], axis=1),
            jnp.concatenate([ref[chip, :value_rows, :] for chip in range(chips)], axis=0),
            preferred_element_type=f32,
        )
        mixed = part if mixed is None else mixed + part
    attended = jnp.concatenate(
        [mixed[h * requests : (h + 1) * requests] for h in range(QH)], axis=1
    ).astype(bf16)
    total = jnp.dot(attended, weights[...], preferred_element_type=f32)
    final[...] = (middle[...] + total).astype(bf16)


def fused_shards(
    hidden,
    mix_gain,
    in_gate_input,
    in_step,
    in_groups,
    conv_input,
    conv_groups,
    taps_input,
    taps_groups,
    decay_rate,
    step_bias,
    skip_gain,
    norm_gain,
    out_mixer,
    ssm_state,
    attn_gain,
    w_qkv,
    w_out,
    kv_cache,
    page_table,
    lengths,
):
    count = lax.axis_size("seq")
    position = lax.axis_index("seq").astype(jnp.int32).reshape(1)
    requests, width = hidden.shape
    columns = width // count
    head_width = in_gate_input.shape[1] // 2
    pages = kv_cache.shape[0]
    chunks = SUB // pages
    chips = count // 2
    gcols = in_groups.shape[1]
    state = ssm_state.reshape(requests, head_width, STATE)
    same_core = [list(range(core, count, 2)) for core in range(2)]
    cores = [(i, i ^ 1) for i in range(count)]
    group_args = (
        hidden,
        mix_gain.reshape(1, width),
        in_groups,
        conv_groups.transpose(1, 0, 2),
        taps_groups,
    )
    group_conv, normed = call(
        group_kernel,
        (near((requests, gcols), bf16), near((requests, width), bf16)),
        [FAR] * 5,
        [pltpu.VMEM(x.shape, x.dtype) for x in group_args]
        + [pltpu.SemaphoreType.DMA((len(group_args) - 1 + BLOCKS,))],
        MOST,
    )(*group_args)
    swap = [(i, (i + GROUPS) % count) for i in range(count)]
    other = lax.ppermute(group_conv, "seq", swap)
    carried = (
        state,
        out_mixer,
        norm_gain.reshape(1, head_width),
        attn_gain.reshape(1, columns),
        page_table.T,
        lengths.reshape(1, requests),
    )
    gate_args = (
        in_gate_input,
        in_step.T,
        conv_input.transpose(1, 0, 2),
        taps_input,
    )
    numbers = jnp.concatenate([decay_rate, step_bias, skip_gain])
    gate, conv, step, decay, stream, state_in, mixer, gain, scale, table, spans = call(
        functools.partial(gate_kernel, len(carried)),
        (
            near((requests, head_width), f32),
            near((requests, 2 * head_width), f32),
            near((requests, LANES), f32),
            near((requests, LANES), f32),
            near((requests, columns), bf16),
        )
        + tuple(near(x.shape, x.dtype) for x in carried),
        [SMEM, NEAR] + [FAR] * 4 + [SMEM] + [FAR] * (1 + len(carried)),
        [pltpu.VMEM(x.shape, x.dtype) for x in gate_args]
        + [pltpu.SemaphoreType.DMA((BLOCKS + 4 + len(carried),))],
    )(position, normed, *gate_args, numbers, hidden, *carried)
    sent = call(
        mixer_kernel,
        near((count, requests, columns + LANES), bf16),
        [SMEM] + [NEAR] * 9,
    )(position, group_conv, other, gate, conv, step, decay, state_in, mixer, gain)
    received = lax.all_to_all(sent, "seq", 0, 0)
    new_state = call(state_kernel, shape(state.shape, f32), [SMEM] + [NEAR] * 6)(
        position, group_conv, other, conv, step, decay, state_in
    )
    chunk = w_qkv.shape[1] // chunks
    keep, give, middle = call(
        functools.partial(project_kernel, chunks, head_width),
        (
            near((chips, SUB, chunk + 2 * LANES), f32),
            near((chips, SUB, chunk + 2 * LANES), bf16),
            near((requests, columns), f32),
        ),
        [SMEM] + [NEAR] * 5,
    )(position, received, stream, scale, w_qkv, table)
    taken = lax.ppermute(give, "seq", cores)
    sent = call(pair_kernel, near(give.shape, bf16), [NEAR] * 2 + [FAR])(keep, taken, new_state)
    received = lax.all_to_all(sent, "seq", 0, 0, axis_index_groups=same_core)
    package = pages * QH + 2 * SUB
    sent = call(
        functools.partial(attend_kernel, width),
        near((chips, package, HD), bf16),
        [SMEM] + [NEAR] * 4,
        [pltpu.VMEM((chunk // HD * SUB, HD), f32)],
    )(position, received, kv_cache, table, spans)
    received = lax.all_to_all(sent, "seq", 0, 0, axis_index_groups=same_core)
    far = lax.ppermute(received, "seq", cores)
    owner_rows = count * pages * QH // LANES
    owner = call(
        functools.partial(owner_kernel, chips, pages),
        near((owner_rows, LANES), jnp.int32),
        [SMEM] * 2 + [NEAR],
    )(position, page_table.T, received)
    final, new_kv = call(
        functools.partial(merge_kernel, pages),
        (
            shape((requests, columns), bf16),
            shape((requests, 2 * KVH * HD), bf16),
        ),
        [SMEM] + [NEAR] * 5,
    )(position, received, far, owner, w_out, middle)
    return (final, new_state.reshape(ssm_state.shape), new_kv)


def shards(*args):
    hidden, in_step, in_groups = args[0], args[3], args[4]
    kv_cache, page_table = args[18], args[19]
    count = lax.axis_size("seq")
    whole_tiles = (
        in_step.shape[1] == 1
        and in_groups.shape[1] == STATE
        and count == 2 * GROUPS
        and hidden.shape[0] == SUB
        and (hidden.shape[1] // count) % LANES == 0
        and SUB % kv_cache.shape[0] == 0
        and LANES % (kv_cache.shape[0] * QH) == 0
        and (count // 2) % (LANES // (kv_cache.shape[0] * QH)) == 0
        and kv_cache.shape[1] == LANES
        and 2 * KVH == count
    )
    return (fused_shards if whole_tiles else plain_shards)(*args)


def solution(mesh):
    placed = (
        P("grp", None),
        P(),
        P(None, "seq"),
        P(None, "seq"),
        P(None, "seq"),
        P("grp", None, "seq"),
        P("grp", None, "seq"),
        P(None, "seq"),
        P(None, "seq"),
        P("seq"),
        P("seq"),
        P("seq"),
        P("seq"),
        P("seq", None),
        P("grp", "seq", None, None),
        P("seq"),
        P("seq", None),
        P(None, "seq"),
        P(("grp", "seq"), None, None),
        P("grp", None),
        P("grp"),
    )
    return jax.shard_map(
        shards,
        mesh=mesh,
        in_specs=placed,
        out_specs=(P("grp", "seq"), P("grp", "seq", None, None), P("grp", None)),
        check_vma=False,
    )
```

```python
import functools

import jax
import jax.numpy as jnp
from jax import lax
from jax.experimental import pallas as pl
from jax.experimental.pallas import tpu as pltpu
from jax.sharding import PartitionSpec as P

QH = 32
KVH = 8
HD = 128
STATE = 128
GROUPS = 8
LANES = 128

epsilon = 1e-05
lowest = -1e30


def conv_step(state, fresh, taps):
    window = jnp.concatenate([state.astype(jnp.float32), fresh[:, None, :]], axis=1)
    summed = jnp.sum(window * taps[:-1][None], axis=1) + taps[-1][None]
    return jax.nn.silu(summed)


def split(value, parts):
    pieces = []
    rest = value
    for _ in range(parts):
        piece = lax.reduce_precision(rest, 8, 7)
        pieces.append(piece.astype(jnp.bfloat16))
        rest = rest - piece
    return pieces


def group_vectors(group_conv, heads_here, requests):
    count = lax.axis_size("seq")
    position = lax.axis_index("seq")
    if heads_here == 1 and group_conv.shape[1] == STATE and count == 2 * GROUPS:
        swap = [(i, (i + GROUPS) % count) for i in range(count)]
        other = lax.ppermute(group_conv, "seq", swap)
        first = position < GROUPS
        inject = jnp.where(first, group_conv, other)
        readout = jnp.where(first, other, group_conv)
        return (
            inject.astype(jnp.float32)[:, None, :],
            readout.astype(jnp.float32)[:, None, :],
        )
    group_all = lax.all_gather(group_conv, "seq", axis=1, tiled=True).astype(jnp.float32)
    inject = group_all[:, : GROUPS * STATE].reshape(requests, GROUPS, STATE)
    readout = group_all[:, GROUPS * STATE :].reshape(requests, GROUPS, STATE)
    head_ids = position * heads_here + jnp.arange(heads_here, dtype=jnp.int32)
    return inject[:, head_ids % GROUPS], readout[:, head_ids % GROUPS]


def plain_shards(
    hidden,
    mix_gain,
    in_gate_input,
    in_step,
    in_groups,
    conv_input,
    conv_groups,
    taps_input,
    taps_groups,
    decay_rate,
    step_bias,
    skip_gain,
    norm_gain,
    out_mixer,
    ssm_state,
    attn_gain,
    w_qkv,
    w_out,
    kv_cache,
    page_table,
    lengths,
):
    count_seq = lax.axis_size("seq")
    position = lax.axis_index("seq")
    requests = hidden.shape[0]
    width = hidden.shape[1]
    heads_here = in_step.shape[1]
    head_width = in_gate_input.shape[1] // (2 * heads_here)
    heads_total = heads_here * count_seq
    per_group = heads_total // GROUPS
    columns = width // count_seq
    stream = hidden.astype(jnp.float32)
    normed = (
        stream * lax.rsqrt(jnp.mean(stream * stream, axis=-1, keepdims=True) + epsilon) * mix_gain
    ).astype(jnp.bfloat16)
    group_raw = jnp.dot(normed, in_groups, preferred_element_type=jnp.float32)
    group_conv = conv_step(conv_groups, group_raw, taps_groups).astype(jnp.bfloat16)
    inject_heads, readout_heads = group_vectors(group_conv, heads_here, requests)
    gate_input = jnp.dot(normed, in_gate_input, preferred_element_type=jnp.float32).reshape(
        requests, heads_here, 2, head_width
    )
    gate_part = gate_input[:, :, 0]
    input_part = gate_input[:, :, 1].reshape(requests, heads_here * head_width)
    step_raw = jnp.dot(normed, in_step, preferred_element_type=jnp.float32)
    conv_out = conv_step(conv_input, input_part, taps_input).reshape(
        requests, heads_here, head_width
    )
    step_size = jax.nn.softplus(step_raw + step_bias)
    decay = jnp.exp(-decay_rate * step_size)
    new_state = (
        decay[:, :, None, None] * ssm_state
        + (step_size[:, :, None] * conv_out)[:, :, :, None] * inject_heads[:, :, None, :]
    )
    ssm_out = (
        jnp.sum(new_state * readout_heads[:, :, None, :], axis=-1)
        + skip_gain[None, :, None] * conv_out
    )
    gated = ssm_out * jax.nn.silu(gate_part)
    head_squares = jnp.sum(gated * gated, axis=-1)
    weighted = (gated * norm_gain.reshape(heads_here, head_width)).astype(jnp.bfloat16)
    products = jnp.einsum(
        "rhp,hpd->hrd",
        weighted,
        out_mixer.reshape(heads_here, head_width, width),
        preferred_element_type=jnp.float32,
    ).astype(jnp.bfloat16)
    products = products.reshape(heads_here, requests, count_seq, columns).transpose(2, 0, 1, 3)
    marks = jnp.stack(split(head_squares.T, 2), axis=-1)
    marks = jnp.pad(marks, ((0, 0), (0, 0), (0, LANES - 2)))
    marks = jnp.broadcast_to(marks[None], (count_seq,) + marks.shape)
    received = lax.all_to_all(jnp.concatenate([products, marks], axis=-1), "seq", 0, 0)
    received = received.astype(jnp.float32)
    squares = (received[..., columns] + received[..., columns + 1]).reshape(
        per_group, GROUPS, requests
    )
    scales = lax.rsqrt(jnp.sum(squares, axis=0) / (per_group * head_width) + epsilon)
    mixer = jnp.sum(
        received[..., :columns].reshape(per_group, GROUPS, requests, columns)
        * scales[None, :, :, None],
        axis=(0, 1),
    )
    stream_cols = lax.dynamic_slice_in_dim(stream, position * columns, columns, 1)
    middle = (stream_cols + mixer).astype(jnp.bfloat16)
    middle_f = middle.astype(jnp.float32)
    scaled = (middle_f * attn_gain).astype(jnp.bfloat16)
    partial_sq = jnp.sum(middle_f * middle_f, axis=-1)
    pages_here = kv_cache.shape[0]
    page_len = kv_cache.shape[1]
    pages_req = page_table.shape[1]
    pages_all = pages_here * count_seq
    matches = page_table[None, :, :] == jnp.arange(pages_all, dtype=jnp.int32)[:, None, None]
    owner = jnp.any(matches, axis=2)
    page_rows = jnp.dot(
        owner.astype(jnp.bfloat16), scaled, preferred_element_type=jnp.float32
    ).astype(jnp.bfloat16)
    page_proj = jnp.dot(page_rows, w_qkv, preferred_element_type=jnp.float32).astype(jnp.bfloat16)
    page_sq = jnp.sum(jnp.where(owner, partial_sq[None, :], 0.0), axis=1)
    sq_parts = jnp.pad(jnp.stack(split(page_sq, 2), axis=-1), ((0, 0), (0, LANES - 2)))
    sent = jnp.concatenate([page_proj, sq_parts], axis=-1).reshape(count_seq, pages_here, -1)
    arrived = jnp.sum(lax.all_to_all(sent, "seq", 0, 0).astype(jnp.float32), axis=0)
    qkv_width = w_qkv.shape[1]
    total_sq = arrived[:, qkv_width] + arrived[:, qkv_width + 1]
    qkv = (arrived[:, :qkv_width] * lax.rsqrt(total_sq / width + epsilon)[:, None]).astype(
        jnp.bfloat16
    )
    group_size = QH // KVH
    queries = qkv[:, : QH * HD].reshape(pages_here, KVH, group_size, HD)
    fresh_kv = qkv[:, QH * HD :]
    fresh_keys = fresh_kv[:, : KVH * HD].reshape(pages_here, KVH, 1, HD).astype(jnp.float32)
    fresh_values = fresh_kv[:, KVH * HD :].reshape(pages_here, KVH, 1, HD).astype(jnp.float32)
    scale = 1.0 / HD**0.5
    slots = position * pages_here + jnp.arange(pages_here, dtype=jnp.int32)
    own_matches = page_table[None, :, :] == slots[:, None, None]
    logical = jnp.sum(
        jnp.any(own_matches, axis=1) * jnp.arange(pages_req, dtype=jnp.int32)[None, :], axis=1
    )
    page_length = jnp.sum(jnp.where(jnp.any(own_matches, axis=2), lengths[None, :], 0), axis=1)
    token_pos = logical[:, None] * page_len + jnp.arange(page_len, dtype=jnp.int32)[None, :]
    live = (token_pos < page_length[:, None])[:, None, None, :]
    leads = (logical == 0)[:, None, None]
    cached = kv_cache.reshape(pages_here, page_len, 2, KVH, HD)
    scores = (
        jnp.einsum("pgjd,ptgd->pgjt", queries, cached[:, :, 0], preferred_element_type=jnp.float32)
        * scale
    )
    own = jnp.sum(queries.astype(jnp.float32) * fresh_keys, axis=-1) * scale
    masked = jnp.where(live, scores, lowest)
    own = jnp.where(leads, own, lowest)
    peak = jnp.maximum(jnp.max(masked, axis=-1), own)
    weights = jnp.where(live, jnp.exp(masked - peak[..., None]), 0.0)
    own_weight = jnp.where(leads, jnp.exp(own - peak), 0.0)
    total = jnp.sum(weights, axis=-1) + own_weight
    values = jnp.einsum(
        "pgjt,ptgd->pgjd",
        weights.astype(jnp.bfloat16),
        cached[:, :, 1],
        preferred_element_type=jnp.float32,
    )
    values = values + own_weight[..., None] * fresh_values
    some = total > 0.0
    safe = jnp.where(some, total, 1.0)
    values = (values / safe[..., None]).astype(jnp.bfloat16)
    logsum = jnp.where(some, peak + jnp.log(safe), lowest)
    logs = jnp.concatenate(split(logsum.reshape(1, pages_here * QH), 3), axis=0)
    logs = jnp.pad(logs, ((0, 5), (0, LANES - pages_here * QH)))
    value_rows = pages_here * QH
    kv_rows = pages_here * 2 * KVH
    package = jnp.concatenate(
        [values.reshape(value_rows, HD), fresh_kv.reshape(kv_rows, HD), logs], axis=0
    )
    package = jnp.broadcast_to(package[None], (count_seq,) + package.shape)
    everything = lax.all_to_all(package, "seq", 0, 0)
    all_values = everything[:, :value_rows].reshape(pages_all, QH, HD)
    all_kv = everything[:, value_rows : value_rows + kv_rows].reshape(pages_all, 2 * KVH * HD)
    all_logs = everything[:, value_rows + kv_rows :, : pages_here * QH].astype(jnp.float32)
    all_logs = (all_logs[:, 0] + all_logs[:, 1] + all_logs[:, 2]).reshape(pages_all, QH)
    new_kv = all_kv[page_table[:, 0]]
    req_logs = all_logs[page_table]
    top = jnp.max(req_logs, axis=1, keepdims=True)
    factors = jnp.exp(req_logs - top)
    summed = jnp.sum(factors[..., None] * all_values[page_table].astype(jnp.float32), axis=1)
    attended = (summed / jnp.sum(factors, axis=1)[..., None]).astype(jnp.bfloat16)
    final = (
        middle_f
        + jnp.dot(
            attended.reshape(requests, QH * HD), w_out, preferred_element_type=jnp.float32
        )
    ).astype(jnp.bfloat16)
    return (final, new_state, new_kv)


f32 = jnp.float32
bf16 = jnp.bfloat16
SUB = 8
PARTS = 3
SCOPED = 16 << 20
MOST = 63500 << 10
BLOCKS = 2
VMEM = pl.BlockSpec(memory_space=pltpu.VMEM)
NEAR = pl.BlockSpec(memory_space=pltpu.VMEM)
SMEM = pl.BlockSpec(memory_space=pltpu.SMEM)
FAR = pl.BlockSpec(memory_space=pltpu.HBM)


def call(kernel, outs, specs, scratch=(), scoped=SCOPED):
    grid_free = pl.pallas_call(
        kernel,
        out_shape=outs,
        in_specs=specs,
        out_specs=jax.tree.map(lambda _: VMEM, outs, is_leaf=lambda x: hasattr(x, "shape")),
        scratch_shapes=scratch,
        compiler_params=pltpu.CompilerParams(vmem_limit_bytes=scoped),
    )

    def run(*args):
        spaces = {id(NEAR): pltpu.VMEM, id(FAR): pltpu.HBM}
        placed = [
            pltpu.with_memory_space_constraint(arg, spaces[id(spec)]) if id(spec) in spaces else arg
            for arg, spec in zip(args, specs)
        ]
        return grid_free(*placed)

    return run


def shape(dims, kind):
    return jax.ShapeDtypeStruct(dims, kind)


def near(dims, kind):
    return pltpu.VMEM(dims, kind)


def silu(x):
    return x * jax.nn.sigmoid(x)


def pieces(value, parts):
    out = []
    for _ in range(parts):
        piece = value.astype(bf16).astype(f32)
        out.append(piece)
        value = value - piece
    return out


def marked(value, parts, first=0):
    lane = lax.broadcasted_iota(jnp.int32, (value.shape[0], LANES), 1)
    out = jnp.zeros((value.shape[0], LANES), f32)
    for k, piece in enumerate(pieces(value, parts)):
        out = jnp.where(lane == first + k, piece, out)
    return out


def summed(marks, first=0):
    return marks[:, first : first + 1] + marks[:, first + 1 : first + 2]


def convolve(state_ref, fresh, taps_ref):
    taps = state_ref.shape[0]
    total = taps_ref[taps : taps + 1, :] * fresh + taps_ref[taps + 1 : taps + 2, :]
    for k in range(taps):
        total = total + taps_ref[k : k + 1, :] * state_ref[k].astype(f32)
    return silu(total)


def fetch_all(pairs, sems):
    copies = [
        pltpu.make_async_copy(source, target, sems.at[k])
        for k, (source, target) in enumerate(pairs)
    ]
    for copy in copies:
        copy.start()
    return copies


def group_kernel(
    hidden_far,
    gain_far,
    weights_far,
    state_far,
    taps_far,
    group_out,
    normed_out,
    hidden,
    gain,
    weights,
    state,
    taps,
    sems,
):
    depth = weights.shape[0] // BLOCKS
    rows = [pl.ds(k * depth, depth) for k in range(BLOCKS)]
    copies = fetch_all(
        [(hidden_far, hidden), (gain_far, gain)]
        + [(weights_far.at[r], weights.at[r]) for r in rows]
        + [(state_far, state), (taps_far, taps)],
        sems,
    )
    copies[0].wait()
    copies[1].wait()
    stream = hidden[...].astype(f32)
    mean = jnp.mean(stream * stream, axis=-1, keepdims=True)
    normed_out[...] = (stream * lax.rsqrt(mean + epsilon) * gain[...]).astype(bf16)
    raw = jnp.zeros(group_out.shape, f32)
    for k in range(BLOCKS):
        copies[2 + k].wait()
        span = slice(k * depth, (k + 1) * depth)
        raw = raw + jnp.dot(normed_out[:, span], weights[span, :], preferred_element_type=f32)
    copies[-2].wait()
    copies[-1].wait()
    group_out[...] = convolve(state, raw, taps).astype(bf16)


def gate_kernel(carried, position, normed_ref, *refs):
    weights_far, step_far, state_far, taps_far, numbers, hidden_far = refs[:6]
    inputs, outputs, scratch = refs[6 : 6 + carried], refs[6 + carried : -5], refs[-5:]
    gate_out, conv_out, step_out, decay_out, columns_out = outputs[:5]
    weights, step_row, state, taps, sems = scratch
    columns = columns_out.shape[1]
    start = pl.multiple_of(position[0] * columns, columns)
    depth = weights.shape[0] // BLOCKS
    rows = [pl.ds(k * depth, depth) for k in range(BLOCKS)]
    copies = fetch_all(
        [(weights_far.at[r], weights.at[r]) for r in rows]
        + [
            (step_far, step_row),
            (state_far, state),
            (taps_far, taps),
            (hidden_far.at[:, pl.ds(start, columns)], columns_out),
        ]
        + list(zip(inputs, outputs[5:])),
        sems,
    )
    half = gate_out.shape[1]
    both = jnp.zeros((gate_out.shape[0], weights.shape[1]), f32)
    for k in range(BLOCKS):
        copies[k].wait()
        span = slice(k * depth, (k + 1) * depth)
        both = both + jnp.dot(normed_ref[:, span], weights[span, :], preferred_element_type=f32)
    for copy in copies[BLOCKS : BLOCKS + 3]:
        copy.wait()
    gate_out[...] = silu(both[:, :half])
    fresh = convolve(state, both[:, half:], taps)
    conv_out[:, :half] = fresh
    conv_out[:, half:] = numbers[:, 2:3] * fresh
    raw = jnp.sum(normed_ref[...].astype(f32) * step_row[...].astype(f32), axis=-1, keepdims=True)
    step = jax.nn.softplus(raw + numbers[:, 1:2])
    step_out[...] = jnp.broadcast_to(step, step_out.shape)
    decay_out[...] = jnp.broadcast_to(jnp.exp(-numbers[:, 0:1] * step), decay_out.shape)
    for copy in copies[BLOCKS + 3 :]:
        copy.wait()


def chosen(position, own, other):
    first = position[0] < GROUPS
    mine, theirs = own[...].astype(f32), other[...].astype(f32)
    return jnp.where(first, mine, theirs), jnp.where(first, theirs, mine)


def mixer_kernel(position, own, other, gate, conv, step, decay, state, weights, gain, sent):
    requests = own.shape[0]
    inject, readout = chosen(position, own, other)
    half = gate.shape[1]
    both = 2 * half
    flat = state[...].reshape(requests * half, state.shape[2])
    high = flat.astype(bf16)
    low = (flat - high.astype(f32)).astype(bf16)
    vectors = readout.astype(bf16)
    full = sum(
        lax.dot_general(
            vectors, term, (((1,), (1,)), ((), ())), preferred_element_type=f32
        )
        for term in (high, low)
    )
    row = lax.broadcasted_iota(jnp.int32, (requests, both), 0)
    pairs = jnp.zeros((requests, both), f32)
    for k in range(requests // 2):
        pairs = jnp.where(row // 2 == k, full[:, k * both : (k + 1) * both], pairs)
    read = jnp.where(row[:, :half] % 2 == 0, pairs[:, :half], pairs[:, half:])
    along = jnp.sum(inject * readout, axis=-1, keepdims=True)
    fresh = conv[:, :half]
    out = decay[:, :1] * read + step[:, :1] * fresh * along + conv[:, half:]
    gated = out * gate[...]
    marks = marked(jnp.sum(gated * gated, axis=-1, keepdims=True), 2).astype(bf16)
    weighted = (gated * gain[...]).astype(bf16)
    count = sent.shape[0]
    columns = weights.shape[1] // count
    for e in range(count):
        product = jnp.dot(
            weighted, weights[:, e * columns : (e + 1) * columns], preferred_element_type=f32
        )
        sent[e, :, :columns] = product.astype(bf16)
        sent[e, :, columns:] = marks


def state_kernel(position, own, other, conv, step, decay, state, new_state):
    inject, _ = chosen(position, own, other)
    fresh = step[:, :1] * conv[:, : state.shape[1]]
    new_state[...] = (
        decay[:, :1][:, :, None] * state[...] + fresh[:, :, None] * inject[:, None, :]
    )


def project_kernel(
    chunks, head_width, position, received, hidden, gain, weights, table, keep, give, middle_out
):
    count, requests, _ = received.shape
    columns = weights.shape[0]
    squares = [received[k, :, columns:].astype(f32) for k in range(count)]
    mixer = jnp.zeros((requests, columns), f32)
    for g in range(GROUPS):
        members = range(g, count, GROUPS)
        marks = sum(squares[k] for k in members)
        total = marks[:, :1] + marks[:, 1:2]
        scale = lax.rsqrt(total / (len(members) * head_width) + epsilon)
        products = sum(received[k, :, :columns].astype(f32) for k in members)
        mixer = mixer + scale * products
    middle = (hidden[...].astype(f32) + mixer).astype(bf16).astype(f32)
    middle_out[...] = middle
    square = jnp.sum(middle * middle, axis=-1, keepdims=True)
    scaled = middle * gain[...]
    extended = jnp.concatenate([scaled, marked(square, 2)], axis=-1).astype(bf16)
    rows = count * SUB
    pages = SUB // chunks
    chips = count // 2
    core = position[0] % 2
    index = lax.broadcasted_iota(jnp.int32, (rows, requests), 0)
    line = index % (chips * SUB)
    parity = jnp.where(index < chips * SUB, core, 1 - core)
    page = ((line // SUB) * 2 + parity) * pages + index % pages
    hits = page == table[0:1, :]
    for j in range(1, table.shape[0]):
        hits = jnp.logical_or(hits, page == table[j : j + 1, :])
    onehot = jnp.where(hits, 1.0, 0.0).astype(bf16)
    spread = jnp.dot(onehot, extended, preferred_element_type=f32)
    lines = spread[:, :columns]
    which = (lax.broadcasted_iota(jnp.int32, lines.shape, 0) % SUB) // pages
    chunk = weights.shape[1] // chunks
    fresh_from = QH * HD
    zeros = jnp.zeros((SUB, columns), f32)
    lhs = []
    for c in range(chunks):
        own = jnp.where(which == c, lines, 0.0)
        if (c + 1) * chunk > fresh_from:
            own = jnp.concatenate([own, scaled, zeros], axis=0)
        lhs.append(own.astype(bf16))
    tile = 2 * HD
    for n in range(0, chunk, tile):
        total = None
        for c in range(chunks):
            first = c * chunk + n
            part = jnp.dot(lhs[c], weights[:, first : first + tile], preferred_element_type=f32)
            if first >= fresh_from:
                fresh = part[rows : rows + SUB]
                chip = (first - fresh_from) // tile
                low, high = fresh[:, :HD], fresh[:, HD:]
                keep[chip, :, chunk + LANES :] = jnp.where(core == 0, low, high)
                give[chip, :, chunk + LANES :] = jnp.where(core == 0, high, low).astype(bf16)
            total = part[:rows] if total is None else total + part[:rows]
        for e in range(chips):
            keep[e, :, n : n + tile] = total[e * SUB : (e + 1) * SUB]
            first = (chips + e) * SUB
            give[e, :, n : n + tile] = total[first : first + SUB].astype(bf16)
    marks = spread[:, columns:]
    request_marks = marked(square, 2, 2)
    for e in range(chips):
        keep[e, :, chunk : chunk + LANES] = marks[e * SUB : (e + 1) * SUB] + request_marks
        first = (chips + e) * SUB
        give[e, :, chunk : chunk + LANES] = (marks[first : first + SUB] + request_marks).astype(
            bf16
        )


def pair_kernel(keep, taken, _, sent):
    chunk = keep.shape[2] - 2 * LANES
    for e in range(keep.shape[0]):
        total = keep[e] + taken[e].astype(f32)
        marks = total[:, chunk : chunk + LANES]
        sent[e, :, :chunk] = total[:, :chunk].astype(bf16)
        sent[e, :, chunk : chunk + LANES] = (
            marked(summed(marks), 2) + marked(summed(marks, 2), 2, 2)
        ).astype(bf16)
        sent[e, :, chunk + LANES :] = total[:, chunk + LANES :].astype(bf16)


def attend_kernel(width, position, received, cache, table, lengths, sent, lines):
    count, _, full = received.shape
    pages, page_len, _ = cache.shape
    chunks = SUB // pages
    chunk = full - 2 * LANES
    tiles = chunk // HD
    total = received[0].astype(f32)
    for k in range(1, count):
        total = total + received[k].astype(f32)
    marks = total[:, chunk : chunk + LANES]
    inverse = lax.rsqrt(summed(marks) / width + epsilon)
    fresh = total[:, chunk + LANES :] * lax.rsqrt(summed(marks, 2) / width + epsilon)
    fresh = fresh.astype(bf16)
    for t in range(tiles):
        lines[t * SUB : (t + 1) * SUB, :] = (
            (total[:, t * HD : (t + 1) * HD] * inverse).astype(bf16).astype(f32)
        )

    def heads(page, first, many):
        start = (first % tiles) * SUB + (first // tiles) * pages + page
        return lines[pl.ds(start, many, stride=SUB), :]

    group = QH // KVH
    scale = 1.0 / HD**0.5
    lane = lax.broadcasted_iota(jnp.int32, (1, page_len), 1)
    head_group = lax.broadcasted_iota(jnp.int32, (QH, HD), 0) // group
    eye = lax.broadcasted_iota(jnp.int32, (QH, LANES), 0)
    value_rows = pages * QH
    place = (position[0] // 2) % (LANES // value_rows) * value_rows
    eye_lane = lax.broadcasted_iota(jnp.int32, (QH, LANES), 1) - place
    order = lax.broadcasted_iota(jnp.int32, table.shape, 0)
    log_row = jnp.zeros((1, LANES), f32)
    for p in range(pages):
        slot = position[0] * pages + p
        hit = table[...] == slot
        logical = jnp.sum(jnp.where(hit, order, 0), axis=(0, 1), keepdims=True)
        length = jnp.sum(
            jnp.where(hit, jnp.broadcast_to(lengths[...], hit.shape), 0),
            axis=(0, 1),
            keepdims=True,
        )
        live = logical * page_len + lane < length
        leads = logical == 0
        query = jnp.concatenate([heads(p, g * group, group) for g in range(KVH)], axis=0)
        keys = [heads(p, QH + g, 1) for g in range(KVH)]
        values = [heads(p, QH + KVH + g, 1) for g in range(KVH)]
        key_rows = jnp.concatenate([jnp.broadcast_to(k, (group, HD)) for k in keys], axis=0)
        value_own = jnp.concatenate([jnp.broadcast_to(v, (group, HD)) for v in values], axis=0)
        spread = jnp.concatenate(
            [jnp.where(head_group == g, query, 0.0).astype(bf16) for g in range(KVH)], axis=-1
        )
        scores = (
            lax.dot_general(
                spread,
                cache[p, :, : KVH * HD],
                (((1,), (1,)), ((), ())),
                preferred_element_type=f32,
            )
            * scale
        )
        own = jnp.sum(query * key_rows, axis=-1, keepdims=True) * scale
        masked = jnp.where(live, scores, lowest)
        own = jnp.where(leads, own, lowest)
        peak = jnp.maximum(jnp.max(masked, axis=-1, keepdims=True), own)
        weights = jnp.where(live, jnp.exp(masked - peak), 0.0)
        own_weight = jnp.where(leads, jnp.exp(own - peak), 0.0)
        mass = jnp.sum(weights, axis=-1, keepdims=True) + own_weight
        wide = jnp.dot(
            weights.astype(bf16), cache[p, :, KVH * HD :], preferred_element_type=f32
        )
        mixed = own_weight * value_own
        for g in range(KVH):
            mixed = mixed + jnp.where(head_group == g, wide[:, g * HD : (g + 1) * HD], 0.0)
        some = mass > 0.0
        safe = jnp.where(some, mass, 1.0)
        result = (mixed / safe).astype(bf16)
        logs = jnp.where(some, peak + jnp.log(safe), lowest)
        log_row = log_row + jnp.sum(
            jnp.where(eye_lane == eye + p * QH, logs, 0.0), axis=0, keepdims=True
        )
        for e in range(count):
            sent[e, p * QH : (p + 1) * QH, :] = result
    terms = pieces(log_row, PARTS) + [jnp.zeros((SUB - PARTS, LANES), f32)]
    terms = jnp.concatenate(terms, axis=0).astype(bf16)
    for e in range(count):
        sent[e, value_rows : value_rows + SUB, :] = fresh
        sent[e, value_rows + SUB :, :] = terms


def owner_kernel(chips, pages, position, table, _, owner):
    pages_req, requests = table.shape
    core = position[0] % 2
    span = pages * QH
    rows_each = owner.shape[0] // 2
    row = lax.broadcasted_iota(jnp.int32, owner.shape, 0)
    lane = lax.broadcasted_iota(jnp.int32, owner.shape, 1)
    chip = (row % rows_each) * (LANES // span) + lane // span
    parity = jnp.where(row < rows_each, core, 1 - core)
    page = (chip * 2 + parity) * pages + (lane % span) // QH
    found = jnp.zeros(owner.shape, jnp.int32)
    for r in range(requests):
        for j in range(pages_req):
            found = jnp.where(page == table[j, r], r, found)
    owner[...] = found


def merge_kernel(pages, position, near_ref, far_ref, owner, weights, middle, final, new_kv):
    chips = near_ref.shape[0]
    requests, width = middle.shape
    value_rows = pages * QH
    core = position[0] % 2
    packages = (near_ref, far_ref)
    for chip in range(chips):
        mine, theirs = (ref[chip, value_rows : value_rows + SUB, :].astype(f32) for ref in packages)
        first = 2 * chip * HD
        new_kv[:, first : first + HD] = jnp.where(core == 0, mine, theirs).astype(bf16)
        new_kv[:, first + HD : first + 2 * HD] = jnp.where(core == 0, theirs, mine).astype(bf16)
    each = LANES // value_rows
    request = lax.broadcasted_iota(jnp.int32, (requests, LANES), 0)
    lane = lax.broadcasted_iota(jnp.int32, (requests, LANES), 1)
    logs, hits = [], []
    for ref in packages:
        for chip in range(0, chips, each):
            terms = sum(ref[chip + k, value_rows + SUB :, :].astype(f32) for k in range(each))
            log = sum(terms[k : k + 1, :] for k in range(PARTS))
            logs.append(jnp.broadcast_to(log, (requests, LANES)))
            row = len(hits)
            hits.append(jnp.broadcast_to(owner[row : row + 1, :], (requests, LANES)) == request)

    def over_pages(value, combine):
        out = value
        for k in range(QH, LANES, QH):
            out = combine(out, pltpu.roll(value, k, 1))
        return out

    tops = functools.reduce(
        jnp.maximum, [jnp.where(hit, log, lowest) for hit, log in zip(hits, logs)]
    )
    tops = over_pages(tops, jnp.maximum)
    factors = [jnp.where(hit, jnp.exp(log - tops), 0.0) for hit, log in zip(hits, logs)]
    inverse = 1.0 / over_pages(functools.reduce(jnp.add, factors), jnp.add)
    shares = []
    for factor in factors:
        share = factor * inverse
        heads = [jnp.where(lane % QH == h, share, 0.0) for h in range(QH)]
        shares.append(jnp.concatenate(heads, axis=0).astype(bf16))
    half = len(shares) // 2
    mixed = None
    for side, ref in enumerate(packages):
        part = jnp.dot(
            jnp.concatenate(shares[side * half : (side + 1) * half], axis=1),
            jnp.concatenate([ref[chip, :value_rows, :] for chip in range(chips)], axis=0),
            preferred_element_type=f32,
        )
        mixed = part if mixed is None else mixed + part
    attended = jnp.concatenate(
        [mixed[h * requests : (h + 1) * requests] for h in range(QH)], axis=1
    ).astype(bf16)
    total = jnp.dot(attended, weights[...], preferred_element_type=f32)
    final[...] = (middle[...] + total).astype(bf16)


def fused_shards(
    hidden,
    mix_gain,
    in_gate_input,
    in_step,
    in_groups,
    conv_input,
    conv_groups,
    taps_input,
    taps_groups,
    decay_rate,
    step_bias,
    skip_gain,
    norm_gain,
    out_mixer,
    ssm_state,
    attn_gain,
    w_qkv,
    w_out,
    kv_cache,
    page_table,
    lengths,
):
    count = lax.axis_size("seq")
    position = lax.axis_index("seq").astype(jnp.int32).reshape(1)
    requests, width = hidden.shape
    columns = width // count
    head_width = in_gate_input.shape[1] // 2
    pages = kv_cache.shape[0]
    chunks = SUB // pages
    chips = count // 2
    gcols = in_groups.shape[1]
    state = ssm_state.reshape(requests, head_width, STATE)
    same_core = [list(range(core, count, 2)) for core in range(2)]
    cores = [(i, i ^ 1) for i in range(count)]
    group_args = (
        hidden,
        mix_gain.reshape(1, width),
        in_groups,
        conv_groups.transpose(1, 0, 2),
        taps_groups,
    )
    group_conv, normed = call(
        group_kernel,
        (near((requests, gcols), bf16), near((requests, width), bf16)),
        [FAR] * 5,
        [pltpu.VMEM(x.shape, x.dtype) for x in group_args]
        + [pltpu.SemaphoreType.DMA((len(group_args) - 1 + BLOCKS,))],
        MOST,
    )(*group_args)
    swap = [(i, (i + GROUPS) % count) for i in range(count)]
    other = lax.ppermute(group_conv, "seq", swap)
    carried = (
        state,
        out_mixer,
        norm_gain.reshape(1, head_width),
        attn_gain.reshape(1, columns),
        page_table.T,
        lengths.reshape(1, requests),
    )
    gate_args = (
        in_gate_input,
        in_step.T,
        conv_input.transpose(1, 0, 2),
        taps_input,
    )
    numbers = jnp.concatenate([decay_rate, step_bias, skip_gain]).reshape(1, 3)
    gate, conv, step, decay, stream, state_in, mixer, gain, scale, table, spans = call(
        functools.partial(gate_kernel, len(carried)),
        (
            near((requests, head_width), f32),
            near((requests, 2 * head_width), f32),
            near((requests, LANES), f32),
            near((requests, LANES), f32),
            near((requests, columns), bf16),
        )
        + tuple(near(x.shape, x.dtype) for x in carried),
        [SMEM, NEAR] + [FAR] * 4 + [NEAR] + [FAR] * (1 + len(carried)),
        [pltpu.VMEM(x.shape, x.dtype) for x in gate_args]
        + [pltpu.SemaphoreType.DMA((BLOCKS + 4 + len(carried),))],
    )(position, normed, *gate_args, numbers, hidden, *carried)
    sent = call(
        mixer_kernel,
        near((count, requests, columns + LANES), bf16),
        [SMEM] + [NEAR] * 9,
    )(position, group_conv, other, gate, conv, step, decay, state_in, mixer, gain)
    received = lax.all_to_all(sent, "seq", 0, 0)
    new_state = call(state_kernel, shape(state.shape, f32), [SMEM] + [NEAR] * 6)(
        position, group_conv, other, conv, step, decay, state_in
    )
    chunk = w_qkv.shape[1] // chunks
    keep, give, middle = call(
        functools.partial(project_kernel, chunks, head_width),
        (
            near((chips, SUB, chunk + 2 * LANES), f32),
            near((chips, SUB, chunk + 2 * LANES), bf16),
            near((requests, columns), f32),
        ),
        [SMEM] + [NEAR] * 5,
    )(position, received, stream, scale, w_qkv, table)
    taken = lax.ppermute(give, "seq", cores)
    sent = call(pair_kernel, near(give.shape, bf16), [NEAR] * 2 + [FAR])(keep, taken, new_state)
    received = lax.all_to_all(sent, "seq", 0, 0, axis_index_groups=same_core)
    package = pages * QH + 2 * SUB
    sent = call(
        functools.partial(attend_kernel, width),
        near((chips, package, HD), bf16),
        [SMEM] + [NEAR] * 4,
        [pltpu.VMEM((chunk // HD * SUB, HD), f32)],
    )(position, received, kv_cache, table, spans)
    received = lax.all_to_all(sent, "seq", 0, 0, axis_index_groups=same_core)
    far = lax.ppermute(received, "seq", cores)
    owner_rows = count * pages * QH // LANES
    owner = call(
        functools.partial(owner_kernel, chips, pages),
        near((owner_rows, LANES), jnp.int32),
        [SMEM] * 2 + [NEAR],
    )(position, page_table.T, received)
    final, new_kv = call(
        functools.partial(merge_kernel, pages),
        (
            shape((requests, columns), bf16),
            shape((requests, 2 * KVH * HD), bf16),
        ),
        [SMEM] + [NEAR] * 5,
    )(position, received, far, owner, w_out, middle)
    return (final, new_state.reshape(ssm_state.shape), new_kv)


def shards(*args):
    hidden, in_step, in_groups = args[0], args[3], args[4]
    kv_cache, page_table = args[18], args[19]
    count = lax.axis_size("seq")
    whole_tiles = (
        in_step.shape[1] == 1
        and in_groups.shape[1] == STATE
        and count == 2 * GROUPS
        and hidden.shape[0] == SUB
        and (hidden.shape[1] // count) % LANES == 0
        and SUB % kv_cache.shape[0] == 0
        and LANES % (kv_cache.shape[0] * QH) == 0
        and (count // 2) % (LANES // (kv_cache.shape[0] * QH)) == 0
        and kv_cache.shape[1] == LANES
        and 2 * KVH == count
    )
    return (fused_shards if whole_tiles else plain_shards)(*args)


def solution(mesh):
    placed = (
        P("grp", None),
        P(),
        P(None, "seq"),
        P(None, "seq"),
        P(None, "seq"),
        P("grp", None, "seq"),
        P("grp", None, "seq"),
        P(None, "seq"),
        P(None, "seq"),
        P("seq"),
        P("seq"),
        P("seq"),
        P("seq"),
        P("seq", None),
        P("grp", "seq", None, None),
        P("seq"),
        P("seq", None),
        P(None, "seq"),
        P(("grp", "seq"), None, None),
        P("grp", None),
        P("grp"),
    )
    return jax.shard_map(
        shards,
        mesh=mesh,
        in_specs=placed,
        out_specs=(P("grp", "seq"), P("grp", "seq", None, None), P("grp", None)),
        check_vma=False,
    )
```

```python
import functools

import jax
import jax.numpy as jnp
from jax import lax
from jax.experimental import pallas as pl
from jax.experimental.pallas import tpu as pltpu
from jax.sharding import PartitionSpec as P

QH = 32
KVH = 8
HD = 128
STATE = 128
GROUPS = 8
LANES = 128

epsilon = 1e-05
lowest = -1e30


def conv_step(state, fresh, taps):
    window = jnp.concatenate([state.astype(jnp.float32), fresh[:, None, :]], axis=1)
    summed = jnp.sum(window * taps[:-1][None], axis=1) + taps[-1][None]
    return jax.nn.silu(summed)


def split(value, parts):
    pieces = []
    rest = value
    for _ in range(parts):
        piece = lax.reduce_precision(rest, 8, 7)
        pieces.append(piece.astype(jnp.bfloat16))
        rest = rest - piece
    return pieces


def group_vectors(group_conv, heads_here, requests):
    count = lax.axis_size("seq")
    position = lax.axis_index("seq")
    if heads_here == 1 and group_conv.shape[1] == STATE and count == 2 * GROUPS:
        swap = [(i, (i + GROUPS) % count) for i in range(count)]
        other = lax.ppermute(group_conv, "seq", swap)
        first = position < GROUPS
        inject = jnp.where(first, group_conv, other)
        readout = jnp.where(first, other, group_conv)
        return (
            inject.astype(jnp.float32)[:, None, :],
            readout.astype(jnp.float32)[:, None, :],
        )
    group_all = lax.all_gather(group_conv, "seq", axis=1, tiled=True).astype(jnp.float32)
    inject = group_all[:, : GROUPS * STATE].reshape(requests, GROUPS, STATE)
    readout = group_all[:, GROUPS * STATE :].reshape(requests, GROUPS, STATE)
    head_ids = position * heads_here + jnp.arange(heads_here, dtype=jnp.int32)
    return inject[:, head_ids % GROUPS], readout[:, head_ids % GROUPS]


def plain_shards(
    hidden,
    mix_gain,
    in_gate_input,
    in_step,
    in_groups,
    conv_input,
    conv_groups,
    taps_input,
    taps_groups,
    decay_rate,
    step_bias,
    skip_gain,
    norm_gain,
    out_mixer,
    ssm_state,
    attn_gain,
    w_qkv,
    w_out,
    kv_cache,
    page_table,
    lengths,
):
    count_seq = lax.axis_size("seq")
    position = lax.axis_index("seq")
    requests = hidden.shape[0]
    width = hidden.shape[1]
    heads_here = in_step.shape[1]
    head_width = in_gate_input.shape[1] // (2 * heads_here)
    heads_total = heads_here * count_seq
    per_group = heads_total // GROUPS
    columns = width // count_seq
    stream = hidden.astype(jnp.float32)
    normed = (
        stream * lax.rsqrt(jnp.mean(stream * stream, axis=-1, keepdims=True) + epsilon) * mix_gain
    ).astype(jnp.bfloat16)
    group_raw = jnp.dot(normed, in_groups, preferred_element_type=jnp.float32)
    group_conv = conv_step(conv_groups, group_raw, taps_groups).astype(jnp.bfloat16)
    inject_heads, readout_heads = group_vectors(group_conv, heads_here, requests)
    gate_input = jnp.dot(normed, in_gate_input, preferred_element_type=jnp.float32).reshape(
        requests, heads_here, 2, head_width
    )
    gate_part = gate_input[:, :, 0]
    input_part = gate_input[:, :, 1].reshape(requests, heads_here * head_width)
    step_raw = jnp.dot(normed, in_step, preferred_element_type=jnp.float32)
    conv_out = conv_step(conv_input, input_part, taps_input).reshape(
        requests, heads_here, head_width
    )
    step_size = jax.nn.softplus(step_raw + step_bias)
    decay = jnp.exp(-decay_rate * step_size)
    new_state = (
        decay[:, :, None, None] * ssm_state
        + (step_size[:, :, None] * conv_out)[:, :, :, None] * inject_heads[:, :, None, :]
    )
    ssm_out = (
        jnp.sum(new_state * readout_heads[:, :, None, :], axis=-1)
        + skip_gain[None, :, None] * conv_out
    )
    gated = ssm_out * jax.nn.silu(gate_part)
    head_squares = jnp.sum(gated * gated, axis=-1)
    weighted = (gated * norm_gain.reshape(heads_here, head_width)).astype(jnp.bfloat16)
    products = jnp.einsum(
        "rhp,hpd->hrd",
        weighted,
        out_mixer.reshape(heads_here, head_width, width),
        preferred_element_type=jnp.float32,
    ).astype(jnp.bfloat16)
    products = products.reshape(heads_here, requests, count_seq, columns).transpose(2, 0, 1, 3)
    marks = jnp.stack(split(head_squares.T, 2), axis=-1)
    marks = jnp.pad(marks, ((0, 0), (0, 0), (0, LANES - 2)))
    marks = jnp.broadcast_to(marks[None], (count_seq,) + marks.shape)
    received = lax.all_to_all(jnp.concatenate([products, marks], axis=-1), "seq", 0, 0)
    received = received.astype(jnp.float32)
    squares = (received[..., columns] + received[..., columns + 1]).reshape(
        per_group, GROUPS, requests
    )
    scales = lax.rsqrt(jnp.sum(squares, axis=0) / (per_group * head_width) + epsilon)
    mixer = jnp.sum(
        received[..., :columns].reshape(per_group, GROUPS, requests, columns)
        * scales[None, :, :, None],
        axis=(0, 1),
    )
    stream_cols = lax.dynamic_slice_in_dim(stream, position * columns, columns, 1)
    middle = (stream_cols + mixer).astype(jnp.bfloat16)
    middle_f = middle.astype(jnp.float32)
    scaled = (middle_f * attn_gain).astype(jnp.bfloat16)
    partial_sq = jnp.sum(middle_f * middle_f, axis=-1)
    pages_here = kv_cache.shape[0]
    page_len = kv_cache.shape[1]
    pages_req = page_table.shape[1]
    pages_all = pages_here * count_seq
    matches = page_table[None, :, :] == jnp.arange(pages_all, dtype=jnp.int32)[:, None, None]
    owner = jnp.any(matches, axis=2)
    page_rows = jnp.dot(
        owner.astype(jnp.bfloat16), scaled, preferred_element_type=jnp.float32
    ).astype(jnp.bfloat16)
    page_proj = jnp.dot(page_rows, w_qkv, preferred_element_type=jnp.float32).astype(jnp.bfloat16)
    page_sq = jnp.sum(jnp.where(owner, partial_sq[None, :], 0.0), axis=1)
    sq_parts = jnp.pad(jnp.stack(split(page_sq, 2), axis=-1), ((0, 0), (0, LANES - 2)))
    sent = jnp.concatenate([page_proj, sq_parts], axis=-1).reshape(count_seq, pages_here, -1)
    arrived = jnp.sum(lax.all_to_all(sent, "seq", 0, 0).astype(jnp.float32), axis=0)
    qkv_width = w_qkv.shape[1]
    total_sq = arrived[:, qkv_width] + arrived[:, qkv_width + 1]
    qkv = (arrived[:, :qkv_width] * lax.rsqrt(total_sq / width + epsilon)[:, None]).astype(
        jnp.bfloat16
    )
    group_size = QH // KVH
    queries = qkv[:, : QH * HD].reshape(pages_here, KVH, group_size, HD)
    fresh_kv = qkv[:, QH * HD :]
    fresh_keys = fresh_kv[:, : KVH * HD].reshape(pages_here, KVH, 1, HD).astype(jnp.float32)
    fresh_values = fresh_kv[:, KVH * HD :].reshape(pages_here, KVH, 1, HD).astype(jnp.float32)
    scale = 1.0 / HD**0.5
    slots = position * pages_here + jnp.arange(pages_here, dtype=jnp.int32)
    own_matches = page_table[None, :, :] == slots[:, None, None]
    logical = jnp.sum(
        jnp.any(own_matches, axis=1) * jnp.arange(pages_req, dtype=jnp.int32)[None, :], axis=1
    )
    page_length = jnp.sum(jnp.where(jnp.any(own_matches, axis=2), lengths[None, :], 0), axis=1)
    token_pos = logical[:, None] * page_len + jnp.arange(page_len, dtype=jnp.int32)[None, :]
    live = (token_pos < page_length[:, None])[:, None, None, :]
    leads = (logical == 0)[:, None, None]
    cached = kv_cache.reshape(pages_here, page_len, 2, KVH, HD)
    scores = (
        jnp.einsum("pgjd,ptgd->pgjt", queries, cached[:, :, 0], preferred_element_type=jnp.float32)
        * scale
    )
    own = jnp.sum(queries.astype(jnp.float32) * fresh_keys, axis=-1) * scale
    masked = jnp.where(live, scores, lowest)
    own = jnp.where(leads, own, lowest)
    peak = jnp.maximum(jnp.max(masked, axis=-1), own)
    weights = jnp.where(live, jnp.exp(masked - peak[..., None]), 0.0)
    own_weight = jnp.where(leads, jnp.exp(own - peak), 0.0)
    total = jnp.sum(weights, axis=-1) + own_weight
    values = jnp.einsum(
        "pgjt,ptgd->pgjd",
        weights.astype(jnp.bfloat16),
        cached[:, :, 1],
        preferred_element_type=jnp.float32,
    )
    values = values + own_weight[..., None] * fresh_values
    some = total > 0.0
    safe = jnp.where(some, total, 1.0)
    values = (values / safe[..., None]).astype(jnp.bfloat16)
    logsum = jnp.where(some, peak + jnp.log(safe), lowest)
    logs = jnp.concatenate(split(logsum.reshape(1, pages_here * QH), 3), axis=0)
    logs = jnp.pad(logs, ((0, 5), (0, LANES - pages_here * QH)))
    value_rows = pages_here * QH
    kv_rows = pages_here * 2 * KVH
    package = jnp.concatenate(
        [values.reshape(value_rows, HD), fresh_kv.reshape(kv_rows, HD), logs], axis=0
    )
    package = jnp.broadcast_to(package[None], (count_seq,) + package.shape)
    everything = lax.all_to_all(package, "seq", 0, 0)
    all_values = everything[:, :value_rows].reshape(pages_all, QH, HD)
    all_kv = everything[:, value_rows : value_rows + kv_rows].reshape(pages_all, 2 * KVH * HD)
    all_logs = everything[:, value_rows + kv_rows :, : pages_here * QH].astype(jnp.float32)
    all_logs = (all_logs[:, 0] + all_logs[:, 1] + all_logs[:, 2]).reshape(pages_all, QH)
    new_kv = all_kv[page_table[:, 0]]
    req_logs = all_logs[page_table]
    top = jnp.max(req_logs, axis=1, keepdims=True)
    factors = jnp.exp(req_logs - top)
    summed = jnp.sum(factors[..., None] * all_values[page_table].astype(jnp.float32), axis=1)
    attended = (summed / jnp.sum(factors, axis=1)[..., None]).astype(jnp.bfloat16)
    final = (
        middle_f
        + jnp.dot(
            attended.reshape(requests, QH * HD), w_out, preferred_element_type=jnp.float32
        )
    ).astype(jnp.bfloat16)
    return (final, new_state, new_kv)


f32 = jnp.float32
bf16 = jnp.bfloat16
SUB = 8
PARTS = 3
SCOPED = 16 << 20
MOST = 63500 << 10
BLOCKS = 2
VMEM = pl.BlockSpec(memory_space=pltpu.VMEM)
NEAR = pl.BlockSpec(memory_space=pltpu.VMEM)
SMEM = pl.BlockSpec(memory_space=pltpu.SMEM)
FAR = pl.BlockSpec(memory_space=pltpu.HBM)


def call(kernel, outs, specs, scratch=(), scoped=SCOPED):
    grid_free = pl.pallas_call(
        kernel,
        out_shape=outs,
        in_specs=specs,
        out_specs=jax.tree.map(lambda _: VMEM, outs, is_leaf=lambda x: hasattr(x, "shape")),
        scratch_shapes=scratch,
        compiler_params=pltpu.CompilerParams(vmem_limit_bytes=scoped),
    )

    def run(*args):
        spaces = {id(NEAR): pltpu.VMEM, id(FAR): pltpu.HBM}
        placed = [
            pltpu.with_memory_space_constraint(arg, spaces[id(spec)]) if id(spec) in spaces else arg
            for arg, spec in zip(args, specs)
        ]
        return grid_free(*placed)

    return run


def shape(dims, kind):
    return jax.ShapeDtypeStruct(dims, kind)


def near(dims, kind):
    return pltpu.VMEM(dims, kind)


def silu(x):
    return x * jax.nn.sigmoid(x)


def pieces(value, parts):
    out = []
    for _ in range(parts):
        piece = value.astype(bf16).astype(f32)
        out.append(piece)
        value = value - piece
    return out


def marked(value, parts, first=0):
    lane = lax.broadcasted_iota(jnp.int32, (value.shape[0], LANES), 1)
    out = jnp.zeros((value.shape[0], LANES), f32)
    for k, piece in enumerate(pieces(value, parts)):
        out = jnp.where(lane == first + k, piece, out)
    return out


def summed(marks, first=0):
    return marks[:, first : first + 1] + marks[:, first + 1 : first + 2]


def convolve(state_ref, fresh, taps_ref):
    taps = state_ref.shape[0]
    total = taps_ref[taps : taps + 1, :] * fresh + taps_ref[taps + 1 : taps + 2, :]
    for k in range(taps):
        total = total + taps_ref[k : k + 1, :] * state_ref[k].astype(f32)
    return silu(total)


def fetch_all(pairs, sems):
    copies = [
        pltpu.make_async_copy(source, target, sems.at[k])
        for k, (source, target) in enumerate(pairs)
    ]
    for copy in copies:
        copy.start()
    return copies


def group_kernel(
    hidden_far,
    gain_far,
    weights_far,
    state_far,
    taps_far,
    group_out,
    normed_out,
    hidden,
    gain,
    weights,
    state,
    taps,
    sems,
):
    depth = weights.shape[0] // BLOCKS
    rows = [pl.ds(k * depth, depth) for k in range(BLOCKS)]
    copies = fetch_all(
        [(hidden_far, hidden), (gain_far, gain)]
        + [(weights_far.at[r], weights.at[r]) for r in rows]
        + [(state_far, state), (taps_far, taps)],
        sems,
    )
    copies[0].wait()
    copies[1].wait()
    stream = hidden[...].astype(f32)
    mean = jnp.mean(stream * stream, axis=-1, keepdims=True)
    normed_out[...] = (stream * lax.rsqrt(mean + epsilon) * gain[...]).astype(bf16)
    raw = jnp.zeros(group_out.shape, f32)
    for k in range(BLOCKS):
        copies[2 + k].wait()
        span = slice(k * depth, (k + 1) * depth)
        raw = raw + jnp.dot(normed_out[:, span], weights[span, :], preferred_element_type=f32)
    copies[-2].wait()
    copies[-1].wait()
    group_out[...] = convolve(state, raw, taps).astype(bf16)


def gate_kernel(carried, position, normed_ref, *refs):
    weights_far, step_far, state_far, taps_far, numbers, hidden_far = refs[:6]
    inputs, outputs, scratch = refs[6 : 6 + carried], refs[6 + carried : -5], refs[-5:]
    gate_out, conv_out, step_out, decay_out, columns_out = outputs[:5]
    weights, step_row, state, taps, sems = scratch
    columns = columns_out.shape[1]
    start = pl.multiple_of(position[0] * columns, columns)
    depth = weights.shape[0] // BLOCKS
    rows = [pl.ds(k * depth, depth) for k in range(BLOCKS)]
    copies = fetch_all(
        [(weights_far.at[r], weights.at[r]) for r in rows]
        + [
            (step_far, step_row),
            (state_far, state),
            (taps_far, taps),
            (hidden_far.at[:, pl.ds(start, columns)], columns_out),
        ]
        + list(zip(inputs, outputs[5:])),
        sems,
    )
    half = gate_out.shape[1]
    both = jnp.zeros((gate_out.shape[0], weights.shape[1]), f32)
    for k in range(BLOCKS):
        copies[k].wait()
        span = slice(k * depth, (k + 1) * depth)
        both = both + jnp.dot(normed_ref[:, span], weights[span, :], preferred_element_type=f32)
    for copy in copies[BLOCKS : BLOCKS + 3]:
        copy.wait()
    gate_out[...] = silu(both[:, :half])
    fresh = convolve(state, both[:, half:], taps)
    conv_out[:, :half] = fresh
    conv_out[:, half:] = numbers[:, 2:3] * fresh
    raw = jnp.sum(normed_ref[...].astype(f32) * step_row[...].astype(f32), axis=-1, keepdims=True)
    step = jax.nn.softplus(raw + numbers[:, 1:2])
    step_out[...] = jnp.broadcast_to(step, step_out.shape)
    decay_out[...] = jnp.broadcast_to(jnp.exp(-numbers[:, 0:1] * step), decay_out.shape)
    for copy in copies[BLOCKS + 3 :]:
        copy.wait()


def chosen(position, own, other):
    first = position[0] < GROUPS
    mine, theirs = own[...].astype(f32), other[...].astype(f32)
    return jnp.where(first, mine, theirs), jnp.where(first, theirs, mine)


def mixer_kernel(position, own, other, gate, conv, step, decay, state, weights, gain, sent):
    requests = own.shape[0]
    inject, readout = chosen(position, own, other)
    half = gate.shape[1]
    both = 2 * half
    flat = state[...].reshape(requests * half, state.shape[2])
    high = flat.astype(bf16)
    low = (flat - high.astype(f32)).astype(bf16)
    vectors = readout.astype(bf16)
    full = sum(
        lax.dot_general(
            vectors, term, (((1,), (1,)), ((), ())), preferred_element_type=f32
        )
        for term in (high, low)
    )
    row = lax.broadcasted_iota(jnp.int32, (requests, both), 0)
    pairs = jnp.zeros((requests, both), f32)
    for k in range(requests // 2):
        pairs = jnp.where(row // 2 == k, full[:, k * both : (k + 1) * both], pairs)
    read = jnp.where(row[:, :half] % 2 == 0, pairs[:, :half], pairs[:, half:])
    along = jnp.sum(inject * readout, axis=-1, keepdims=True)
    fresh = conv[:, :half]
    out = decay[:, :1] * read + step[:, :1] * fresh * along + conv[:, half:]
    gated = out * gate[...]
    marks = marked(jnp.sum(gated * gated, axis=-1, keepdims=True), 2).astype(bf16)
    weighted = (gated * gain[...]).astype(bf16)
    count = sent.shape[0]
    columns = weights.shape[1] // count
    for e in range(count):
        product = jnp.dot(
            weighted, weights[:, e * columns : (e + 1) * columns], preferred_element_type=f32
        )
        sent[e, :, :columns] = product.astype(bf16)
        sent[e, :, columns:] = marks


def state_kernel(position, own, other, conv, step, decay, state, new_state):
    inject, _ = chosen(position, own, other)
    fresh = step[:, :1] * conv[:, : state.shape[1]]
    new_state[...] = (
        decay[:, :1][:, :, None] * state[...] + fresh[:, :, None] * inject[:, None, :]
    )


def project_kernel(
    chunks, head_width, position, received, hidden, gain, weights, table, keep, give, middle_out
):
    count, requests, _ = received.shape
    columns = weights.shape[0]
    squares = [received[k, :, columns:].astype(f32) for k in range(count)]
    mixer = jnp.zeros((requests, columns), f32)
    for g in range(GROUPS):
        members = range(g, count, GROUPS)
        marks = sum(squares[k] for k in members)
        total = marks[:, :1] + marks[:, 1:2]
        scale = lax.rsqrt(total / (len(members) * head_width) + epsilon)
        products = sum(received[k, :, :columns].astype(f32) for k in members)
        mixer = mixer + scale * products
    middle = (hidden[...].astype(f32) + mixer).astype(bf16).astype(f32)
    middle_out[...] = middle
    square = jnp.sum(middle * middle, axis=-1, keepdims=True)
    scaled = middle * gain[...]
    extended = jnp.concatenate([scaled, marked(square, 2)], axis=-1).astype(bf16)
    rows = count * SUB
    pages = SUB // chunks
    chips = count // 2
    core = position[0] % 2
    index = lax.broadcasted_iota(jnp.int32, (rows, requests), 0)
    line = index % (chips * SUB)
    parity = jnp.where(index < chips * SUB, core, 1 - core)
    page = ((line // SUB) * 2 + parity) * pages + index % pages
    hits = page == table[0:1, :]
    for j in range(1, table.shape[0]):
        hits = jnp.logical_or(hits, page == table[j : j + 1, :])
    onehot = jnp.where(hits, 1.0, 0.0).astype(bf16)
    spread = jnp.dot(onehot, extended, preferred_element_type=f32)
    lines = spread[:, :columns]
    which = (lax.broadcasted_iota(jnp.int32, lines.shape, 0) % SUB) // pages
    fresh_from = QH * HD
    value_from = fresh_from + KVH * HD
    chunk = value_from // chunks
    plain = jnp.concatenate([scaled, jnp.zeros((SUB, columns), f32)], axis=0)
    lhs = []
    for c in range(chunks):
        own = jnp.where(which == c, lines, 0.0)
        if (c + 1) * chunk > fresh_from:
            own = jnp.concatenate([own, plain], axis=0)
        lhs.append(own.astype(bf16))
    tile = 2 * HD

    def share_out(first, fresh):
        chip = (first - fresh_from) // tile
        low, high = fresh[:, :HD], fresh[:, HD:]
        keep[chip, :, chunk + LANES :] = jnp.where(core == 0, low, high)
        give[chip, :, chunk + LANES :] = jnp.where(core == 0, high, low).astype(bf16)

    plain = plain.astype(bf16)
    for first in range(value_from, weights.shape[1], tile):
        fresh = jnp.dot(plain, weights[:, first : first + tile], preferred_element_type=f32)
        share_out(first, fresh[:SUB])
    for n in range(0, chunk, tile):
        total = None
        for c in range(chunks):
            first = c * chunk + n
            part = jnp.dot(lhs[c], weights[:, first : first + tile], preferred_element_type=f32)
            if first >= fresh_from:
                share_out(first, part[rows : rows + SUB])
            total = part[:rows] if total is None else total + part[:rows]
        for e in range(chips):
            keep[e, :, n : n + tile] = total[e * SUB : (e + 1) * SUB]
            first = (chips + e) * SUB
            give[e, :, n : n + tile] = total[first : first + SUB].astype(bf16)
    marks = spread[:, columns:]
    request_marks = marked(square, 2, 2)
    for e in range(chips):
        keep[e, :, chunk : chunk + LANES] = marks[e * SUB : (e + 1) * SUB] + request_marks
        first = (chips + e) * SUB
        give[e, :, chunk : chunk + LANES] = (marks[first : first + SUB] + request_marks).astype(
            bf16
        )


def pair_kernel(keep, taken, _, sent):
    chunk = keep.shape[2] - 2 * LANES
    for e in range(keep.shape[0]):
        total = keep[e] + taken[e].astype(f32)
        marks = total[:, chunk : chunk + LANES]
        sent[e, :, :chunk] = total[:, :chunk].astype(bf16)
        sent[e, :, chunk : chunk + LANES] = (
            marked(summed(marks), 2) + marked(summed(marks, 2), 2, 2)
        ).astype(bf16)
        sent[e, :, chunk + LANES :] = total[:, chunk + LANES :].astype(bf16)


def attend_kernel(width, position, received, cache, table, lengths, sent, lines):
    count, _, full = received.shape
    pages, page_len, _ = cache.shape
    chunks = SUB // pages
    chunk = full - 2 * LANES
    tiles = chunk // HD
    total = received[0].astype(f32)
    for k in range(1, count):
        total = total + received[k].astype(f32)
    marks = total[:, chunk : chunk + LANES]
    inverse = lax.rsqrt(summed(marks) / width + epsilon)
    fresh = total[:, chunk + LANES :] * lax.rsqrt(summed(marks, 2) / width + epsilon)
    fresh = fresh.astype(bf16)
    for t in range(tiles):
        lines[t * SUB : (t + 1) * SUB, :] = (
            (total[:, t * HD : (t + 1) * HD] * inverse).astype(bf16).astype(f32)
        )

    def heads(page, first, many):
        runs = []
        while many:
            run = min(many, tiles - first % tiles)
            start = (first % tiles) * SUB + (first // tiles) * pages + page
            runs.append(lines[pl.ds(start, run, stride=SUB), :])
            first, many = first + run, many - run
        return runs[0] if len(runs) == 1 else jnp.concatenate(runs, axis=0)

    group = QH // KVH
    scale = 1.0 / HD**0.5
    lane = lax.broadcasted_iota(jnp.int32, (1, page_len), 1)
    head_group = lax.broadcasted_iota(jnp.int32, (QH, HD), 0) // group
    eye = lax.broadcasted_iota(jnp.int32, (QH, LANES), 0)
    value_rows = pages * QH
    place = (position[0] // 2) % (LANES // value_rows) * value_rows
    eye_lane = lax.broadcasted_iota(jnp.int32, (QH, LANES), 1) - place
    order = lax.broadcasted_iota(jnp.int32, table.shape, 0)
    log_row = jnp.zeros((1, LANES), f32)
    own_row = jnp.zeros((1, LANES), f32)
    for p in range(pages):
        slot = position[0] * pages + p
        hit = table[...] == slot
        logical = jnp.sum(jnp.where(hit, order, 0), axis=(0, 1), keepdims=True)
        length = jnp.sum(
            jnp.where(hit, jnp.broadcast_to(lengths[...], hit.shape), 0),
            axis=(0, 1),
            keepdims=True,
        )
        live = logical * page_len + lane < length
        leads = logical == 0
        query = jnp.concatenate([heads(p, g * group, group) for g in range(KVH)], axis=0)
        keys = [heads(p, QH + g, 1) for g in range(KVH)]
        key_rows = jnp.concatenate([jnp.broadcast_to(k, (group, HD)) for k in keys], axis=0)
        spread = jnp.concatenate(
            [jnp.where(head_group == g, query, 0.0).astype(bf16) for g in range(KVH)], axis=-1
        )
        scores = (
            lax.dot_general(
                spread,
                cache[p, :, : KVH * HD],
                (((1,), (1,)), ((), ())),
                preferred_element_type=f32,
            )
            * scale
        )
        own = jnp.sum(query * key_rows, axis=-1, keepdims=True) * scale
        masked = jnp.where(live, scores, lowest)
        own = jnp.where(leads, own, lowest)
        peak = jnp.max(masked, axis=-1, keepdims=True)
        weights = jnp.where(live, jnp.exp(masked - peak), 0.0)
        mass = jnp.sum(weights, axis=-1, keepdims=True)
        wide = jnp.dot(
            weights.astype(bf16), cache[p, :, KVH * HD :], preferred_element_type=f32
        )
        mixed = jnp.zeros((QH, HD), f32)
        for g in range(KVH):
            mixed = mixed + jnp.where(head_group == g, wide[:, g * HD : (g + 1) * HD], 0.0)
        some = mass > 0.0
        safe = jnp.where(some, mass, 1.0)
        result = (mixed / safe).astype(bf16)
        logs = jnp.where(some, peak + jnp.log(safe), lowest)
        here = eye_lane == eye + p * QH
        log_row = log_row + jnp.sum(jnp.where(here, logs, 0.0), axis=0, keepdims=True)
        own_row = own_row + jnp.sum(jnp.where(here, own, 0.0), axis=0, keepdims=True)
        for e in range(count):
            sent[e, p * QH : (p + 1) * QH, :] = result
    terms = pieces(log_row, PARTS) + pieces(own_row, PARTS)
    terms.append(jnp.zeros((SUB - 2 * PARTS, LANES), f32))
    terms = jnp.concatenate(terms, axis=0).astype(bf16)
    for e in range(count):
        sent[e, value_rows : value_rows + SUB, :] = fresh
        sent[e, value_rows + SUB :, :] = terms


def owner_kernel(chips, pages, position, table, _, owner):
    pages_req, requests = table.shape
    core = position[0] % 2
    span = pages * QH
    rows_each = owner.shape[0] // 2
    row = lax.broadcasted_iota(jnp.int32, owner.shape, 0)
    lane = lax.broadcasted_iota(jnp.int32, owner.shape, 1)
    chip = (row % rows_each) * (LANES // span) + lane // span
    parity = jnp.where(row < rows_each, core, 1 - core)
    page = (chip * 2 + parity) * pages + (lane % span) // QH
    found = jnp.zeros(owner.shape, jnp.int32)
    for r in range(requests):
        for j in range(pages_req):
            found = jnp.where(page == table[j, r], r, found)
    owner[...] = found


def merge_kernel(pages, position, near_ref, far_ref, owner, weights, middle, final, new_kv):
    chips = near_ref.shape[0]
    requests, width = middle.shape
    value_rows = pages * QH
    core = position[0] % 2
    packages = (near_ref, far_ref)
    fresh = []
    for chip in range(chips):
        mine, theirs = (ref[chip, value_rows : value_rows + SUB, :].astype(f32) for ref in packages)
        fresh += [jnp.where(core == 0, mine, theirs), jnp.where(core == 0, theirs, mine)]
    for k, part in enumerate(fresh):
        new_kv[:, k * HD : (k + 1) * HD] = part.astype(bf16)
    each = LANES // value_rows
    request = lax.broadcasted_iota(jnp.int32, (requests, LANES), 0)
    lane = lax.broadcasted_iota(jnp.int32, (requests, LANES), 1)
    logs, own_logs, hits = [], [], []
    for ref in packages:
        for chip in range(0, chips, each):
            terms = sum(ref[chip + k, value_rows + SUB :, :].astype(f32) for k in range(each))
            for first, rows in ((0, logs), (PARTS, own_logs)):
                log = sum(terms[first + k : first + k + 1, :] for k in range(PARTS))
                rows.append(jnp.broadcast_to(log, (requests, LANES)))
            row = len(hits)
            hits.append(jnp.broadcast_to(owner[row : row + 1, :], (requests, LANES)) == request)

    def over_pages(value, combine):
        out = value
        for k in range(QH, LANES, QH):
            out = combine(out, pltpu.roll(value, k, 1))
        return out

    tops = functools.reduce(
        jnp.maximum,
        [
            jnp.where(hit, jnp.maximum(log, own), lowest)
            for hit, log, own in zip(hits, logs, own_logs)
        ],
    )
    tops = over_pages(tops, jnp.maximum)
    factors = [jnp.where(hit, jnp.exp(log - tops), 0.0) for hit, log in zip(hits, logs)]
    own = sum(jnp.where(hit, jnp.exp(log - tops), 0.0) for hit, log in zip(hits, own_logs))
    own = over_pages(own, jnp.add)
    inverse = 1.0 / (over_pages(functools.reduce(jnp.add, factors), jnp.add) + own)
    own_share = own * inverse
    shares = []
    for factor in factors:
        share = factor * inverse
        heads = [jnp.where(lane % QH == h, share, 0.0) for h in range(QH)]
        shares.append(jnp.concatenate(heads, axis=0).astype(bf16))
    half = len(shares) // 2
    mixed = None
    for side, ref in enumerate(packages):
        part = jnp.dot(
            jnp.concatenate(shares[side * half : (side + 1) * half], axis=1),
            jnp.concatenate([ref[chip, :value_rows, :] for chip in range(chips)], axis=0),
            preferred_element_type=f32,
        )
        mixed = part if mixed is None else mixed + part
    attended = jnp.concatenate(
        [
            mixed[h * requests : (h + 1) * requests]
            + own_share[:, h : h + 1] * fresh[KVH + h // (QH // KVH)]
            for h in range(QH)
        ],
        axis=1,
    ).astype(bf16)
    total = jnp.dot(attended, weights[...], preferred_element_type=f32)
    final[...] = (middle[...] + total).astype(bf16)


def fused_shards(
    hidden,
    mix_gain,
    in_gate_input,
    in_step,
    in_groups,
    conv_input,
    conv_groups,
    taps_input,
    taps_groups,
    decay_rate,
    step_bias,
    skip_gain,
    norm_gain,
    out_mixer,
    ssm_state,
    attn_gain,
    w_qkv,
    w_out,
    kv_cache,
    page_table,
    lengths,
):
    count = lax.axis_size("seq")
    position = lax.axis_index("seq").astype(jnp.int32).reshape(1)
    requests, width = hidden.shape
    columns = width // count
    head_width = in_gate_input.shape[1] // 2
    pages = kv_cache.shape[0]
    chunks = SUB // pages
    chips = count // 2
    gcols = in_groups.shape[1]
    state = ssm_state.reshape(requests, head_width, STATE)
    same_core = [list(range(core, count, 2)) for core in range(2)]
    cores = [(i, i ^ 1) for i in range(count)]
    group_args = (
        hidden,
        mix_gain.reshape(1, width),
        in_groups,
        conv_groups.transpose(1, 0, 2),
        taps_groups,
    )
    group_conv, normed = call(
        group_kernel,
        (near((requests, gcols), bf16), near((requests, width), bf16)),
        [FAR] * 5,
        [pltpu.VMEM(x.shape, x.dtype) for x in group_args]
        + [pltpu.SemaphoreType.DMA((len(group_args) - 1 + BLOCKS,))],
        MOST,
    )(*group_args)
    swap = [(i, (i + GROUPS) % count) for i in range(count)]
    other = lax.ppermute(group_conv, "seq", swap)
    carried = (
        state,
        out_mixer,
        norm_gain.reshape(1, head_width),
        attn_gain.reshape(1, columns),
        page_table.T,
        lengths.reshape(1, requests),
    )
    gate_args = (
        in_gate_input,
        in_step.T,
        conv_input.transpose(1, 0, 2),
        taps_input,
    )
    numbers = jnp.concatenate([decay_rate, step_bias, skip_gain]).reshape(1, 3)
    gate, conv, step, decay, stream, state_in, mixer, gain, scale, table, spans = call(
        functools.partial(gate_kernel, len(carried)),
        (
            near((requests, head_width), f32),
            near((requests, 2 * head_width), f32),
            near((requests, LANES), f32),
            near((requests, LANES), f32),
            near((requests, columns), bf16),
        )
        + tuple(near(x.shape, x.dtype) for x in carried),
        [SMEM, NEAR] + [FAR] * 4 + [NEAR] + [FAR] * (1 + len(carried)),
        [pltpu.VMEM(x.shape, x.dtype) for x in gate_args]
        + [pltpu.SemaphoreType.DMA((BLOCKS + 4 + len(carried),))],
    )(position, normed, *gate_args, numbers, hidden, *carried)
    sent = call(
        mixer_kernel,
        near((count, requests, columns + LANES), bf16),
        [SMEM] + [NEAR] * 9,
    )(position, group_conv, other, gate, conv, step, decay, state_in, mixer, gain)
    received = lax.all_to_all(sent, "seq", 0, 0)
    new_state = call(state_kernel, shape(state.shape, f32), [SMEM] + [NEAR] * 6)(
        position, group_conv, other, conv, step, decay, state_in
    )
    chunk = (QH + KVH) * HD // chunks
    keep, give, middle = call(
        functools.partial(project_kernel, chunks, head_width),
        (
            near((chips, SUB, chunk + 2 * LANES), f32),
            near((chips, SUB, chunk + 2 * LANES), bf16),
            near((requests, columns), f32),
        ),
        [SMEM] + [NEAR] * 5,
    )(position, received, stream, scale, w_qkv, table)
    taken = lax.ppermute(give, "seq", cores)
    sent = call(pair_kernel, near(give.shape, bf16), [NEAR] * 2 + [FAR])(keep, taken, new_state)
    received = lax.all_to_all(sent, "seq", 0, 0, axis_index_groups=same_core)
    package = pages * QH + 2 * SUB
    sent = call(
        functools.partial(attend_kernel, width),
        near((chips, package, HD), bf16),
        [SMEM] + [NEAR] * 4,
        [pltpu.VMEM((chunk // HD * SUB, HD), f32)],
    )(position, received, kv_cache, table, spans)
    received = lax.all_to_all(sent, "seq", 0, 0, axis_index_groups=same_core)
    far = lax.ppermute(received, "seq", cores)
    owner_rows = count * pages * QH // LANES
    owner = call(
        functools.partial(owner_kernel, chips, pages),
        near((owner_rows, LANES), jnp.int32),
        [SMEM] * 2 + [NEAR],
    )(position, page_table.T, received)
    final, new_kv = call(
        functools.partial(merge_kernel, pages),
        (
            shape((requests, columns), bf16),
            shape((requests, 2 * KVH * HD), bf16),
        ),
        [SMEM] + [NEAR] * 5,
    )(position, received, far, owner, w_out, middle)
    return (final, new_state.reshape(ssm_state.shape), new_kv)


def shards(*args):
    hidden, in_step, in_groups = args[0], args[3], args[4]
    kv_cache, page_table = args[18], args[19]
    count = lax.axis_size("seq")
    whole_tiles = (
        in_step.shape[1] == 1
        and in_groups.shape[1] == STATE
        and count == 2 * GROUPS
        and hidden.shape[0] == SUB
        and (hidden.shape[1] // count) % LANES == 0
        and SUB % kv_cache.shape[0] == 0
        and LANES % (kv_cache.shape[0] * QH) == 0
        and (count // 2) % (LANES // (kv_cache.shape[0] * QH)) == 0
        and kv_cache.shape[1] == LANES
        and 2 * KVH == count
        and (QH + KVH) * HD % (SUB // kv_cache.shape[0] * 2 * HD) == 0
    )
    return (fused_shards if whole_tiles else plain_shards)(*args)


def solution(mesh):
    placed = (
        P("grp", None),
        P(),
        P(None, "seq"),
        P(None, "seq"),
        P(None, "seq"),
        P("grp", None, "seq"),
        P("grp", None, "seq"),
        P(None, "seq"),
        P(None, "seq"),
        P("seq"),
        P("seq"),
        P("seq"),
        P("seq"),
        P("seq", None),
        P("grp", "seq", None, None),
        P("seq"),
        P("seq", None),
        P(None, "seq"),
        P(("grp", "seq"), None, None),
        P("grp", None),
        P("grp"),
    )
    return jax.shard_map(
        shards,
        mesh=mesh,
        in_specs=placed,
        out_specs=(P("grp", "seq"), P("grp", "seq", None, None), P("grp", None)),
        check_vma=False,
    )
```

```python
import functools

import jax
import jax.numpy as jnp
from jax import lax
from jax.experimental import pallas as pl
from jax.experimental.pallas import tpu as pltpu
from jax.sharding import PartitionSpec as P

QH = 32
KVH = 8
HD = 128
STATE = 128
GROUPS = 8
LANES = 128

epsilon = 1e-05
lowest = -1e30


def conv_step(state, fresh, taps):
    window = jnp.concatenate([state.astype(jnp.float32), fresh[:, None, :]], axis=1)
    summed = jnp.sum(window * taps[:-1][None], axis=1) + taps[-1][None]
    return jax.nn.silu(summed)


def split(value, parts):
    pieces = []
    rest = value
    for _ in range(parts):
        piece = lax.reduce_precision(rest, 8, 7)
        pieces.append(piece.astype(jnp.bfloat16))
        rest = rest - piece
    return pieces


def group_vectors(group_conv, heads_here, requests):
    count = lax.axis_size("seq")
    position = lax.axis_index("seq")
    if heads_here == 1 and group_conv.shape[1] == STATE and count == 2 * GROUPS:
        swap = [(i, (i + GROUPS) % count) for i in range(count)]
        other = lax.ppermute(group_conv, "seq", swap)
        first = position < GROUPS
        inject = jnp.where(first, group_conv, other)
        readout = jnp.where(first, other, group_conv)
        return (
            inject.astype(jnp.float32)[:, None, :],
            readout.astype(jnp.float32)[:, None, :],
        )
    group_all = lax.all_gather(group_conv, "seq", axis=1, tiled=True).astype(jnp.float32)
    inject = group_all[:, : GROUPS * STATE].reshape(requests, GROUPS, STATE)
    readout = group_all[:, GROUPS * STATE :].reshape(requests, GROUPS, STATE)
    head_ids = position * heads_here + jnp.arange(heads_here, dtype=jnp.int32)
    return inject[:, head_ids % GROUPS], readout[:, head_ids % GROUPS]


def plain_shards(
    hidden,
    mix_gain,
    in_gate_input,
    in_step,
    in_groups,
    conv_input,
    conv_groups,
    taps_input,
    taps_groups,
    decay_rate,
    step_bias,
    skip_gain,
    norm_gain,
    out_mixer,
    ssm_state,
    attn_gain,
    w_qkv,
    w_out,
    kv_cache,
    page_table,
    lengths,
):
    count_seq = lax.axis_size("seq")
    position = lax.axis_index("seq")
    requests = hidden.shape[0]
    width = hidden.shape[1]
    heads_here = in_step.shape[1]
    head_width = in_gate_input.shape[1] // (2 * heads_here)
    heads_total = heads_here * count_seq
    per_group = heads_total // GROUPS
    columns = width // count_seq
    stream = hidden.astype(jnp.float32)
    normed = (
        stream * lax.rsqrt(jnp.mean(stream * stream, axis=-1, keepdims=True) + epsilon) * mix_gain
    ).astype(jnp.bfloat16)
    group_raw = jnp.dot(normed, in_groups, preferred_element_type=jnp.float32)
    group_conv = conv_step(conv_groups, group_raw, taps_groups).astype(jnp.bfloat16)
    inject_heads, readout_heads = group_vectors(group_conv, heads_here, requests)
    gate_input = jnp.dot(normed, in_gate_input, preferred_element_type=jnp.float32).reshape(
        requests, heads_here, 2, head_width
    )
    gate_part = gate_input[:, :, 0]
    input_part = gate_input[:, :, 1].reshape(requests, heads_here * head_width)
    step_raw = jnp.dot(normed, in_step, preferred_element_type=jnp.float32)
    conv_out = conv_step(conv_input, input_part, taps_input).reshape(
        requests, heads_here, head_width
    )
    step_size = jax.nn.softplus(step_raw + step_bias)
    decay = jnp.exp(-decay_rate * step_size)
    new_state = (
        decay[:, :, None, None] * ssm_state
        + (step_size[:, :, None] * conv_out)[:, :, :, None] * inject_heads[:, :, None, :]
    )
    ssm_out = (
        jnp.sum(new_state * readout_heads[:, :, None, :], axis=-1)
        + skip_gain[None, :, None] * conv_out
    )
    gated = ssm_out * jax.nn.silu(gate_part)
    head_squares = jnp.sum(gated * gated, axis=-1)
    weighted = (gated * norm_gain.reshape(heads_here, head_width)).astype(jnp.bfloat16)
    products = jnp.einsum(
        "rhp,hpd->hrd",
        weighted,
        out_mixer.reshape(heads_here, head_width, width),
        preferred_element_type=jnp.float32,
    ).astype(jnp.bfloat16)
    products = products.reshape(heads_here, requests, count_seq, columns).transpose(2, 0, 1, 3)
    marks = jnp.stack(split(head_squares.T, 2), axis=-1)
    marks = jnp.pad(marks, ((0, 0), (0, 0), (0, LANES - 2)))
    marks = jnp.broadcast_to(marks[None], (count_seq,) + marks.shape)
    received = lax.all_to_all(jnp.concatenate([products, marks], axis=-1), "seq", 0, 0)
    received = received.astype(jnp.float32)
    squares = (received[..., columns] + received[..., columns + 1]).reshape(
        per_group, GROUPS, requests
    )
    scales = lax.rsqrt(jnp.sum(squares, axis=0) / (per_group * head_width) + epsilon)
    mixer = jnp.sum(
        received[..., :columns].reshape(per_group, GROUPS, requests, columns)
        * scales[None, :, :, None],
        axis=(0, 1),
    )
    stream_cols = lax.dynamic_slice_in_dim(stream, position * columns, columns, 1)
    middle = (stream_cols + mixer).astype(jnp.bfloat16)
    middle_f = middle.astype(jnp.float32)
    scaled = (middle_f * attn_gain).astype(jnp.bfloat16)
    partial_sq = jnp.sum(middle_f * middle_f, axis=-1)
    pages_here = kv_cache.shape[0]
    page_len = kv_cache.shape[1]
    pages_req = page_table.shape[1]
    pages_all = pages_here * count_seq
    matches = page_table[None, :, :] == jnp.arange(pages_all, dtype=jnp.int32)[:, None, None]
    owner = jnp.any(matches, axis=2)
    page_rows = jnp.dot(
        owner.astype(jnp.bfloat16), scaled, preferred_element_type=jnp.float32
    ).astype(jnp.bfloat16)
    page_proj = jnp.dot(page_rows, w_qkv, preferred_element_type=jnp.float32).astype(jnp.bfloat16)
    page_sq = jnp.sum(jnp.where(owner, partial_sq[None, :], 0.0), axis=1)
    sq_parts = jnp.pad(jnp.stack(split(page_sq, 2), axis=-1), ((0, 0), (0, LANES - 2)))
    sent = jnp.concatenate([page_proj, sq_parts], axis=-1).reshape(count_seq, pages_here, -1)
    arrived = jnp.sum(lax.all_to_all(sent, "seq", 0, 0).astype(jnp.float32), axis=0)
    qkv_width = w_qkv.shape[1]
    total_sq = arrived[:, qkv_width] + arrived[:, qkv_width + 1]
    qkv = (arrived[:, :qkv_width] * lax.rsqrt(total_sq / width + epsilon)[:, None]).astype(
        jnp.bfloat16
    )
    group_size = QH // KVH
    queries = qkv[:, : QH * HD].reshape(pages_here, KVH, group_size, HD)
    fresh_kv = qkv[:, QH * HD :]
    fresh_keys = fresh_kv[:, : KVH * HD].reshape(pages_here, KVH, 1, HD).astype(jnp.float32)
    fresh_values = fresh_kv[:, KVH * HD :].reshape(pages_here, KVH, 1, HD).astype(jnp.float32)
    scale = 1.0 / HD**0.5
    slots = position * pages_here + jnp.arange(pages_here, dtype=jnp.int32)
    own_matches = page_table[None, :, :] == slots[:, None, None]
    logical = jnp.sum(
        jnp.any(own_matches, axis=1) * jnp.arange(pages_req, dtype=jnp.int32)[None, :], axis=1
    )
    page_length = jnp.sum(jnp.where(jnp.any(own_matches, axis=2), lengths[None, :], 0), axis=1)
    token_pos = logical[:, None] * page_len + jnp.arange(page_len, dtype=jnp.int32)[None, :]
    live = (token_pos < page_length[:, None])[:, None, None, :]
    leads = (logical == 0)[:, None, None]
    cached = kv_cache.reshape(pages_here, page_len, 2, KVH, HD)
    scores = (
        jnp.einsum("pgjd,ptgd->pgjt", queries, cached[:, :, 0], preferred_element_type=jnp.float32)
        * scale
    )
    own = jnp.sum(queries.astype(jnp.float32) * fresh_keys, axis=-1) * scale
    masked = jnp.where(live, scores, lowest)
    own = jnp.where(leads, own, lowest)
    peak = jnp.maximum(jnp.max(masked, axis=-1), own)
    weights = jnp.where(live, jnp.exp(masked - peak[..., None]), 0.0)
    own_weight = jnp.where(leads, jnp.exp(own - peak), 0.0)
    total = jnp.sum(weights, axis=-1) + own_weight
    values = jnp.einsum(
        "pgjt,ptgd->pgjd",
        weights.astype(jnp.bfloat16),
        cached[:, :, 1],
        preferred_element_type=jnp.float32,
    )
    values = values + own_weight[..., None] * fresh_values
    some = total > 0.0
    safe = jnp.where(some, total, 1.0)
    values = (values / safe[..., None]).astype(jnp.bfloat16)
    logsum = jnp.where(some, peak + jnp.log(safe), lowest)
    logs = jnp.concatenate(split(logsum.reshape(1, pages_here * QH), 3), axis=0)
    logs = jnp.pad(logs, ((0, 5), (0, LANES - pages_here * QH)))
    value_rows = pages_here * QH
    kv_rows = pages_here * 2 * KVH
    package = jnp.concatenate(
        [values.reshape(value_rows, HD), fresh_kv.reshape(kv_rows, HD), logs], axis=0
    )
    package = jnp.broadcast_to(package[None], (count_seq,) + package.shape)
    everything = lax.all_to_all(package, "seq", 0, 0)
    all_values = everything[:, :value_rows].reshape(pages_all, QH, HD)
    all_kv = everything[:, value_rows : value_rows + kv_rows].reshape(pages_all, 2 * KVH * HD)
    all_logs = everything[:, value_rows + kv_rows :, : pages_here * QH].astype(jnp.float32)
    all_logs = (all_logs[:, 0] + all_logs[:, 1] + all_logs[:, 2]).reshape(pages_all, QH)
    new_kv = all_kv[page_table[:, 0]]
    req_logs = all_logs[page_table]
    top = jnp.max(req_logs, axis=1, keepdims=True)
    factors = jnp.exp(req_logs - top)
    summed = jnp.sum(factors[..., None] * all_values[page_table].astype(jnp.float32), axis=1)
    attended = (summed / jnp.sum(factors, axis=1)[..., None]).astype(jnp.bfloat16)
    final = (
        middle_f
        + jnp.dot(
            attended.reshape(requests, QH * HD), w_out, preferred_element_type=jnp.float32
        )
    ).astype(jnp.bfloat16)
    return (final, new_state, new_kv)


f32 = jnp.float32
bf16 = jnp.bfloat16
SUB = 8
PARTS = 3
SCOPED = 16 << 20
MOST = 63500 << 10
BLOCKS = 2
VMEM = pl.BlockSpec(memory_space=pltpu.VMEM)
NEAR = pl.BlockSpec(memory_space=pltpu.VMEM)
SMEM = pl.BlockSpec(memory_space=pltpu.SMEM)
FAR = pl.BlockSpec(memory_space=pltpu.HBM)


def call(kernel, outs, specs, scratch=(), scoped=SCOPED):
    grid_free = pl.pallas_call(
        kernel,
        out_shape=outs,
        in_specs=specs,
        out_specs=jax.tree.map(lambda _: VMEM, outs, is_leaf=lambda x: hasattr(x, "shape")),
        scratch_shapes=scratch,
        compiler_params=pltpu.CompilerParams(vmem_limit_bytes=scoped),
    )

    def run(*args):
        spaces = {id(NEAR): pltpu.VMEM, id(FAR): pltpu.HBM}
        placed = [
            pltpu.with_memory_space_constraint(arg, spaces[id(spec)]) if id(spec) in spaces else arg
            for arg, spec in zip(args, specs)
        ]
        return grid_free(*placed)

    return run


def shape(dims, kind):
    return jax.ShapeDtypeStruct(dims, kind)


def near(dims, kind):
    return pltpu.VMEM(dims, kind)


def silu(x):
    return x * jax.nn.sigmoid(x)


def pieces(value, parts):
    out = []
    for _ in range(parts):
        piece = value.astype(bf16).astype(f32)
        out.append(piece)
        value = value - piece
    return out


def marked(value, parts, first=0):
    lane = lax.broadcasted_iota(jnp.int32, (value.shape[0], LANES), 1)
    out = jnp.zeros((value.shape[0], LANES), f32)
    for k, piece in enumerate(pieces(value, parts)):
        out = jnp.where(lane == first + k, piece, out)
    return out


def summed(marks, first=0):
    return marks[:, first : first + 1] + marks[:, first + 1 : first + 2]


def convolve(state_ref, fresh, taps_ref):
    taps = state_ref.shape[0]
    total = taps_ref[taps : taps + 1, :] * fresh + taps_ref[taps + 1 : taps + 2, :]
    for k in range(taps):
        total = total + taps_ref[k : k + 1, :] * state_ref[k].astype(f32)
    return silu(total)


def fetch_all(pairs, sems):
    copies = [
        pltpu.make_async_copy(source, target, sems.at[k])
        for k, (source, target) in enumerate(pairs)
    ]
    for copy in copies:
        copy.start()
    return copies


def group_kernel(
    hidden_far,
    gain_far,
    weights_far,
    state_far,
    taps_far,
    group_out,
    normed_out,
    hidden,
    gain,
    weights,
    state,
    taps,
    sems,
):
    depth = weights.shape[0] // BLOCKS
    rows = [pl.ds(k * depth, depth) for k in range(BLOCKS)]
    copies = fetch_all(
        [(hidden_far, hidden), (gain_far, gain)]
        + [(weights_far.at[r], weights.at[r]) for r in rows]
        + [(state_far, state), (taps_far, taps)],
        sems,
    )
    copies[0].wait()
    copies[1].wait()
    stream = hidden[...].astype(f32)
    mean = jnp.mean(stream * stream, axis=-1, keepdims=True)
    normed_out[...] = (stream * lax.rsqrt(mean + epsilon) * gain[...]).astype(bf16)
    raw = jnp.zeros(group_out.shape, f32)
    for k in range(BLOCKS):
        copies[2 + k].wait()
        span = slice(k * depth, (k + 1) * depth)
        raw = raw + jnp.dot(normed_out[:, span], weights[span, :], preferred_element_type=f32)
    copies[-2].wait()
    copies[-1].wait()
    group_out[...] = convolve(state, raw, taps).astype(bf16)


def gate_kernel(carried, position, normed_ref, *refs):
    weights_far, step_far, state_far, taps_far, numbers, hidden_far = refs[:6]
    inputs, outputs, scratch = refs[6 : 6 + carried], refs[6 + carried : -5], refs[-5:]
    gate_out, conv_out, step_out, decay_out, columns_out = outputs[:5]
    weights, step_row, state, taps, sems = scratch
    columns = columns_out.shape[1]
    start = pl.multiple_of(position[0] * columns, columns)
    depth = weights.shape[0] // BLOCKS
    rows = [pl.ds(k * depth, depth) for k in range(BLOCKS)]
    copies = fetch_all(
        [(weights_far.at[r], weights.at[r]) for r in rows]
        + [
            (step_far, step_row),
            (state_far, state),
            (taps_far, taps),
            (hidden_far.at[:, pl.ds(start, columns)], columns_out),
        ]
        + list(zip(inputs, outputs[5:])),
        sems,
    )
    half = gate_out.shape[1]
    both = jnp.zeros((gate_out.shape[0], weights.shape[1]), f32)
    for k in range(BLOCKS):
        copies[k].wait()
        span = slice(k * depth, (k + 1) * depth)
        both = both + jnp.dot(normed_ref[:, span], weights[span, :], preferred_element_type=f32)
    for copy in copies[BLOCKS : BLOCKS + 3]:
        copy.wait()
    gate_out[...] = silu(both[:, :half])
    fresh = convolve(state, both[:, half:], taps)
    conv_out[:, :half] = fresh
    conv_out[:, half:] = numbers[:, 2:3] * fresh
    raw = jnp.sum(normed_ref[...].astype(f32) * step_row[...].astype(f32), axis=-1, keepdims=True)
    step = jax.nn.softplus(raw + numbers[:, 1:2])
    step_out[...] = jnp.broadcast_to(step, step_out.shape)
    decay_out[...] = jnp.broadcast_to(jnp.exp(-numbers[:, 0:1] * step), decay_out.shape)
    for copy in copies[BLOCKS + 3 :]:
        copy.wait()


def chosen(position, own, other):
    first = position[0] < GROUPS
    mine, theirs = own[...].astype(f32), other[...].astype(f32)
    return jnp.where(first, mine, theirs), jnp.where(first, theirs, mine)


def mixer_kernel(position, own, other, gate, conv, step, decay, state, weights, gain, sent):
    requests = own.shape[0]
    inject, readout = chosen(position, own, other)
    half = gate.shape[1]
    both = 2 * half
    flat = state[...].reshape(requests * half, state.shape[2])
    high = flat.astype(bf16)
    low = (flat - high.astype(f32)).astype(bf16)
    vectors = readout.astype(bf16)
    full = sum(
        lax.dot_general(
            vectors, term, (((1,), (1,)), ((), ())), preferred_element_type=f32
        )
        for term in (high, low)
    )
    row = lax.broadcasted_iota(jnp.int32, (requests, both), 0)
    pairs = jnp.zeros((requests, both), f32)
    for k in range(requests // 2):
        pairs = jnp.where(row // 2 == k, full[:, k * both : (k + 1) * both], pairs)
    read = jnp.where(row[:, :half] % 2 == 0, pairs[:, :half], pairs[:, half:])
    along = jnp.sum(inject * readout, axis=-1, keepdims=True)
    fresh = conv[:, :half]
    out = decay[:, :1] * read + step[:, :1] * fresh * along + conv[:, half:]
    gated = out * gate[...]
    marks = marked(jnp.sum(gated * gated, axis=-1, keepdims=True), 2).astype(bf16)
    weighted = (gated * gain[...]).astype(bf16)
    count = sent.shape[0]
    columns = weights.shape[1] // count
    for e in range(count):
        product = jnp.dot(
            weighted, weights[:, e * columns : (e + 1) * columns], preferred_element_type=f32
        )
        sent[e, :, :columns] = product.astype(bf16)
        sent[e, :, columns:] = marks


def state_kernel(
    pages, page_len, position, own, other, conv, step, decay, state, table, lengths, new_state, bounds
):
    order = lax.broadcasted_iota(jnp.int32, table.shape, 0)
    spans = jnp.broadcast_to(lengths[...], table.shape)
    for p in range(pages):
        hit = table[...] == position[0] * pages + p
        logical = jnp.sum(jnp.where(hit, order, 0), axis=(0, 1), keepdims=True)
        length = jnp.sum(jnp.where(hit, spans, 0), axis=(0, 1), keepdims=True)
        lane = jnp.zeros((1, LANES), jnp.int32)
        bounds[p : p + 1, :] = lane + (length - logical * page_len)
        bounds[pages + p : pages + p + 1, :] = lane + jnp.where(logical == 0, 1, 0)
    inject, _ = chosen(position, own, other)
    fresh = step[:, :1] * conv[:, : state.shape[1]]
    new_state[...] = (
        decay[:, :1][:, :, None] * state[...] + fresh[:, :, None] * inject[:, None, :]
    )


def project_kernel(
    chunks, head_width, position, received, hidden, gain, weights, table, keep, give, middle_out
):
    count, requests, _ = received.shape
    columns = weights.shape[0]
    squares = [received[k, :, columns:].astype(f32) for k in range(count)]
    mixer = jnp.zeros((requests, columns), f32)
    for g in range(GROUPS):
        members = range(g, count, GROUPS)
        marks = sum(squares[k] for k in members)
        total = marks[:, :1] + marks[:, 1:2]
        scale = lax.rsqrt(total / (len(members) * head_width) + epsilon)
        products = sum(received[k, :, :columns].astype(f32) for k in members)
        mixer = mixer + scale * products
    middle = (hidden[...].astype(f32) + mixer).astype(bf16).astype(f32)
    middle_out[...] = middle
    square = jnp.sum(middle * middle, axis=-1, keepdims=True)
    scaled = middle * gain[...]
    extended = jnp.concatenate([scaled, marked(square, 2)], axis=-1).astype(bf16)
    rows = count * SUB
    pages = SUB // chunks
    chips = count // 2
    core = position[0] % 2
    index = lax.broadcasted_iota(jnp.int32, (rows, requests), 0)
    line = index % (chips * SUB)
    parity = jnp.where(index < chips * SUB, core, 1 - core)
    page = ((line // SUB) * 2 + parity) * pages + index % pages
    hits = page == table[0:1, :]
    for j in range(1, table.shape[0]):
        hits = jnp.logical_or(hits, page == table[j : j + 1, :])
    onehot = jnp.where(hits, 1.0, 0.0).astype(bf16)
    spread = jnp.dot(onehot, extended, preferred_element_type=f32)
    lines = spread[:, :columns]
    which = (lax.broadcasted_iota(jnp.int32, lines.shape, 0) % SUB) // pages
    fresh_from = QH * HD
    value_from = fresh_from + KVH * HD
    chunk = value_from // chunks
    plain = jnp.concatenate([scaled, jnp.zeros((SUB, columns), f32)], axis=0)
    lhs = []
    for c in range(chunks):
        own = jnp.where(which == c, lines, 0.0)
        if (c + 1) * chunk > fresh_from:
            own = jnp.concatenate([own, plain], axis=0)
        lhs.append(own.astype(bf16))
    tile = 2 * HD

    def share_out(first, fresh):
        chip = (first - fresh_from) // tile
        low, high = fresh[:, :HD], fresh[:, HD:]
        keep[chip, :, chunk + LANES :] = jnp.where(core == 0, low, high)
        give[chip, :, chunk + LANES :] = jnp.where(core == 0, high, low).astype(bf16)

    plain = plain.astype(bf16)
    for first in range(value_from, weights.shape[1], tile):
        fresh = jnp.dot(plain, weights[:, first : first + tile], preferred_element_type=f32)
        share_out(first, fresh[:SUB])
    for n in range(0, chunk, tile):
        total = None
        for c in range(chunks):
            first = c * chunk + n
            part = jnp.dot(lhs[c], weights[:, first : first + tile], preferred_element_type=f32)
            if first >= fresh_from:
                share_out(first, part[rows : rows + SUB])
            total = part[:rows] if total is None else total + part[:rows]
        for e in range(chips):
            keep[e, :, n : n + tile] = total[e * SUB : (e + 1) * SUB]
            first = (chips + e) * SUB
            give[e, :, n : n + tile] = total[first : first + SUB].astype(bf16)
    marks = spread[:, columns:]
    request_marks = marked(square, 2, 2)
    for e in range(chips):
        keep[e, :, chunk : chunk + LANES] = marks[e * SUB : (e + 1) * SUB] + request_marks
        first = (chips + e) * SUB
        give[e, :, chunk : chunk + LANES] = (marks[first : first + SUB] + request_marks).astype(
            bf16
        )


def pair_kernel(keep, taken, _, sent):
    chunk = keep.shape[2] - 2 * LANES
    for e in range(keep.shape[0]):
        total = keep[e] + taken[e].astype(f32)
        marks = total[:, chunk : chunk + LANES]
        sent[e, :, :chunk] = total[:, :chunk].astype(bf16)
        sent[e, :, chunk : chunk + LANES] = (
            marked(summed(marks), 2) + marked(summed(marks, 2), 2, 2)
        ).astype(bf16)
        sent[e, :, chunk + LANES :] = total[:, chunk + LANES :].astype(bf16)


def attend_kernel(width, position, received, cache, bounds, sent, lines):
    count, _, full = received.shape
    pages, page_len, _ = cache.shape
    chunks = SUB // pages
    chunk = full - 2 * LANES
    tiles = chunk // HD
    total = received[0].astype(f32)
    for k in range(1, count):
        total = total + received[k].astype(f32)
    marks = total[:, chunk : chunk + LANES]
    inverse = lax.rsqrt(summed(marks) / width + epsilon)
    fresh = total[:, chunk + LANES :] * lax.rsqrt(summed(marks, 2) / width + epsilon)
    fresh = fresh.astype(bf16)
    for t in range(tiles):
        lines[t * SUB : (t + 1) * SUB, :] = (
            (total[:, t * HD : (t + 1) * HD] * inverse).astype(bf16).astype(f32)
        )

    def heads(page, first, many):
        runs = []
        while many:
            run = min(many, tiles - first % tiles)
            start = (first % tiles) * SUB + (first // tiles) * pages + page
            runs.append(lines[pl.ds(start, run, stride=SUB), :])
            first, many = first + run, many - run
        return runs[0] if len(runs) == 1 else jnp.concatenate(runs, axis=0)

    group = QH // KVH
    scale = 1.0 / HD**0.5
    lane = lax.broadcasted_iota(jnp.int32, (1, page_len), 1)
    head_group = lax.broadcasted_iota(jnp.int32, (QH, HD), 0) // group
    eye = lax.broadcasted_iota(jnp.int32, (QH, LANES), 0)
    value_rows = pages * QH
    place = (position[0] // 2) % (LANES // value_rows) * value_rows
    eye_lane = lax.broadcasted_iota(jnp.int32, (QH, LANES), 1) - place
    log_row = jnp.zeros((1, LANES), f32)
    own_row = jnp.zeros((1, LANES), f32)
    for p in range(pages):
        live = lane < bounds[p : p + 1, :]
        leads = bounds[pages + p : pages + p + 1, :1] == 1
        query = jnp.concatenate([heads(p, g * group, group) for g in range(KVH)], axis=0)
        keys = [heads(p, QH + g, 1) for g in range(KVH)]
        key_rows = jnp.concatenate([jnp.broadcast_to(k, (group, HD)) for k in keys], axis=0)
        spread = jnp.concatenate(
            [jnp.where(head_group == g, query, 0.0).astype(bf16) for g in range(KVH)], axis=-1
        )
        scores = (
            lax.dot_general(
                spread,
                cache[p, :, : KVH * HD],
                (((1,), (1,)), ((), ())),
                preferred_element_type=f32,
            )
            * scale
        )
        own = jnp.sum(query * key_rows, axis=-1, keepdims=True) * scale
        masked = jnp.where(live, scores, lowest)
        own = jnp.where(leads, own, lowest)
        peak = jnp.max(masked, axis=-1, keepdims=True)
        weights = jnp.where(live, jnp.exp(masked - peak), 0.0)
        mass = jnp.sum(weights, axis=-1, keepdims=True)
        wide = jnp.dot(
            weights.astype(bf16), cache[p, :, KVH * HD :], preferred_element_type=f32
        )
        mixed = jnp.zeros((QH, HD), f32)
        for g in range(KVH):
            mixed = mixed + jnp.where(head_group == g, wide[:, g * HD : (g + 1) * HD], 0.0)
        some = mass > 0.0
        safe = jnp.where(some, mass, 1.0)
        result = (mixed / safe).astype(bf16)
        logs = jnp.where(some, peak + jnp.log(safe), lowest)
        here = eye_lane == eye + p * QH
        log_row = log_row + jnp.sum(jnp.where(here, logs, 0.0), axis=0, keepdims=True)
        own_row = own_row + jnp.sum(jnp.where(here, own, 0.0), axis=0, keepdims=True)
        for e in range(count):
            sent[e, p * QH : (p + 1) * QH, :] = result
    terms = pieces(log_row, PARTS) + pieces(own_row, PARTS)
    terms.append(jnp.zeros((SUB - 2 * PARTS, LANES), f32))
    terms = jnp.concatenate(terms, axis=0).astype(bf16)
    for e in range(count):
        sent[e, value_rows : value_rows + SUB, :] = fresh
        sent[e, value_rows + SUB :, :] = terms


def owner_kernel(chips, pages, position, table, _, owner):
    pages_req, requests = table.shape
    core = position[0] % 2
    span = pages * QH
    rows_each = owner.shape[0] // 2
    row = lax.broadcasted_iota(jnp.int32, owner.shape, 0)
    lane = lax.broadcasted_iota(jnp.int32, owner.shape, 1)
    chip = (row % rows_each) * (LANES // span) + lane // span
    parity = jnp.where(row < rows_each, core, 1 - core)
    page = (chip * 2 + parity) * pages + (lane % span) // QH
    found = jnp.zeros(owner.shape, jnp.int32)
    for r in range(requests):
        for j in range(pages_req):
            found = jnp.where(page == table[j, r], r, found)
    owner[...] = found


def merge_kernel(pages, position, near_ref, far_ref, owner, weights, middle, final, new_kv):
    chips = near_ref.shape[0]
    requests, width = middle.shape
    value_rows = pages * QH
    core = position[0] % 2
    packages = (near_ref, far_ref)
    fresh = []
    for chip in range(chips):
        mine, theirs = (ref[chip, value_rows : value_rows + SUB, :].astype(f32) for ref in packages)
        fresh += [jnp.where(core == 0, mine, theirs), jnp.where(core == 0, theirs, mine)]
    for k, part in enumerate(fresh):
        new_kv[:, k * HD : (k + 1) * HD] = part.astype(bf16)
    each = LANES // value_rows
    request = lax.broadcasted_iota(jnp.int32, (requests, LANES), 0)
    lane = lax.broadcasted_iota(jnp.int32, (requests, LANES), 1)
    logs, own_logs, hits = [], [], []
    for ref in packages:
        for chip in range(0, chips, each):
            terms = sum(ref[chip + k, value_rows + SUB :, :].astype(f32) for k in range(each))
            for first, rows in ((0, logs), (PARTS, own_logs)):
                log = sum(terms[first + k : first + k + 1, :] for k in range(PARTS))
                rows.append(jnp.broadcast_to(log, (requests, LANES)))
            row = len(hits)
            hits.append(jnp.broadcast_to(owner[row : row + 1, :], (requests, LANES)) == request)

    def over_pages(value, combine):
        out = value
        for k in range(QH, LANES, QH):
            out = combine(out, pltpu.roll(value, k, 1))
        return out

    tops = functools.reduce(
        jnp.maximum,
        [
            jnp.where(hit, jnp.maximum(log, own), lowest)
            for hit, log, own in zip(hits, logs, own_logs)
        ],
    )
    tops = over_pages(tops, jnp.maximum)
    factors = [jnp.where(hit, jnp.exp(log - tops), 0.0) for hit, log in zip(hits, logs)]
    own = sum(jnp.where(hit, jnp.exp(log - tops), 0.0) for hit, log in zip(hits, own_logs))
    own = over_pages(own, jnp.add)
    inverse = 1.0 / (over_pages(functools.reduce(jnp.add, factors), jnp.add) + own)
    own_share = own * inverse
    shares = []
    for factor in factors:
        share = factor * inverse
        heads = [jnp.where(lane % QH == h, share, 0.0) for h in range(QH)]
        shares.append(jnp.concatenate(heads, axis=0).astype(bf16))
    half = len(shares) // 2
    mixed = None
    for side, ref in enumerate(packages):
        part = jnp.dot(
            jnp.concatenate(shares[side * half : (side + 1) * half], axis=1),
            jnp.concatenate([ref[chip, :value_rows, :] for chip in range(chips)], axis=0),
            preferred_element_type=f32,
        )
        mixed = part if mixed is None else mixed + part
    attended = jnp.concatenate(
        [
            mixed[h * requests : (h + 1) * requests]
            + own_share[:, h : h + 1] * fresh[KVH + h // (QH // KVH)]
            for h in range(QH)
        ],
        axis=1,
    ).astype(bf16)
    total = jnp.dot(attended, weights[...], preferred_element_type=f32)
    final[...] = (middle[...] + total).astype(bf16)


def fused_shards(
    hidden,
    mix_gain,
    in_gate_input,
    in_step,
    in_groups,
    conv_input,
    conv_groups,
    taps_input,
    taps_groups,
    decay_rate,
    step_bias,
    skip_gain,
    norm_gain,
    out_mixer,
    ssm_state,
    attn_gain,
    w_qkv,
    w_out,
    kv_cache,
    page_table,
    lengths,
):
    count = lax.axis_size("seq")
    position = lax.axis_index("seq").astype(jnp.int32).reshape(1)
    requests, width = hidden.shape
    columns = width // count
    head_width = in_gate_input.shape[1] // 2
    pages = kv_cache.shape[0]
    chunks = SUB // pages
    chips = count // 2
    gcols = in_groups.shape[1]
    state = ssm_state.reshape(requests, head_width, STATE)
    same_core = [list(range(core, count, 2)) for core in range(2)]
    cores = [(i, i ^ 1) for i in range(count)]
    group_args = (
        hidden,
        mix_gain.reshape(1, width),
        in_groups,
        conv_groups.transpose(1, 0, 2),
        taps_groups,
    )
    group_conv, normed = call(
        group_kernel,
        (near((requests, gcols), bf16), near((requests, width), bf16)),
        [FAR] * 5,
        [pltpu.VMEM(x.shape, x.dtype) for x in group_args]
        + [pltpu.SemaphoreType.DMA((len(group_args) - 1 + BLOCKS,))],
        MOST,
    )(*group_args)
    swap = [(i, (i + GROUPS) % count) for i in range(count)]
    other = lax.ppermute(group_conv, "seq", swap)
    carried = (
        state,
        out_mixer,
        norm_gain.reshape(1, head_width),
        attn_gain.reshape(1, columns),
        page_table.T,
        lengths.reshape(1, requests),
    )
    gate_args = (
        in_gate_input,
        in_step.T,
        conv_input.transpose(1, 0, 2),
        taps_input,
    )
    numbers = jnp.concatenate([decay_rate, step_bias, skip_gain]).reshape(1, 3)
    gate, conv, step, decay, stream, state_in, mixer, gain, scale, table, spans = call(
        functools.partial(gate_kernel, len(carried)),
        (
            near((requests, head_width), f32),
            near((requests, 2 * head_width), f32),
            near((requests, LANES), f32),
            near((requests, LANES), f32),
            near((requests, columns), bf16),
        )
        + tuple(near(x.shape, x.dtype) for x in carried),
        [SMEM, NEAR] + [FAR] * 4 + [NEAR] + [FAR] * (1 + len(carried)),
        [pltpu.VMEM(x.shape, x.dtype) for x in gate_args]
        + [pltpu.SemaphoreType.DMA((BLOCKS + 4 + len(carried),))],
    )(position, normed, *gate_args, numbers, hidden, *carried)
    sent = call(
        mixer_kernel,
        near((count, requests, columns + LANES), bf16),
        [SMEM] + [NEAR] * 9,
    )(position, group_conv, other, gate, conv, step, decay, state_in, mixer, gain)
    received = lax.all_to_all(sent, "seq", 0, 0)
    new_state, bounds = call(
        functools.partial(state_kernel, pages, kv_cache.shape[1]),
        (shape(state.shape, f32), near((SUB, LANES), jnp.int32)),
        [SMEM] + [NEAR] * 8,
    )(position, group_conv, other, conv, step, decay, state_in, table, spans)
    chunk = (QH + KVH) * HD // chunks
    keep, give, middle = call(
        functools.partial(project_kernel, chunks, head_width),
        (
            near((chips, SUB, chunk + 2 * LANES), f32),
            near((chips, SUB, chunk + 2 * LANES), bf16),
            near((requests, columns), f32),
        ),
        [SMEM] + [NEAR] * 5,
    )(position, received, stream, scale, w_qkv, table)
    taken = lax.ppermute(give, "seq", cores)
    sent = call(pair_kernel, near(give.shape, bf16), [NEAR] * 2 + [FAR])(keep, taken, new_state)
    received = lax.all_to_all(sent, "seq", 0, 0, axis_index_groups=same_core)
    package = pages * QH + 2 * SUB
    sent = call(
        functools.partial(attend_kernel, width),
        near((chips, package, HD), bf16),
        [SMEM] + [NEAR] * 3,
        [pltpu.VMEM((chunk // HD * SUB, HD), f32)],
    )(position, received, kv_cache, bounds)
    received = lax.all_to_all(sent, "seq", 0, 0, axis_index_groups=same_core)
    far = lax.ppermute(received, "seq", cores)
    owner_rows = count * pages * QH // LANES
    owner = call(
        functools.partial(owner_kernel, chips, pages),
        near((owner_rows, LANES), jnp.int32),
        [SMEM] * 2 + [NEAR],
    )(position, page_table.T, received)
    final, new_kv = call(
        functools.partial(merge_kernel, pages),
        (
            shape((requests, columns), bf16),
            shape((requests, 2 * KVH * HD), bf16),
        ),
        [SMEM] + [NEAR] * 5,
    )(position, received, far, owner, w_out, middle)
    return (final, new_state.reshape(ssm_state.shape), new_kv)


def shards(*args):
    hidden, in_step, in_groups = args[0], args[3], args[4]
    kv_cache, page_table = args[18], args[19]
    count = lax.axis_size("seq")
    whole_tiles = (
        in_step.shape[1] == 1
        and in_groups.shape[1] == STATE
        and count == 2 * GROUPS
        and hidden.shape[0] == SUB
        and (hidden.shape[1] // count) % LANES == 0
        and SUB % kv_cache.shape[0] == 0
        and LANES % (kv_cache.shape[0] * QH) == 0
        and (count // 2) % (LANES // (kv_cache.shape[0] * QH)) == 0
        and kv_cache.shape[1] == LANES
        and 2 * KVH == count
        and (QH + KVH) * HD % (SUB // kv_cache.shape[0] * 2 * HD) == 0
    )
    return (fused_shards if whole_tiles else plain_shards)(*args)


def solution(mesh):
    placed = (
        P("grp", None),
        P(),
        P(None, "seq"),
        P(None, "seq"),
        P(None, "seq"),
        P("grp", None, "seq"),
        P("grp", None, "seq"),
        P(None, "seq"),
        P(None, "seq"),
        P("seq"),
        P("seq"),
        P("seq"),
        P("seq"),
        P("seq", None),
        P("grp", "seq", None, None),
        P("seq"),
        P("seq", None),
        P(None, "seq"),
        P(("grp", "seq"), None, None),
        P("grp", None),
        P("grp"),
    )
    return jax.shard_map(
        shards,
        mesh=mesh,
        in_specs=placed,
        out_specs=(P("grp", "seq"), P("grp", "seq", None, None), P("grp", None)),
        check_vma=False,
    )
```

```python
import functools

import jax
import jax.numpy as jnp
from jax import lax
from jax.experimental import pallas as pl
from jax.experimental.pallas import tpu as pltpu
from jax.sharding import PartitionSpec as P

QH = 32
KVH = 8
HD = 128
STATE = 128
GROUPS = 8
LANES = 128

epsilon = 1e-05
lowest = -1e30


def conv_step(state, fresh, taps):
    window = jnp.concatenate([state.astype(jnp.float32), fresh[:, None, :]], axis=1)
    summed = jnp.sum(window * taps[:-1][None], axis=1) + taps[-1][None]
    return jax.nn.silu(summed)


def split(value, parts):
    pieces = []
    rest = value
    for _ in range(parts):
        piece = lax.reduce_precision(rest, 8, 7)
        pieces.append(piece.astype(jnp.bfloat16))
        rest = rest - piece
    return pieces


def group_vectors(group_conv, heads_here, requests):
    count = lax.axis_size("seq")
    position = lax.axis_index("seq")
    if heads_here == 1 and group_conv.shape[1] == STATE and count == 2 * GROUPS:
        swap = [(i, (i + GROUPS) % count) for i in range(count)]
        other = lax.ppermute(group_conv, "seq", swap)
        first = position < GROUPS
        inject = jnp.where(first, group_conv, other)
        readout = jnp.where(first, other, group_conv)
        return (
            inject.astype(jnp.float32)[:, None, :],
            readout.astype(jnp.float32)[:, None, :],
        )
    group_all = lax.all_gather(group_conv, "seq", axis=1, tiled=True).astype(jnp.float32)
    inject = group_all[:, : GROUPS * STATE].reshape(requests, GROUPS, STATE)
    readout = group_all[:, GROUPS * STATE :].reshape(requests, GROUPS, STATE)
    head_ids = position * heads_here + jnp.arange(heads_here, dtype=jnp.int32)
    return inject[:, head_ids % GROUPS], readout[:, head_ids % GROUPS]


def plain_shards(
    hidden,
    mix_gain,
    in_gate_input,
    in_step,
    in_groups,
    conv_input,
    conv_groups,
    taps_input,
    taps_groups,
    decay_rate,
    step_bias,
    skip_gain,
    norm_gain,
    out_mixer,
    ssm_state,
    attn_gain,
    w_qkv,
    w_out,
    kv_cache,
    page_table,
    lengths,
):
    count_seq = lax.axis_size("seq")
    position = lax.axis_index("seq")
    requests = hidden.shape[0]
    width = hidden.shape[1]
    heads_here = in_step.shape[1]
    head_width = in_gate_input.shape[1] // (2 * heads_here)
    heads_total = heads_here * count_seq
    per_group = heads_total // GROUPS
    columns = width // count_seq
    stream = hidden.astype(jnp.float32)
    normed = (
        stream * lax.rsqrt(jnp.mean(stream * stream, axis=-1, keepdims=True) + epsilon) * mix_gain
    ).astype(jnp.bfloat16)
    group_raw = jnp.dot(normed, in_groups, preferred_element_type=jnp.float32)
    group_conv = conv_step(conv_groups, group_raw, taps_groups).astype(jnp.bfloat16)
    inject_heads, readout_heads = group_vectors(group_conv, heads_here, requests)
    gate_input = jnp.dot(normed, in_gate_input, preferred_element_type=jnp.float32).reshape(
        requests, heads_here, 2, head_width
    )
    gate_part = gate_input[:, :, 0]
    input_part = gate_input[:, :, 1].reshape(requests, heads_here * head_width)
    step_raw = jnp.dot(normed, in_step, preferred_element_type=jnp.float32)
    conv_out = conv_step(conv_input, input_part, taps_input).reshape(
        requests, heads_here, head_width
    )
    step_size = jax.nn.softplus(step_raw + step_bias)
    decay = jnp.exp(-decay_rate * step_size)
    new_state = (
        decay[:, :, None, None] * ssm_state
        + (step_size[:, :, None] * conv_out)[:, :, :, None] * inject_heads[:, :, None, :]
    )
    ssm_out = (
        jnp.sum(new_state * readout_heads[:, :, None, :], axis=-1)
        + skip_gain[None, :, None] * conv_out
    )
    gated = ssm_out * jax.nn.silu(gate_part)
    head_squares = jnp.sum(gated * gated, axis=-1)
    weighted = (gated * norm_gain.reshape(heads_here, head_width)).astype(jnp.bfloat16)
    products = jnp.einsum(
        "rhp,hpd->hrd",
        weighted,
        out_mixer.reshape(heads_here, head_width, width),
        preferred_element_type=jnp.float32,
    ).astype(jnp.bfloat16)
    products = products.reshape(heads_here, requests, count_seq, columns).transpose(2, 0, 1, 3)
    marks = jnp.stack(split(head_squares.T, 2), axis=-1)
    marks = jnp.pad(marks, ((0, 0), (0, 0), (0, LANES - 2)))
    marks = jnp.broadcast_to(marks[None], (count_seq,) + marks.shape)
    received = lax.all_to_all(jnp.concatenate([products, marks], axis=-1), "seq", 0, 0)
    received = received.astype(jnp.float32)
    squares = (received[..., columns] + received[..., columns + 1]).reshape(
        per_group, GROUPS, requests
    )
    scales = lax.rsqrt(jnp.sum(squares, axis=0) / (per_group * head_width) + epsilon)
    mixer = jnp.sum(
        received[..., :columns].reshape(per_group, GROUPS, requests, columns)
        * scales[None, :, :, None],
        axis=(0, 1),
    )
    stream_cols = lax.dynamic_slice_in_dim(stream, position * columns, columns, 1)
    middle = (stream_cols + mixer).astype(jnp.bfloat16)
    middle_f = middle.astype(jnp.float32)
    scaled = (middle_f * attn_gain).astype(jnp.bfloat16)
    partial_sq = jnp.sum(middle_f * middle_f, axis=-1)
    pages_here = kv_cache.shape[0]
    page_len = kv_cache.shape[1]
    pages_req = page_table.shape[1]
    pages_all = pages_here * count_seq
    matches = page_table[None, :, :] == jnp.arange(pages_all, dtype=jnp.int32)[:, None, None]
    owner = jnp.any(matches, axis=2)
    page_rows = jnp.dot(
        owner.astype(jnp.bfloat16), scaled, preferred_element_type=jnp.float32
    ).astype(jnp.bfloat16)
    page_proj = jnp.dot(page_rows, w_qkv, preferred_element_type=jnp.float32).astype(jnp.bfloat16)
    page_sq = jnp.sum(jnp.where(owner, partial_sq[None, :], 0.0), axis=1)
    sq_parts = jnp.pad(jnp.stack(split(page_sq, 2), axis=-1), ((0, 0), (0, LANES - 2)))
    sent = jnp.concatenate([page_proj, sq_parts], axis=-1).reshape(count_seq, pages_here, -1)
    arrived = jnp.sum(lax.all_to_all(sent, "seq", 0, 0).astype(jnp.float32), axis=0)
    qkv_width = w_qkv.shape[1]
    total_sq = arrived[:, qkv_width] + arrived[:, qkv_width + 1]
    qkv = (arrived[:, :qkv_width] * lax.rsqrt(total_sq / width + epsilon)[:, None]).astype(
        jnp.bfloat16
    )
    group_size = QH // KVH
    queries = qkv[:, : QH * HD].reshape(pages_here, KVH, group_size, HD)
    fresh_kv = qkv[:, QH * HD :]
    fresh_keys = fresh_kv[:, : KVH * HD].reshape(pages_here, KVH, 1, HD).astype(jnp.float32)
    fresh_values = fresh_kv[:, KVH * HD :].reshape(pages_here, KVH, 1, HD).astype(jnp.float32)
    scale = 1.0 / HD**0.5
    slots = position * pages_here + jnp.arange(pages_here, dtype=jnp.int32)
    own_matches = page_table[None, :, :] == slots[:, None, None]
    logical = jnp.sum(
        jnp.any(own_matches, axis=1) * jnp.arange(pages_req, dtype=jnp.int32)[None, :], axis=1
    )
    page_length = jnp.sum(jnp.where(jnp.any(own_matches, axis=2), lengths[None, :], 0), axis=1)
    token_pos = logical[:, None] * page_len + jnp.arange(page_len, dtype=jnp.int32)[None, :]
    live = (token_pos < page_length[:, None])[:, None, None, :]
    leads = (logical == 0)[:, None, None]
    cached = kv_cache.reshape(pages_here, page_len, 2, KVH, HD)
    scores = (
        jnp.einsum("pgjd,ptgd->pgjt", queries, cached[:, :, 0], preferred_element_type=jnp.float32)
        * scale
    )
    own = jnp.sum(queries.astype(jnp.float32) * fresh_keys, axis=-1) * scale
    masked = jnp.where(live, scores, lowest)
    own = jnp.where(leads, own, lowest)
    peak = jnp.maximum(jnp.max(masked, axis=-1), own)
    weights = jnp.where(live, jnp.exp(masked - peak[..., None]), 0.0)
    own_weight = jnp.where(leads, jnp.exp(own - peak), 0.0)
    total = jnp.sum(weights, axis=-1) + own_weight
    values = jnp.einsum(
        "pgjt,ptgd->pgjd",
        weights.astype(jnp.bfloat16),
        cached[:, :, 1],
        preferred_element_type=jnp.float32,
    )
    values = values + own_weight[..., None] * fresh_values
    some = total > 0.0
    safe = jnp.where(some, total, 1.0)
    values = (values / safe[..., None]).astype(jnp.bfloat16)
    logsum = jnp.where(some, peak + jnp.log(safe), lowest)
    logs = jnp.concatenate(split(logsum.reshape(1, pages_here * QH), 3), axis=0)
    logs = jnp.pad(logs, ((0, 5), (0, LANES - pages_here * QH)))
    value_rows = pages_here * QH
    kv_rows = pages_here * 2 * KVH
    package = jnp.concatenate(
        [values.reshape(value_rows, HD), fresh_kv.reshape(kv_rows, HD), logs], axis=0
    )
    package = jnp.broadcast_to(package[None], (count_seq,) + package.shape)
    everything = lax.all_to_all(package, "seq", 0, 0)
    all_values = everything[:, :value_rows].reshape(pages_all, QH, HD)
    all_kv = everything[:, value_rows : value_rows + kv_rows].reshape(pages_all, 2 * KVH * HD)
    all_logs = everything[:, value_rows + kv_rows :, : pages_here * QH].astype(jnp.float32)
    all_logs = (all_logs[:, 0] + all_logs[:, 1] + all_logs[:, 2]).reshape(pages_all, QH)
    new_kv = all_kv[page_table[:, 0]]
    req_logs = all_logs[page_table]
    top = jnp.max(req_logs, axis=1, keepdims=True)
    factors = jnp.exp(req_logs - top)
    summed = jnp.sum(factors[..., None] * all_values[page_table].astype(jnp.float32), axis=1)
    attended = (summed / jnp.sum(factors, axis=1)[..., None]).astype(jnp.bfloat16)
    final = (
        middle_f
        + jnp.dot(
            attended.reshape(requests, QH * HD), w_out, preferred_element_type=jnp.float32
        )
    ).astype(jnp.bfloat16)
    return (final, new_state, new_kv)


f32 = jnp.float32
bf16 = jnp.bfloat16
SUB = 8
PARTS = 3
SCOPED = 16 << 20
MOST = 63500 << 10
BLOCKS = 2
GATE_BLOCKS = 1
VMEM = pl.BlockSpec(memory_space=pltpu.VMEM)
NEAR = pl.BlockSpec(memory_space=pltpu.VMEM)
SMEM = pl.BlockSpec(memory_space=pltpu.SMEM)
FAR = pl.BlockSpec(memory_space=pltpu.HBM)


def call(kernel, outs, specs, scratch=(), scoped=SCOPED):
    grid_free = pl.pallas_call(
        kernel,
        out_shape=outs,
        in_specs=specs,
        out_specs=jax.tree.map(lambda _: VMEM, outs, is_leaf=lambda x: hasattr(x, "shape")),
        scratch_shapes=scratch,
        compiler_params=pltpu.CompilerParams(vmem_limit_bytes=scoped),
    )

    def run(*args):
        spaces = {id(NEAR): pltpu.VMEM, id(FAR): pltpu.HBM}
        placed = [
            pltpu.with_memory_space_constraint(arg, spaces[id(spec)]) if id(spec) in spaces else arg
            for arg, spec in zip(args, specs)
        ]
        return grid_free(*placed)

    return run


def shape(dims, kind):
    return jax.ShapeDtypeStruct(dims, kind)


def near(dims, kind):
    return pltpu.VMEM(dims, kind)


def silu(x):
    return x * jax.nn.sigmoid(x)


def pieces(value, parts):
    out = []
    for _ in range(parts):
        piece = value.astype(bf16).astype(f32)
        out.append(piece)
        value = value - piece
    return out


def marked(value, parts, first=0):
    lane = lax.broadcasted_iota(jnp.int32, (value.shape[0], LANES), 1)
    out = jnp.zeros((value.shape[0], LANES), f32)
    for k, piece in enumerate(pieces(value, parts)):
        out = jnp.where(lane == first + k, piece, out)
    return out


def summed(marks, first=0):
    return marks[:, first : first + 1] + marks[:, first + 1 : first + 2]


def convolve(state_ref, fresh, taps_ref):
    taps = state_ref.shape[0]
    total = taps_ref[taps : taps + 1, :] * fresh + taps_ref[taps + 1 : taps + 2, :]
    for k in range(taps):
        total = total + taps_ref[k : k + 1, :] * state_ref[k].astype(f32)
    return silu(total)


def fetch_all(pairs, sems):
    copies = [
        pltpu.make_async_copy(source, target, sems.at[k])
        for k, (source, target) in enumerate(pairs)
    ]
    for copy in copies:
        copy.start()
    return copies


def group_kernel(
    hidden_far,
    gain_far,
    weights_far,
    state_far,
    taps_far,
    group_out,
    normed_out,
    hidden,
    gain,
    weights,
    state,
    taps,
    sems,
):
    depth = weights.shape[0] // BLOCKS
    rows = [pl.ds(k * depth, depth) for k in range(BLOCKS)]
    copies = fetch_all(
        [(hidden_far, hidden), (gain_far, gain)]
        + [(weights_far.at[r], weights.at[r]) for r in rows]
        + [(state_far, state), (taps_far, taps)],
        sems,
    )
    copies[0].wait()
    copies[1].wait()
    stream = hidden[...].astype(f32)
    mean = jnp.mean(stream * stream, axis=-1, keepdims=True)
    normed_out[...] = (stream * lax.rsqrt(mean + epsilon) * gain[...]).astype(bf16)
    raw = jnp.zeros(group_out.shape, f32)
    for k in range(BLOCKS):
        copies[2 + k].wait()
        span = slice(k * depth, (k + 1) * depth)
        raw = raw + jnp.dot(normed_out[:, span], weights[span, :], preferred_element_type=f32)
    copies[-2].wait()
    copies[-1].wait()
    group_out[...] = convolve(state, raw, taps).astype(bf16)


def gate_kernel(carried, position, normed_ref, *refs):
    weights_far, step_far, state_far, taps_far, numbers, hidden_far = refs[:6]
    inputs, outputs, scratch = refs[6 : 6 + carried], refs[6 + carried : -5], refs[-5:]
    gate_out, conv_out, step_out, decay_out, columns_out = outputs[:5]
    weights, step_row, state, taps, sems = scratch
    columns = columns_out.shape[1]
    start = pl.multiple_of(position[0] * columns, columns)
    depth = weights.shape[0] // GATE_BLOCKS
    rows = [pl.ds(k * depth, depth) for k in range(GATE_BLOCKS)]
    copies = fetch_all(
        [(weights_far.at[r], weights.at[r]) for r in rows]
        + [
            (step_far, step_row),
            (state_far, state),
            (taps_far, taps),
            (hidden_far.at[:, pl.ds(start, columns)], columns_out),
        ]
        + list(zip(inputs, outputs[5:])),
        sems,
    )
    half = gate_out.shape[1]
    both = jnp.zeros((gate_out.shape[0], weights.shape[1]), f32)
    for k in range(GATE_BLOCKS):
        copies[k].wait()
        span = slice(k * depth, (k + 1) * depth)
        both = both + jnp.dot(normed_ref[:, span], weights[span, :], preferred_element_type=f32)
    for copy in copies[GATE_BLOCKS : GATE_BLOCKS + 3]:
        copy.wait()
    gate_out[...] = silu(both[:, :half])
    fresh = convolve(state, both[:, half:], taps)
    conv_out[:, :half] = fresh
    conv_out[:, half:] = numbers[:, 2:3] * fresh
    raw = jnp.sum(normed_ref[...].astype(f32) * step_row[...].astype(f32), axis=-1, keepdims=True)
    step = jax.nn.softplus(raw + numbers[:, 1:2])
    step_out[...] = jnp.broadcast_to(step, step_out.shape)
    decay_out[...] = jnp.broadcast_to(jnp.exp(-numbers[:, 0:1] * step), decay_out.shape)
    for copy in copies[GATE_BLOCKS + 3 :]:
        copy.wait()


def chosen(position, own, other):
    first = position[0] < GROUPS
    mine, theirs = own[...].astype(f32), other[...].astype(f32)
    return jnp.where(first, mine, theirs), jnp.where(first, theirs, mine)


def mixer_kernel(position, own, other, gate, conv, step, decay, state, weights, gain, sent):
    requests = own.shape[0]
    inject, readout = chosen(position, own, other)
    half = gate.shape[1]
    both = 2 * half
    flat = state[...].reshape(requests * half, state.shape[2])
    high = flat.astype(bf16)
    low = (flat - high.astype(f32)).astype(bf16)
    vectors = readout.astype(bf16)
    full = sum(
        lax.dot_general(
            vectors, term, (((1,), (1,)), ((), ())), preferred_element_type=f32
        )
        for term in (high, low)
    )
    row = lax.broadcasted_iota(jnp.int32, (requests, both), 0)
    pairs = jnp.zeros((requests, both), f32)
    for k in range(requests // 2):
        pairs = jnp.where(row // 2 == k, full[:, k * both : (k + 1) * both], pairs)
    read = jnp.where(row[:, :half] % 2 == 0, pairs[:, :half], pairs[:, half:])
    along = jnp.sum(inject * readout, axis=-1, keepdims=True)
    fresh = conv[:, :half]
    out = decay[:, :1] * read + step[:, :1] * fresh * along + conv[:, half:]
    gated = out * gate[...]
    marks = marked(jnp.sum(gated * gated, axis=-1, keepdims=True), 2).astype(bf16)
    weighted = (gated * gain[...]).astype(bf16)
    count = sent.shape[0]
    columns = weights.shape[1] // count
    for e in range(count):
        product = jnp.dot(
            weighted, weights[:, e * columns : (e + 1) * columns], preferred_element_type=f32
        )
        sent[e, :, :columns] = product.astype(bf16)
        sent[e, :, columns:] = marks


def state_kernel(
    pages, page_len, position, own, other, conv, step, decay, state, table, lengths, new_state, bounds
):
    order = lax.broadcasted_iota(jnp.int32, table.shape, 0)
    spans = jnp.broadcast_to(lengths[...], table.shape)
    for p in range(pages):
        hit = table[...] == position[0] * pages + p
        logical = jnp.sum(jnp.where(hit, order, 0), axis=(0, 1), keepdims=True)
        length = jnp.sum(jnp.where(hit, spans, 0), axis=(0, 1), keepdims=True)
        lane = jnp.zeros((1, LANES), jnp.int32)
        bounds[p : p + 1, :] = lane + (length - logical * page_len)
        bounds[pages + p : pages + p + 1, :] = lane + jnp.where(logical == 0, 1, 0)
    inject, _ = chosen(position, own, other)
    fresh = step[:, :1] * conv[:, : state.shape[1]]
    new_state[...] = (
        decay[:, :1][:, :, None] * state[...] + fresh[:, :, None] * inject[:, None, :]
    )


def project_kernel(
    chunks, head_width, position, received, hidden, gain, weights, table, keep, give, middle_out
):
    count, requests, _ = received.shape
    columns = weights.shape[0]
    squares = [received[k, :, columns:].astype(f32) for k in range(count)]
    mixer = jnp.zeros((requests, columns), f32)
    for g in range(GROUPS):
        members = range(g, count, GROUPS)
        marks = sum(squares[k] for k in members)
        total = marks[:, :1] + marks[:, 1:2]
        scale = lax.rsqrt(total / (len(members) * head_width) + epsilon)
        products = sum(received[k, :, :columns].astype(f32) for k in members)
        mixer = mixer + scale * products
    middle = (hidden[...].astype(f32) + mixer).astype(bf16).astype(f32)
    middle_out[...] = middle
    square = jnp.sum(middle * middle, axis=-1, keepdims=True)
    scaled = middle * gain[...]
    extended = jnp.concatenate([scaled, marked(square, 2)], axis=-1).astype(bf16)
    rows = count * SUB
    pages = SUB // chunks
    chips = count // 2
    core = position[0] % 2
    index = lax.broadcasted_iota(jnp.int32, (rows, requests), 0)
    line = index % (chips * SUB)
    parity = jnp.where(index < chips * SUB, core, 1 - core)
    page = ((line // SUB) * 2 + parity) * pages + index % pages
    hits = page == table[0:1, :]
    for j in range(1, table.shape[0]):
        hits = jnp.logical_or(hits, page == table[j : j + 1, :])
    onehot = jnp.where(hits, 1.0, 0.0).astype(bf16)
    spread = jnp.dot(onehot, extended, preferred_element_type=f32)
    lines = spread[:, :columns]
    which = (lax.broadcasted_iota(jnp.int32, lines.shape, 0) % SUB) // pages
    fresh_from = QH * HD
    value_from = fresh_from + KVH * HD
    chunk = value_from // chunks
    plain = jnp.concatenate([scaled, jnp.zeros((SUB, columns), f32)], axis=0)
    lhs = []
    for c in range(chunks):
        own = jnp.where(which == c, lines, 0.0)
        if (c + 1) * chunk > fresh_from:
            own = jnp.concatenate([own, plain], axis=0)
        lhs.append(own.astype(bf16))
    tile = 2 * HD

    def share_out(first, fresh):
        chip = (first - fresh_from) // tile
        low, high = fresh[:, :HD], fresh[:, HD:]
        keep[chip, :, chunk + LANES :] = jnp.where(core == 0, low, high)
        give[chip, :, chunk + LANES :] = jnp.where(core == 0, high, low).astype(bf16)

    plain = plain.astype(bf16)
    for first in range(value_from, weights.shape[1], tile):
        fresh = jnp.dot(plain, weights[:, first : first + tile], preferred_element_type=f32)
        share_out(first, fresh[:SUB])
    for n in range(0, chunk, tile):
        total = None
        for c in range(chunks):
            first = c * chunk + n
            part = jnp.dot(lhs[c], weights[:, first : first + tile], preferred_element_type=f32)
            if first >= fresh_from:
                share_out(first, part[rows : rows + SUB])
            total = part[:rows] if total is None else total + part[:rows]
        for e in range(chips):
            keep[e, :, n : n + tile] = total[e * SUB : (e + 1) * SUB]
            first = (chips + e) * SUB
            give[e, :, n : n + tile] = total[first : first + SUB].astype(bf16)
    marks = spread[:, columns:]
    request_marks = marked(square, 2, 2)
    for e in range(chips):
        keep[e, :, chunk : chunk + LANES] = marks[e * SUB : (e + 1) * SUB] + request_marks
        first = (chips + e) * SUB
        give[e, :, chunk : chunk + LANES] = (marks[first : first + SUB] + request_marks).astype(
            bf16
        )


def pair_kernel(keep, taken, _, sent):
    chunk = keep.shape[2] - 2 * LANES
    for e in range(keep.shape[0]):
        total = keep[e] + taken[e].astype(f32)
        marks = total[:, chunk : chunk + LANES]
        sent[e, :, :chunk] = total[:, :chunk].astype(bf16)
        sent[e, :, chunk : chunk + LANES] = (
            marked(summed(marks), 2) + marked(summed(marks, 2), 2, 2)
        ).astype(bf16)
        sent[e, :, chunk + LANES :] = total[:, chunk + LANES :].astype(bf16)


def attend_kernel(width, position, received, cache, bounds, sent, lines):
    count, _, full = received.shape
    pages, page_len, _ = cache.shape
    chunks = SUB // pages
    chunk = full - 2 * LANES
    tiles = chunk // HD
    total = received[0].astype(f32)
    for k in range(1, count):
        total = total + received[k].astype(f32)
    marks = total[:, chunk : chunk + LANES]
    inverse = lax.rsqrt(summed(marks) / width + epsilon)
    fresh = total[:, chunk + LANES :] * lax.rsqrt(summed(marks, 2) / width + epsilon)
    fresh = fresh.astype(bf16)
    for t in range(tiles):
        lines[t * SUB : (t + 1) * SUB, :] = (
            (total[:, t * HD : (t + 1) * HD] * inverse).astype(bf16).astype(f32)
        )

    def heads(page, first, many):
        runs = []
        while many:
            run = min(many, tiles - first % tiles)
            start = (first % tiles) * SUB + (first // tiles) * pages + page
            runs.append(lines[pl.ds(start, run, stride=SUB), :])
            first, many = first + run, many - run
        return runs[0] if len(runs) == 1 else jnp.concatenate(runs, axis=0)

    group = QH // KVH
    scale = 1.0 / HD**0.5
    lane = lax.broadcasted_iota(jnp.int32, (1, page_len), 1)
    head_group = lax.broadcasted_iota(jnp.int32, (QH, HD), 0) // group
    eye = lax.broadcasted_iota(jnp.int32, (QH, LANES), 0)
    value_rows = pages * QH
    place = (position[0] // 2) % (LANES // value_rows) * value_rows
    eye_lane = lax.broadcasted_iota(jnp.int32, (QH, LANES), 1) - place
    log_row = jnp.zeros((1, LANES), f32)
    own_row = jnp.zeros((1, LANES), f32)
    for p in range(pages):
        live = lane < bounds[p : p + 1, :]
        leads = bounds[pages + p : pages + p + 1, :1] == 1
        query = jnp.concatenate([heads(p, g * group, group) for g in range(KVH)], axis=0)
        keys = [heads(p, QH + g, 1) for g in range(KVH)]
        key_rows = jnp.concatenate([jnp.broadcast_to(k, (group, HD)) for k in keys], axis=0)
        spread = jnp.concatenate(
            [jnp.where(head_group == g, query, 0.0).astype(bf16) for g in range(KVH)], axis=-1
        )
        scores = (
            lax.dot_general(
                spread,
                cache[p, :, : KVH * HD],
                (((1,), (1,)), ((), ())),
                preferred_element_type=f32,
            )
            * scale
        )
        own = jnp.sum(query * key_rows, axis=-1, keepdims=True) * scale
        masked = jnp.where(live, scores, lowest)
        own = jnp.where(leads, own, lowest)
        peak = jnp.max(masked, axis=-1, keepdims=True)
        weights = jnp.where(live, jnp.exp(masked - peak), 0.0)
        mass = jnp.sum(weights, axis=-1, keepdims=True)
        wide = jnp.dot(
            weights.astype(bf16), cache[p, :, KVH * HD :], preferred_element_type=f32
        )
        mixed = jnp.zeros((QH, HD), f32)
        for g in range(KVH):
            mixed = mixed + jnp.where(head_group == g, wide[:, g * HD : (g + 1) * HD], 0.0)
        some = mass > 0.0
        safe = jnp.where(some, mass, 1.0)
        result = (mixed / safe).astype(bf16)
        logs = jnp.where(some, peak + jnp.log(safe), lowest)
        here = eye_lane == eye + p * QH
        log_row = log_row + jnp.sum(jnp.where(here, logs, 0.0), axis=0, keepdims=True)
        own_row = own_row + jnp.sum(jnp.where(here, own, 0.0), axis=0, keepdims=True)
        for e in range(count):
            sent[e, p * QH : (p + 1) * QH, :] = result
    terms = pieces(log_row, PARTS) + pieces(own_row, PARTS)
    terms.append(jnp.zeros((SUB - 2 * PARTS, LANES), f32))
    terms = jnp.concatenate(terms, axis=0).astype(bf16)
    for e in range(count):
        sent[e, value_rows : value_rows + SUB, :] = fresh
        sent[e, value_rows + SUB :, :] = terms


def owner_kernel(chips, pages, position, table, _, owner):
    pages_req, requests = table.shape
    core = position[0] % 2
    span = pages * QH
    rows_each = owner.shape[0] // 2
    row = lax.broadcasted_iota(jnp.int32, owner.shape, 0)
    lane = lax.broadcasted_iota(jnp.int32, owner.shape, 1)
    chip = (row % rows_each) * (LANES // span) + lane // span
    parity = jnp.where(row < rows_each, core, 1 - core)
    page = (chip * 2 + parity) * pages + (lane % span) // QH
    found = jnp.zeros(owner.shape, jnp.int32)
    for r in range(requests):
        for j in range(pages_req):
            found = jnp.where(page == table[j, r], r, found)
    owner[...] = found


def merge_kernel(pages, position, near_ref, far_ref, owner, weights, middle, final, new_kv):
    chips = near_ref.shape[0]
    requests, width = middle.shape
    value_rows = pages * QH
    core = position[0] % 2
    packages = (near_ref, far_ref)
    fresh = []
    for chip in range(chips):
        mine, theirs = (ref[chip, value_rows : value_rows + SUB, :].astype(f32) for ref in packages)
        fresh += [jnp.where(core == 0, mine, theirs), jnp.where(core == 0, theirs, mine)]
    for k, part in enumerate(fresh):
        new_kv[:, k * HD : (k + 1) * HD] = part.astype(bf16)
    each = LANES // value_rows
    request = lax.broadcasted_iota(jnp.int32, (requests, LANES), 0)
    lane = lax.broadcasted_iota(jnp.int32, (requests, LANES), 1)
    logs, own_logs, hits = [], [], []
    for ref in packages:
        for chip in range(0, chips, each):
            terms = sum(ref[chip + k, value_rows + SUB :, :].astype(f32) for k in range(each))
            for first, rows in ((0, logs), (PARTS, own_logs)):
                log = sum(terms[first + k : first + k + 1, :] for k in range(PARTS))
                rows.append(jnp.broadcast_to(log, (requests, LANES)))
            row = len(hits)
            hits.append(jnp.broadcast_to(owner[row : row + 1, :], (requests, LANES)) == request)

    def over_pages(value, combine):
        out = value
        for k in range(QH, LANES, QH):
            out = combine(out, pltpu.roll(value, k, 1))
        return out

    tops = functools.reduce(
        jnp.maximum,
        [
            jnp.where(hit, jnp.maximum(log, own), lowest)
            for hit, log, own in zip(hits, logs, own_logs)
        ],
    )
    tops = over_pages(tops, jnp.maximum)
    factors = [jnp.where(hit, jnp.exp(log - tops), 0.0) for hit, log in zip(hits, logs)]
    own = sum(jnp.where(hit, jnp.exp(log - tops), 0.0) for hit, log in zip(hits, own_logs))
    own = over_pages(own, jnp.add)
    inverse = 1.0 / (over_pages(functools.reduce(jnp.add, factors), jnp.add) + own)
    own_share = own * inverse
    shares = []
    for factor in factors:
        share = factor * inverse
        heads = [jnp.where(lane % QH == h, share, 0.0) for h in range(QH)]
        shares.append(jnp.concatenate(heads, axis=0).astype(bf16))
    half = len(shares) // 2
    mixed = None
    for side, ref in enumerate(packages):
        part = jnp.dot(
            jnp.concatenate(shares[side * half : (side + 1) * half], axis=1),
            jnp.concatenate([ref[chip, :value_rows, :] for chip in range(chips)], axis=0),
            preferred_element_type=f32,
        )
        mixed = part if mixed is None else mixed + part
    attended = jnp.concatenate(
        [
            mixed[h * requests : (h + 1) * requests]
            + own_share[:, h : h + 1] * fresh[KVH + h // (QH // KVH)]
            for h in range(QH)
        ],
        axis=1,
    ).astype(bf16)
    total = jnp.dot(attended, weights[...], preferred_element_type=f32)
    final[...] = (middle[...] + total).astype(bf16)


def fused_shards(
    hidden,
    mix_gain,
    in_gate_input,
    in_step,
    in_groups,
    conv_input,
    conv_groups,
    taps_input,
    taps_groups,
    decay_rate,
    step_bias,
    skip_gain,
    norm_gain,
    out_mixer,
    ssm_state,
    attn_gain,
    w_qkv,
    w_out,
    kv_cache,
    page_table,
    lengths,
):
    count = lax.axis_size("seq")
    position = lax.axis_index("seq").astype(jnp.int32).reshape(1)
    requests, width = hidden.shape
    columns = width // count
    head_width = in_gate_input.shape[1] // 2
    pages = kv_cache.shape[0]
    chunks = SUB // pages
    chips = count // 2
    gcols = in_groups.shape[1]
    state = ssm_state.reshape(requests, head_width, STATE)
    same_core = [list(range(core, count, 2)) for core in range(2)]
    cores = [(i, i ^ 1) for i in range(count)]
    group_args = (
        hidden,
        mix_gain.reshape(1, width),
        in_groups,
        conv_groups.transpose(1, 0, 2),
        taps_groups,
    )
    group_conv, normed = call(
        group_kernel,
        (near((requests, gcols), bf16), near((requests, width), bf16)),
        [FAR] * 5,
        [pltpu.VMEM(x.shape, x.dtype) for x in group_args]
        + [pltpu.SemaphoreType.DMA((len(group_args) - 1 + BLOCKS,))],
        MOST,
    )(*group_args)
    swap = [(i, (i + GROUPS) % count) for i in range(count)]
    other = lax.ppermute(group_conv, "seq", swap)
    carried = (
        state,
        out_mixer,
        norm_gain.reshape(1, head_width),
        attn_gain.reshape(1, columns),
        page_table.T,
    )
    gate_args = (
        in_gate_input,
        in_step.T,
        conv_input.transpose(1, 0, 2),
        taps_input,
    )
    numbers = jnp.concatenate([decay_rate, step_bias, skip_gain]).reshape(1, 3)
    gate, conv, step, decay, stream, state_in, mixer, gain, scale, table = call(
        functools.partial(gate_kernel, len(carried)),
        (
            near((requests, head_width), f32),
            near((requests, 2 * head_width), f32),
            near((requests, LANES), f32),
            near((requests, LANES), f32),
            near((requests, columns), bf16),
        )
        + tuple(near(x.shape, x.dtype) for x in carried),
        [SMEM, NEAR] + [FAR] * 4 + [NEAR] + [FAR] * (1 + len(carried)),
        [pltpu.VMEM(x.shape, x.dtype) for x in gate_args]
        + [pltpu.SemaphoreType.DMA((GATE_BLOCKS + 4 + len(carried),))],
    )(position, normed, *gate_args, numbers, hidden, *carried)
    sent = call(
        mixer_kernel,
        near((count, requests, columns + LANES), bf16),
        [SMEM] + [NEAR] * 9,
    )(position, group_conv, other, gate, conv, step, decay, state_in, mixer, gain)
    received = lax.all_to_all(sent, "seq", 0, 0)
    new_state, bounds = call(
        functools.partial(state_kernel, pages, kv_cache.shape[1]),
        (shape(state.shape, f32), near((SUB, LANES), jnp.int32)),
        [SMEM] + [NEAR] * 7 + [VMEM],
    )(position, group_conv, other, conv, step, decay, state_in, table, lengths.reshape(1, requests))
    chunk = (QH + KVH) * HD // chunks
    keep, give, middle = call(
        functools.partial(project_kernel, chunks, head_width),
        (
            near((chips, SUB, chunk + 2 * LANES), f32),
            near((chips, SUB, chunk + 2 * LANES), bf16),
            near((requests, columns), f32),
        ),
        [SMEM] + [NEAR] * 5,
    )(position, received, stream, scale, w_qkv, table)
    taken = lax.ppermute(give, "seq", cores)
    sent = call(pair_kernel, near(give.shape, bf16), [NEAR] * 2 + [FAR])(keep, taken, new_state)
    received = lax.all_to_all(sent, "seq", 0, 0, axis_index_groups=same_core)
    package = pages * QH + 2 * SUB
    sent = call(
        functools.partial(attend_kernel, width),
        near((chips, package, HD), bf16),
        [SMEM] + [NEAR] * 3,
        [pltpu.VMEM((chunk // HD * SUB, HD), f32)],
    )(position, received, kv_cache, bounds)
    received = lax.all_to_all(sent, "seq", 0, 0, axis_index_groups=same_core)
    far = lax.ppermute(received, "seq", cores)
    owner_rows = count * pages * QH // LANES
    owner = call(
        functools.partial(owner_kernel, chips, pages),
        near((owner_rows, LANES), jnp.int32),
        [SMEM] * 2 + [NEAR],
    )(position, page_table.T, received)
    final, new_kv = call(
        functools.partial(merge_kernel, pages),
        (
            shape((requests, columns), bf16),
            shape((requests, 2 * KVH * HD), bf16),
        ),
        [SMEM] + [NEAR] * 5,
    )(position, received, far, owner, w_out, middle)
    return (final, new_state.reshape(ssm_state.shape), new_kv)


def shards(*args):
    hidden, in_step, in_groups = args[0], args[3], args[4]
    kv_cache, page_table = args[18], args[19]
    count = lax.axis_size("seq")
    whole_tiles = (
        in_step.shape[1] == 1
        and in_groups.shape[1] == STATE
        and count == 2 * GROUPS
        and hidden.shape[0] == SUB
        and (hidden.shape[1] // count) % LANES == 0
        and SUB % kv_cache.shape[0] == 0
        and LANES % (kv_cache.shape[0] * QH) == 0
        and (count // 2) % (LANES // (kv_cache.shape[0] * QH)) == 0
        and kv_cache.shape[1] == LANES
        and 2 * KVH == count
        and (QH + KVH) * HD % (SUB // kv_cache.shape[0] * 2 * HD) == 0
    )
    return (fused_shards if whole_tiles else plain_shards)(*args)


def solution(mesh):
    placed = (
        P("grp", None),
        P(),
        P(None, "seq"),
        P(None, "seq"),
        P(None, "seq"),
        P("grp", None, "seq"),
        P("grp", None, "seq"),
        P(None, "seq"),
        P(None, "seq"),
        P("seq"),
        P("seq"),
        P("seq"),
        P("seq"),
        P("seq", None),
        P("grp", "seq", None, None),
        P("seq"),
        P("seq", None),
        P(None, "seq"),
        P(("grp", "seq"), None, None),
        P("grp", None),
        P("grp"),
    )
    return jax.shard_map(
        shards,
        mesh=mesh,
        in_specs=placed,
        out_specs=(P("grp", "seq"), P("grp", "seq", None, None), P("grp", None)),
        check_vma=False,
    )
```
